32 devices in a mesh: dp: 8 (over z, x), tensor: 4 (over y, core).
Axes of the slice: x: 2, y: 2, z: 4, core: 2. Of those that a mesh axis runs over, the one named last changes fastest.
Arguments:
- inputs: bfloat16 [4096, 2048], P(('dp', 'tensor')), may hold values from -6 to 6
- cotangent: bfloat16 [4096, 2048], P(('dp', 'tensor')), may hold values from -6 to 6
- log_decay: float32 [8, 4096], P('tensor', 'dp'), may hold values from -1 to 0, as said below
- query_weight: bfloat16 [2048, 2048], P('dp', 'tensor'), may hold values from -0.125 to 0.125
- key_weight: bfloat16 [2048, 2048], P('dp', 'tensor'), may hold values from -0.125 to 0.125
- value_weight: bfloat16 [2048, 4096], P('dp', 'tensor'), may hold values from -0.125 to 0.125
- gate_weight: bfloat16 [2048, 4096], P('dp', 'tensor'), may hold values from -0.125 to 0.125
- out_weight: bfloat16 [4096, 2048], P('tensor', 'dp'), may hold values from -0.09375 to 0.09375
- group_gain: bfloat16 [8, 512], P('tensor', 'dp'), may hold values from 0.25 to 1.75
- norm_gains: bfloat16 [2, 2048], P(None, 'dp'), may hold values from 0.25 to 1.75
- norm_biases: bfloat16 [2, 2048], P(None, 'dp'), may hold values from -1.5 to 1.5
- ffn_gate_weight: bfloat16 [2048, 4096], P('dp', 'tensor'), may hold values from -0.125 to 0.125
- ffn_up_weight: bfloat16 [2048, 4096], P('dp', 'tensor'), may hold values from -0.125 to 0.125
- ffn_down_weight: bfloat16 [4096, 2048], P('tensor', 'dp'), may hold values from -0.09375 to 0.09375
Outputs:
- layer_out: bfloat16 [4096, 2048], P(('dp', 'tensor'))
- input_grad: bfloat16 [4096, 2048], P(('dp', 'tensor'))
- query_grad: float32 [2048, 2048], P('dp', 'tensor')
- key_grad: float32 [2048, 2048], P('dp', 'tensor')
- value_grad: float32 [2048, 4096], P('dp', 'tensor')
- gate_grad: float32 [2048, 4096], P('dp', 'tensor')
- out_weight_grad: float32 [4096, 2048], P('tensor', 'dp')
- group_gain_grad: float32 [8, 512], P('tensor', 'dp')
- norm_gain_grad: float32 [2, 2048], P(None, ('dp', 'tensor'))
- norm_bias_grad: float32 [2, 2048], P(None, ('dp', 'tensor'))
- ffn_gate_grad: float32 [2048, 4096], P('dp', 'tensor')
- ffn_up_grad: float32 [2048, 4096], P('dp', 'tensor')
- ffn_down_grad: float32 [4096, 2048], P('tensor', 'dp')
The draws below stay inside these ranges and needn't reach their ends.
Inputs may be any that keep to these rules, and one draw needn't show every extreme that they name: `log_decay`: every entry is negative: a per-position log-decay of its head.
All inputs are finite; a program needn't handle non-finite values.
Results may differ from the reference program's by a relative error of at most 0.022.
Values may be sent and summed in bfloat16 or wider, within the bound.
A program may use at most 192 MiB of HBM per device.

```python
import math
import jax
import jax.numpy as jnp
from jax import lax

D = 2048
MEMORY_CHANNELS = 8
HK = 256
HV = 512
FF = 4096
TOKEN_COUNT = 512
TOKENS = 4096
N_DP = 8


def draw_log_decay(key, part):
    stacked_strings = TOKENS // TOKEN_COUNT
    key_rate, key_rough, lookup_offsets, key_drop = jax.random.split(key, 4)
    low_end = math.log(1.0 / (2 * TOKEN_COUNT))
    high_end = math.log(1.0 / 30.0)
    fading_rate_floor = jnp.exp(jax.random.uniform(key_rate, (MEMORY_CHANNELS, stacked_strings, 1), jnp.float32, low_end, high_end))
    rough_approximation = jnp.exp(jax.random.uniform(key_rough, (MEMORY_CHANNELS, stacked_strings, TOKEN_COUNT), jnp.float32, math.log(0.5), math.log(2.0)))
    clustered_spans = jax.random.uniform(lookup_offsets, (MEMORY_CHANNELS, stacked_strings, TOKEN_COUNT), jnp.float32) < 4.0 / TOKEN_COUNT
    fading_falloffs = jnp.log(jax.random.uniform(key_drop, (MEMORY_CHANNELS, stacked_strings, TOKEN_COUNT), jnp.float32, 0.5, 0.8))
    single_increment = -fading_rate_floor * rough_approximation + jnp.where(clustered_spans, fading_falloffs, 0.0)
    return single_increment.reshape(MEMORY_CHANNELS, TOKENS)


def block_scale(stream_key, shape, shards, low, high):
    gain = 1.0
    for position, shards_of in shards:
        heights = jax.random.uniform(jax.random.fold_in(jax.random.fold_in(stream_key, 6), position), (shards_of,), jnp.float32, low / len(shards), high / len(shards))
        gain = gain * jnp.repeat(jnp.exp(heights), shape[position] // shards_of).reshape((-1,) + (1,) * (len(shape) - 1 - position))
    return gain


def normal_values(stream_key, extent, scale, limit, cuts=(), kind=jnp.bfloat16):
    drawn = scale * jax.random.normal(stream_key, extent, jnp.float32)
    if cuts:
        drawn = drawn * block_scale(stream_key, extent, cuts, -0.22, 0.18)
    return jnp.clip(drawn, -limit, limit).astype(kind)


def setup_inputs(seed: int = 0) -> dict:
    streams_of = jax.random.split(jax.random.key(seed), 15)
    inputs = normal_values(streams_of[0], (TOKENS, D), 1.0, 6.0, ((0, 32),))
    cotangent = normal_values(streams_of[1], (TOKENS, D), 1.0, 6.0, ((0, 32),))
    log_decay = draw_log_decay(jax.random.fold_in(streams_of[14], 71), 0)
    query_weight = normal_values(streams_of[3], (D, MEMORY_CHANNELS * HK), D ** -0.5, 0.125, ((0, 8), (1, 4)))
    key_weight = normal_values(streams_of[4], (D, MEMORY_CHANNELS * HK), D ** -0.5, 0.125, ((0, 8), (1, 4)))
    value_weight = normal_values(streams_of[5], (D, MEMORY_CHANNELS * HV), D ** -0.5, 0.125, ((0, 8), (1, 4)))
    gate_weight = normal_values(streams_of[6], (D, MEMORY_CHANNELS * HV), D ** -0.5, 0.125, ((0, 8), (1, 4)))
    out_weight = normal_values(streams_of[7], (MEMORY_CHANNELS * HV, D), (MEMORY_CHANNELS * HV) ** -0.5, 0.09375, ((0, 4), (1, 8)))
    group_gain = jnp.clip(1.0 + 0.15 * jax.random.normal(streams_of[8], (MEMORY_CHANNELS, HV), jnp.float32), 0.25, 1.75).astype(jnp.bfloat16)
    norm_gains = jnp.clip(1.0 + 0.15 * jax.random.normal(streams_of[9], (2, D), jnp.float32), 0.25, 1.75).astype(jnp.bfloat16)
    norm_biases = normal_values(streams_of[10], (2, D), 0.3, 1.5, ((1, 8),))
    ffn_gate_weight = normal_values(streams_of[11], (D, FF), D ** -0.5, 0.125, ((0, 8), (1, 4)))
    ffn_up_weight = normal_values(streams_of[12], (D, FF), D ** -0.5, 0.125, ((0, 8), (1, 4)))
    ffn_down_weight = normal_values(streams_of[13], (FF, D), FF ** -0.5, 0.09375, ((0, 4), (1, 8)))
    return {"inputs": inputs, "cotangent": cotangent, "log_decay": log_decay, "query_weight": query_weight, "key_weight": key_weight, "value_weight": value_weight, "gate_weight": gate_weight, "out_weight": out_weight, "group_gain": group_gain, "norm_gains": norm_gains, "norm_biases": norm_biases, "ffn_gate_weight": ffn_gate_weight, "ffn_up_weight": ffn_up_weight, "ffn_down_weight": ffn_down_weight}


@jax.custom_vjp
def low(v):
    return lax.optimization_barrier(v.astype(jnp.bfloat16)).astype(jnp.float32)

@jax.custom_vjp
def low_back(v):
    return v

def low_keep(v):
    return (low(v), None)

def low_pass(kept, grad):
    return (grad,)

def back_keep(v):
    return (v, None)

def back_low(kept, grad):
    return (low(grad),)
low.defvjp(low_keep, low_pass)
low_back.defvjp(back_keep, back_low)
HIGH_PRECISION = lax.Precision.HIGHEST
EPSILON = 1e-05
GROUP_FLOOR = 1.0

def matmul(left, right):
    return jnp.dot(left, right, precision=HIGH_PRECISION, preferred_element_type=jnp.float32)

def layer_norm(values, gain_row, bias_row):
    center = values - lax.optimization_barrier(jnp.mean(values, axis=-1, keepdims=True))
    spread = lax.optimization_barrier(jnp.mean(center * center, axis=-1, keepdims=True))
    return center * lax.rsqrt(spread + EPSILON) * gain_row + bias_row

def group_norm(values, gain_rows):
    center = values - lax.optimization_barrier(jnp.mean(values, axis=-1, keepdims=True))
    spread = lax.optimization_barrier(jnp.mean(center * center, axis=-1, keepdims=True))
    return center * lax.rsqrt(jnp.maximum(spread, GROUP_FLOOR)) * gain_rows

def gated_product(gate_hidden, up_hidden):
    return jax.nn.gelu(gate_hidden) * up_hidden

def one_sequence(params, seq_inputs, log_rates):
    query_weight, key_weight, value_weight, gate_weight, out_weight, group_gain, norm_gains, norm_biases, ffn_gate_weight, ffn_up_weight, ffn_down_weight = params
    length = seq_inputs.shape[0]
    scale_factor = 1.0 / math.sqrt(HK)
    normed = low(layer_norm(seq_inputs, norm_gains[0], norm_biases[0]))
    query_rows = low(low_back(matmul(normed, query_weight))).reshape(length, MEMORY_CHANNELS, HK)
    every_key = low(low_back(matmul(normed, key_weight))).reshape(length, MEMORY_CHANNELS, HK)
    values_all = low(low_back(matmul(normed, value_weight))).reshape(length, MEMORY_CHANNELS, HV)
    gate_in = low_back(matmul(normed, gate_weight))
    cumul = jnp.cumsum(log_rates, axis=1)
    positions = jnp.arange(length)
    causal = (positions[:, None] >= positions[None, :])[None]
    differ = cumul[:, :, None] - cumul[:, None, :]
    decays = jnp.where(causal, jnp.exp(jnp.where(causal, differ, 0.0)), 0.0)
    retention_scores = low_back(jnp.einsum('jfq,kfq->fjk', query_rows, every_key, precision=HIGH_PRECISION))
    scores_w = low(retention_scores * decays * scale_factor)
    mixed = low_back(jnp.einsum('hlm,mhe->lhe', scores_w, values_all, precision=HIGH_PRECISION))
    group_out = group_norm(mixed, group_gain).reshape(length, MEMORY_CHANNELS * HV)
    gated = low(group_out * jax.nn.silu(gate_in))
    middle = seq_inputs + low_back(matmul(gated, out_weight))
    normed_two = low(layer_norm(middle, norm_gains[1], norm_biases[1]))
    gate_hidden = low_back(matmul(normed_two, ffn_gate_weight))
    up_hidden = low_back(matmul(normed_two, ffn_up_weight))
    hidden = low(gated_product(gate_hidden, up_hidden))
    return middle + low_back(matmul(hidden, ffn_down_weight))

def reference(inputs, cotangent, log_decay, query_weight, key_weight, value_weight, gate_weight, out_weight, group_gain, norm_gains, norm_biases, ffn_gate_weight, ffn_up_weight, ffn_down_weight):
    params = tuple((item.astype(jnp.float32) for item in (query_weight, key_weight, value_weight, gate_weight, out_weight, group_gain, norm_gains, norm_biases, ffn_gate_weight, ffn_up_weight, ffn_down_weight)))
    seqs_in = inputs.astype(jnp.float32).reshape(N_DP, TOKEN_COUNT, D)
    rates = log_decay.astype(jnp.float32).reshape(MEMORY_CHANNELS, N_DP, TOKEN_COUNT).transpose(1, 0, 2)
    checked = jax.checkpoint(one_sequence)

    def forward(stacked_strings, weights):

        def scan_step(carry, pair):
            return (carry, checked(weights, pair[0], pair[1]))
        _, outputs = lax.scan(scan_step, jnp.zeros((), jnp.float32), (stacked_strings, rates))
        return outputs
    outputs, pullback = jax.vjp(forward, seqs_in, params)
    seq_grad, grads = pullback(cotangent.astype(jnp.float32).reshape(N_DP, TOKEN_COUNT, D))
    return (outputs.reshape(TOKENS, D).astype(jnp.bfloat16), seq_grad.reshape(TOKENS, D).astype(jnp.bfloat16), grads[0], grads[1], grads[2], grads[3], grads[4], grads[5], grads[6], grads[7], grads[8], grads[9], grads[10])
```

```python
import functools
import math

import jax
import jax.numpy as jnp
from jax import lax
from jax.sharding import PartitionSpec as P

EPSILON = 1e-05
GROUP_FLOOR = 1.0
BF = jnp.bfloat16
F32 = jnp.float32
PAIR = 2


def layer_norm(values, gain_row, bias_row):
    center = values - jnp.mean(values, axis=-1, keepdims=True)
    spread = jnp.mean(center * center, axis=-1, keepdims=True)
    return center * lax.rsqrt(spread + EPSILON) * gain_row + bias_row


def group_norm(values, gain_rows):
    center = values - jnp.mean(values, axis=-1, keepdims=True)
    spread = jnp.mean(center * center, axis=-1, keepdims=True)
    return center * lax.rsqrt(jnp.maximum(spread, GROUP_FLOOR)) * gain_rows


def gated_product(gate_hidden, up_hidden):
    return jax.nn.gelu(gate_hidden) * up_hidden


def dot_nn(a, b):
    return lax.dot_general(a, b, (((1,), (0,)), ((), ())), preferred_element_type=F32)


def dot_nt(a, b):
    return lax.dot_general(a, b, (((1,), (1,)), ((), ())), preferred_element_type=F32)


def dot_tn(a, b):
    return lax.dot_general(a, b, (((0,), (0,)), ((), ())), preferred_element_type=F32)


def after(value, *others):
    return lax.optimization_barrier((value, *others))[0]


def per_device(
    n_dp,
    n_tensor,
    inputs,
    cotangent,
    log_decay,
    query_weight,
    key_weight,
    value_weight,
    gate_weight,
    out_weight,
    group_gain,
    norm_gains,
    norm_biases,
    ffn_gate_weight,
    ffn_up_weight,
    ffn_down_weight,
):
    d = lax.axis_index("dp")
    t = lax.axis_index("tensor")
    z = (d // PAIR) % 2
    rest = [1 << i for i in range(2, n_dp.bit_length() - 1)] + [1]
    tokens, width = inputs.shape
    block = width // n_dp
    length = tokens * n_tensor
    head_k = query_weight.shape[1] // 2
    head_v = value_weight.shape[1] // 2
    hidden_dev = ffn_gate_weight.shape[1] // 2
    scale_factor = 1.0 / math.sqrt(head_k)

    def swap_dp(value, bit):
        return lax.ppermute(value, "dp", [(i, i ^ bit) for i in range(n_dp)])

    def swap_t(value, bit):
        return lax.ppermute(value, "tensor", [(i, i ^ bit) for i in range(n_tensor)])

    def dp_of(p):
        out = (p & 1) * PAIR
        for k, bit in enumerate(rest):
            out = out + ((d // bit) % 2 ^ ((p >> (k + 1)) & 1)) * bit
        return out

    def position_of(q):
        out = (q // PAIR) & 1
        for k, bit in enumerate(rest):
            out = out + ((d // bit) % 2 ^ ((q // bit) & 1)) * (2 << k)
        return out

    def permuted(value):
        return jnp.concatenate(
            [lax.dynamic_slice_in_dim(value, dp_of(p) * block, block, 1) for p in range(n_dp)], axis=1
        )

    def natural(value):
        return jnp.concatenate(
            [lax.dynamic_slice_in_dim(value, position_of(q) * block, block, 1) for q in range(n_dp)], axis=1
        )

    def half(value, which, axis):
        size = value.shape[axis] // 2
        return lax.dynamic_slice_in_dim(value, which * size, size, axis)

    def ordered(mine, theirs):
        return jnp.where(z == 0, mine, theirs), jnp.where(z == 0, theirs, mine)

    def gather_small(value):
        got = swap_dp(value, PAIR)
        blocks = list(ordered(value, got))
        for bit in rest:
            more = swap_dp(jnp.stack(blocks), bit)
            blocks = blocks + [more[i] for i in range(len(blocks))]
        return blocks

    small = jnp.concatenate([norm_gains, norm_biases, group_gain], axis=1)
    small_blocks = gather_small(small)
    gains_float = jnp.concatenate([b[:, :block] for b in small_blocks], axis=1).astype(F32)
    biases_float = jnp.concatenate([b[:, block : 2 * block] for b in small_blocks], axis=1).astype(F32)
    group_stack = jnp.stack([lax.dynamic_index_in_dim(b[:, 2 * block :], z, 0, False) for b in small_blocks])
    group_float = jnp.concatenate(
        [lax.dynamic_index_in_dim(group_stack, position_of(q), 0, False) for q in range(n_dp)]
    ).astype(F32)[None]

    decay_mine = lax.dynamic_index_in_dim(log_decay, z, 0, True)
    decay_theirs = swap_dp(lax.dynamic_index_in_dim(log_decay, 1 - z, 0, True), PAIR)
    cumul = jnp.cumsum(jnp.concatenate([decay_mine, decay_theirs], axis=0), axis=1)
    chunk_of = [t ^ (((j & 1) << 1) | (j >> 1)) for j in range(n_tensor)]
    cumul = jnp.concatenate([lax.dynamic_slice_in_dim(cumul, c * tokens, tokens, 1) for c in chunk_of], axis=1)
    positions = jnp.concatenate([c * tokens + jnp.arange(tokens) for c in chunk_of])
    causal = (positions[:, None] >= positions[None, :])[None]
    decays = jnp.where(causal, jnp.exp(jnp.where(causal, cumul[:, :, None] - cumul[:, None, :], 0.0)), 0.0)

    def my_half(w, axis):
        return half(w, z, axis), half(w, 1 - z, axis)

    def pack(ws):
        mine, theirs = [], []
        for w in ws:
            a, b = my_half(w, 1)
            mine.append(a)
            theirs.append(b)
        return jnp.concatenate(mine, axis=1), jnp.concatenate(theirs, axis=1)

    groups = [
        pack([query_weight, key_weight, value_weight, gate_weight]),
        pack([out_weight.T]),
        pack([ffn_gate_weight, ffn_up_weight]),
        pack([ffn_down_weight.T]),
    ]
    full = []
    last = [()] * (1 + len(rest))
    for mine, theirs in groups:
        got = swap_dp(after(theirs, *last[0]), PAIR)
        last[0] = (got,)
        blocks = list(ordered(mine, got))
        for k, bit in enumerate(rest):
            more = [swap_dp(after(b, *last[k + 1]), bit) for b in blocks]
            last[k + 1] = (more[-1],)
            blocks = blocks + more
        full.append(jnp.concatenate(blocks, axis=0))
    qkvg_full, out_full, gate_up_full, down_full = full

    def gather_tokens(own):
        zr = swap_dp(own, PAIR)
        yr = swap_t(own, 2)
        zy = swap_t(zr, 2)
        near = [own, yr, zr, zy]
        far = [swap_t(v, 1) for v in near]
        return jnp.concatenate([near[0], near[1], far[0], far[1], near[2], near[3], far[2], far[3]], axis=0)

    def scatter_tokens(part):
        part = part.reshape(2, 2, 2 * tokens, width)
        near = []
        for j in (1, 0):
            got = swap_t(part[j, 1].astype(BF), 1)
            near.insert(0, part[j, 0].astype(F32) + got.astype(F32))
        far_y = near[1][tokens:].astype(BF)
        zr = (near[1][:tokens] + swap_t(far_y, 2).astype(F32)).astype(BF)
        yr = near[0][tokens:].astype(BF)
        return near[0][:tokens] + swap_t(yr, 2).astype(F32) + swap_dp(zr, PAIR).astype(F32)

    inputs_float = permuted(inputs).astype(F32)
    cot = permuted(cotangent)
    normed = layer_norm(inputs_float, gains_float[0], biases_float[0]).astype(BF)
    normed_all = gather_tokens(normed)
    cot_all = gather_tokens(after(cot, normed_all))
    q_end, k_end, v_end = head_k, 2 * head_k, 2 * head_k + head_v
    qkv = dot_nn(normed_all, qkvg_full[:, :v_end]).astype(BF)
    gate_in = dot_nn(normed_all, qkvg_full[:, v_end:])
    queries = qkv[:, :q_end].reshape(2, length, head_k)
    keys = qkv[:, q_end:k_end].reshape(2, length, head_k)
    values = qkv[:, k_end:].reshape(2, length, head_v)
    scores = jnp.einsum("ztk,zsk->zts", queries, keys, preferred_element_type=F32)
    scores_w = (scores * decays * scale_factor).astype(BF)
    mixed = jnp.einsum("zts,zse->zte", scores_w, values, preferred_element_type=F32).reshape(2 * length, head_v)
    flat_norm = group_norm(mixed, group_float)
    silu_gate = jax.nn.silu(gate_in)
    gated = (flat_norm * silu_gate).astype(BF)
    middle = inputs_float + scatter_tokens(dot_nt(gated, out_full).astype(BF))
    normed_two = layer_norm(middle, gains_float[1], biases_float[1]).astype(BF)
    ffn_in = gather_tokens(normed_two)
    gate_hidden = dot_nn(ffn_in, gate_up_full[:, :hidden_dev])
    up_hidden = dot_nn(ffn_in, gate_up_full[:, hidden_dev:])
    hidden = gated_product(gate_hidden, up_hidden).astype(BF)

    def reduce_rows(left, right, previous):
        count = width // 2
        send = dot_tn(left[:, count:], right).astype(BF)
        keep = dot_tn(left[:, :count], right)
        for k, bit in enumerate(reversed(rest)):
            got = swap_dp(after(send, *previous), bit)
            keep = keep + got.astype(F32)
            count //= 2
            if k + 1 < len(rest):
                send, keep = keep[count:].astype(BF), keep[:count]
        send = half(keep, 1 - z, 0).astype(BF)
        got = swap_dp(send, PAIR)
        return half(keep, z, 0), got.astype(F32)

    def both(mine, theirs, axis):
        first, second = ordered(mine, theirs)
        return jnp.concatenate([first, second], axis=axis)

    grad_hidden = dot_nn(cot_all, down_full)
    unused, pull_gelu = jax.vjp(gated_product, gate_hidden, up_hidden)
    grad_gate_hidden, grad_up_hidden = pull_gelu(grad_hidden)
    grad_gate_up = jnp.concatenate([grad_gate_hidden.astype(BF), grad_up_hidden.astype(BF)], axis=1)
    grad_normed_two = scatter_tokens(dot_nt(grad_gate_up, gate_up_full).astype(BF))
    down_mine, down_theirs = reduce_rows(cot_all, hidden, ())
    gu_mine, gu_theirs = reduce_rows(ffn_in, grad_gate_up, ())
    ffn_out = scatter_tokens(dot_nt(hidden, down_full).astype(BF))
    layer_out = natural((middle + ffn_out).astype(BF))
    unused, pull_second = jax.vjp(layer_norm, middle, gains_float[1], biases_float[1])
    grad_mid_norm, grad_gain_two, grad_bias_two = pull_second(grad_normed_two)
    grad_middle = cot.astype(F32) + grad_mid_norm
    branch_all = gather_tokens(grad_middle.astype(BF))

    grad_gated = dot_nn(branch_all, out_full)
    out_mine, out_theirs = reduce_rows(branch_all, gated, ())
    unused, pull_silu = jax.vjp(jax.nn.silu, gate_in)
    (grad_gate_in,) = pull_silu(grad_gated * flat_norm)
    grad_gate_in = grad_gate_in.astype(BF)
    unused, pull_group = jax.vjp(group_norm, mixed, group_float)
    grad_mixed, group_gain_grad = pull_group(grad_gated * silu_gate)
    grad_mixed = grad_mixed.astype(BF).reshape(2, length, head_v)
    grad_weights = jnp.einsum("zte,zse->zts", grad_mixed, values, preferred_element_type=F32)
    score_gradient = (grad_weights * decays * scale_factor).astype(BF)
    grad_values = jnp.einsum("zts,zte->zse", scores_w, grad_mixed, preferred_element_type=F32)
    grad_queries = jnp.einsum("zts,zsk->ztk", score_gradient, keys, preferred_element_type=F32)
    grad_keys = jnp.einsum("zts,ztk->zsk", score_gradient, queries, preferred_element_type=F32)
    grad_qkvg = jnp.concatenate(
        [
            grad_queries.astype(BF).reshape(2 * length, head_k),
            grad_keys.astype(BF).reshape(2 * length, head_k),
            grad_values.astype(BF).reshape(2 * length, head_v),
            grad_gate_in,
        ],
        axis=1,
    )
    qkvg_mine, qkvg_theirs = reduce_rows(normed_all, grad_qkvg, ())
    grad_normed = scatter_tokens(dot_nt(grad_qkvg, qkvg_full).astype(BF))
    unused, pull_first = jax.vjp(layer_norm, inputs_float, gains_float[0], biases_float[0])
    grad_in_norm, grad_gain_one, grad_bias_one = pull_first(grad_normed)
    input_grad = natural((grad_middle + grad_in_norm).astype(BF))

    norm_rows = natural(jnp.stack([grad_gain_one, grad_gain_two, grad_bias_one, grad_bias_two], axis=0))
    zero = jnp.zeros_like(group_gain_grad)
    group_rows = both(group_gain_grad, zero, 0)
    group_flat = group_rows.reshape(1, -1)
    sums = jnp.concatenate([norm_rows.reshape(1, -1), group_flat], axis=1).reshape(-1, 128)
    for bit in [PAIR] + rest:
        sums = sums + swap_dp(sums, bit)
    sums = sums.reshape(-1)
    norm_sums, group_sums = sums[: 4 * width], sums[4 * width :].reshape(2, head_v)
    norm_sums = norm_sums.reshape(-1, 128)
    for bit in (1, 2):
        norm_sums = norm_sums + swap_t(norm_sums, bit)
    cols = width // (n_dp * n_tensor)
    norm_mine = lax.dynamic_slice_in_dim(norm_sums.reshape(4, width), (d * n_tensor + t) * cols, cols, 1)
    norm_gain_grad, norm_bias_grad = norm_mine[:2], norm_mine[2:]
    group_cols = head_v // n_dp
    group_gain_out = lax.dynamic_slice_in_dim(group_sums, d * group_cols, group_cols, 1)

    def split(value, sizes):
        out, start = [], 0
        for size in sizes:
            out.append(value[:, start : start + size])
            start += size
        return out

    sizes = (head_k, head_k, head_v, head_v)
    query_grad, key_grad, value_grad, gate_grad = (
        both(a, b, 1) for a, b in zip(split(qkvg_mine, sizes), split(qkvg_theirs, sizes), strict=True)
    )
    sizes = (hidden_dev, hidden_dev)
    ffn_gate_grad, ffn_up_grad = (
        both(a, b, 1) for a, b in zip(split(gu_mine, sizes), split(gu_theirs, sizes), strict=True)
    )
    ffn_down_grad = both(down_mine, down_theirs, 1).T
    out_weight_grad = both(out_mine, out_theirs, 1).T
    return (
        layer_out,
        input_grad,
        query_grad,
        key_grad,
        value_grad,
        gate_grad,
        out_weight_grad,
        group_gain_out,
        norm_gain_grad,
        norm_bias_grad,
        ffn_gate_grad,
        ffn_up_grad,
        ffn_down_grad,
    )


def solution(mesh):
    tokens = P(("dp", "tensor"), None)
    rows, cols, norms = P("dp", "tensor"), P("tensor", "dp"), P(None, "dp")
    sums = P(None, ("dp", "tensor"))
    in_specs = (tokens, tokens, cols, rows, rows, rows, rows, cols, cols, norms, norms, rows, rows, cols)
    out_specs = (tokens, tokens, rows, rows, rows, rows, cols, cols, sums, sums, rows, rows, cols)
    body = functools.partial(per_device, mesh.shape["dp"], mesh.shape["tensor"])
    return jax.shard_map(body, mesh=mesh, in_specs=in_specs, out_specs=out_specs, check_vma=False)
```

```python
import functools
import math

import jax
import jax.numpy as jnp
from jax import lax
from jax.experimental import pallas as pl
from jax.experimental.pallas import tpu as pltpu
from jax.sharding import PartitionSpec as P

EPSILON = 1e-05
GROUP_FLOOR = 1.0
BF = jnp.bfloat16
F32 = jnp.float32
PAIR = 2
MESH = pl.DeviceIdType.MESH
QK, V, G, O, FG, FU, FD = range(7)
GROUPS = 7


def dot_nn(a, b):
    return lax.dot_general(a, b, (((1,), (0,)), ((), ())), preferred_element_type=F32)


def dot_nt(a, b):
    return lax.dot_general(a, b, (((1,), (1,)), ((), ())), preferred_element_type=F32)


def dot_tn(a, b):
    return lax.dot_general(a, b, (((0,), (0,)), ((), ())), preferred_element_type=F32)


def flip(index, bit):
    return index + bit - 2 * bit * ((index // bit) % 2)


class Place:
    def __init__(self, n_dp):
        self.n_dp = n_dp
        self.d = lax.axis_index("dp")
        self.t = lax.axis_index("tensor")
        self.z = (self.d // PAIR) % 2
        self.rest = [1 << i for i in range(2, n_dp.bit_length() - 1)] + [1]
        self.inner = self.rest[:-1]
        self.masks = []
        for pick in range(1, 1 << (1 + len(self.inner))):
            bits = [PAIR] * (pick & 1) + [b for k, b in enumerate(self.inner) if (pick >> (k + 1)) & 1]
            self.masks.append((bits, pick & ~1, pick & 1))

    def peer(self, bits):
        out = self.d
        for bit in bits:
            out = flip(out, bit)
        return {"dp": out}

    def x_peer(self):
        return {"dp": flip(self.d, 1)}

    def z_peer(self):
        return {"dp": flip(self.d, PAIR)}

    def y_peer(self):
        return {"tensor": flip(self.t, 2)}

    def c_peer(self):
        return {"tensor": flip(self.t, 1)}

    def everyone(self):
        return [self.peer(bits) for bits, _, _ in self.masks] + [self.x_peer(), self.y_peer(), self.c_peer()]


def entry_barrier(place):
    barrier = pltpu.get_barrier_semaphore()
    peers = place.everyone()
    for peer in peers:
        pl.semaphore_signal(barrier, inc=1, device_id=peer, device_id_type=MESH)
    pl.semaphore_wait(barrier, len(peers))


def remote(src, dst, send, recv, peer):
    return pltpu.make_async_remote_copy(
        src_ref=src, dst_ref=dst, send_sem=send, recv_sem=recv, device_id=peer, device_id_type=MESH
    )


class Weights:
    def __init__(self, place, sources, full, sems):
        self.place, self.sources, self.full = place, sources, full
        self.z_send, self.z_recv, self.x_send, self.x_recv, self.local = sems
        self.block = sources[0].shape[0]
        self.cols = sources[0].shape[1] // 2
        self.half = place.n_dp // 2

    def rows(self, position, count=1):
        return pl.ds(pl.multiple_of(position * self.block, self.block), count * self.block)

    def source(self, g, half):
        return self.sources[g].at[:, pl.ds(pl.multiple_of(half * self.cols, self.cols), self.cols)]

    def start(self, g):
        place = self.place
        z = place.z
        own = pltpu.make_async_copy(self.source(g, z), self.full.at[g, self.rows(z), :], self.local.at[g])
        own.start()
        for i, (bits, above, flips) in enumerate(place.masks):
            half = 1 - z if flips else z
            remote(
                self.source(g, half),
                self.full.at[g, self.rows(z + above), :],
                self.z_send.at[g],
                self.z_recv.at[g, i],
                place.peer(bits),
            ).start()
        remote(
            self.source(g, z),
            self.full.at[g, self.rows(z + self.half), :],
            self.x_send.at[g],
            self.x_recv.at[g],
            place.x_peer(),
        ).start()

    def forward(self, g, i):
        place = self.place
        bits, above, flips = place.masks[i]
        position = (1 - place.z if flips else place.z) + above
        here = self.full.at[g, self.rows(position), :]
        remote(here, here, self.z_send.at[g], self.z_recv.at[g, i], place.peer(bits)).wait_recv()
        remote(
            here,
            self.full.at[g, self.rows(position + self.half), :],
            self.x_send.at[g],
            self.x_recv.at[g],
            place.x_peer(),
        ).start()

    def forward_all(self, g):
        for i in range(len(self.place.masks)):
            self.forward(g, i)

    def finish(self, g):
        z = self.place.z
        pltpu.make_async_copy(self.source(g, z), self.full.at[g, self.rows(z), :], self.local.at[g]).wait()
        there = self.full.at[g, self.rows(self.half, self.half), :]
        remote(there, there, self.x_send.at[g], self.x_recv.at[g], self.place.x_peer()).wait_recv()

    def sent(self, g):
        there = self.full.at[g, self.rows(self.half, self.half), :]
        remote(there, there, self.x_send.at[g], self.x_recv.at[g], self.place.x_peer()).wait_send()
        count = self.half - 1
        those = self.full.at[g, self.rows(0, count), :]
        remote(those, those, self.z_send.at[g], self.z_recv.at[g, 0], self.place.x_peer()).wait_send()


class Gather:
    def __init__(self, place, buffer, send, recv):
        self.place, self.buffer = place, buffer
        self.send, self.recv = send, recv
        self.tokens = buffer.shape[0] // 8
        self.peers = {1: place.c_peer(), 2: place.y_peer(), 4: place.z_peer()}

    def slot(self, s):
        return self.buffer.at[pl.ds(s * self.tokens, self.tokens), :]

    def copy(self, source, bit, src=None):
        s = source + bit
        return remote(self.slot(source) if src is None else src, self.slot(s), self.send.at[s - 1], self.recv.at[s - 1], self.peers[bit])

    def start(self, src=None):
        for bit in (4, 2, 1):
            self.copy(0, bit, src).start()

    def from_z(self):
        self.copy(0, 4).wait_recv()
        self.copy(4, 2).start()
        self.copy(4, 1).start()

    def from_y(self):
        self.copy(0, 2).wait_recv()
        self.copy(2, 1).start()

    def from_zy(self):
        self.copy(4, 2).wait_recv()
        self.copy(6, 1).start()

    def chip(self, source):
        self.copy(source, 1).wait_recv()

    def sent(self, src=None):
        self.copy(0, 4, src).wait_send()
        self.copy(0, 2, src).wait_send()
        self.copy(0, 1, src).wait_send()
        self.copy(4, 2).wait_send()
        self.copy(4, 1).wait_send()
        self.copy(2, 1).wait_send()
        self.copy(6, 1).wait_send()


class Scatter:
    def __init__(self, place, keep, c_out, c_in, far_out, far_in, sems):
        self.place = place
        self.keep, self.c_out, self.c_in, self.far_out, self.far_in = keep, c_out, c_in, far_out, far_in
        self.c_send, self.c_recv, self.far_send, self.far_recv = sems
        self.tokens = c_out.shape[1]

    def part(self, b, value):
        self.keep[b] = value[: self.tokens]
        self.c_out[b] = value[self.tokens :].astype(BF)
        self.c_copy(b).start()

    def c_copy(self, b):
        return remote(self.c_out.at[b], self.c_in.at[b], self.c_send.at[b], self.c_recv.at[b], self.place.c_peer())

    def far_copy(self, b):
        peer = self.place.z_peer() if b == 2 else self.place.y_peer()
        return remote(
            self.far_out.at[b - 1], self.far_in.at[b - 1], self.far_send.at[b - 1], self.far_recv.at[b - 1], peer
        )

    def rows(self, body, step=16):
        def loop(i, carry):
            body(pl.ds(pl.multiple_of(i * step, step), step))
            return carry

        lax.fori_loop(0, self.tokens // step, loop, 0)

    def pass_on(self, b):
        self.c_copy(b).wait_recv()
        if b == 2:
            self.far_copy(3).wait_recv()

        def body(r):
            total = self.keep[b, r, :] + self.c_in[b, r, :].astype(F32)
            if b == 2:
                total = total + self.far_in[2, r, :].astype(F32)
            self.far_out[b - 1, r, :] = total.astype(BF)

        self.rows(body)
        self.far_copy(b).start()

    def wait_own(self):
        self.c_copy(0).wait_recv()
        self.far_copy(1).wait_recv()
        self.far_copy(2).wait_recv()

    def own(self, r):
        return (
            self.keep[0, r, :]
            + self.c_in[0, r, :].astype(F32)
            + self.far_in[0, r, :].astype(F32)
            + self.far_in[1, r, :].astype(F32)
        )

    def sent(self):
        for b in range(4):
            self.c_copy(b).wait_send()
        for b in (3, 2, 1):
            self.far_copy(b).wait_send()


def normalized(value):
    center = value - jnp.mean(value, axis=-1, keepdims=True)
    spread = jnp.mean(center * center, axis=-1, keepdims=True)
    return center * lax.rsqrt(spread + EPSILON)


def decay_tile(t, cumul_rows, cumul_cols, first, rows, length, tokens):
    index = lax.broadcasted_iota(jnp.int32, (rows, length), 0) + first
    other = lax.broadcasted_iota(jnp.int32, (rows, length), 1)
    at = ((index // tokens) ^ t) * tokens + index % tokens
    to = ((other // tokens) ^ t) * tokens + other % tokens
    causal = at >= to
    return jnp.where(causal, jnp.exp(jnp.where(causal, cumul_cols - cumul_rows, 0.0)), 0.0)


def forward_kernel(
    n_dp,
    x_ref,
    cot_ref,
    params_ref,
    group_ref,
    cum_row_ref,
    cum_col_ref,
    s_qk,
    s_v,
    s_g,
    s_o,
    s_fg,
    s_fu,
    s_fd,
    w_out,
    normed_out,
    qkv_out,
    gate_out,
    mixed_out,
    ffn_in_out,
    hidden_out,
    grads_out,
    cot_out,
    middle_out,
    w,
    normed_all,
    cot_all,
    ffn_in,
    qkv,
    gate_in,
    mixed,
    gated,
    gate_hidden,
    up_hidden,
    hidden,
    grads,
    middle,
    keep,
    c_out,
    c_in,
    far_out,
    far_in,
    z_send,
    z_recv,
    x_send,
    x_recv,
    w_local,
    ag_send,
    ag_recv,
    c_send,
    c_recv,
    far_send,
    far_recv,
    out_sem,
):
    place = Place(n_dp)
    tokens, width = x_ref.shape
    rows_all = 8 * tokens
    length = rows_all // 2
    head_k = qkv.shape[1] // 4
    scale = 1.0 / math.sqrt(head_k)
    tile = 2 * tokens
    weights = Weights(place, [s_qk, s_v, s_g, s_o, s_fg, s_fu, s_fd], w, (z_send, z_recv, x_send, x_recv, w_local))
    ag_normed = Gather(place, normed_all, ag_send.at[0], ag_recv.at[0])
    ag_cot = Gather(place, cot_all, ag_send.at[1], ag_recv.at[1])
    ag_two = Gather(place, ffn_in, ag_send.at[2], ag_recv.at[2])
    branch = Scatter(place, keep, c_out, c_in, far_out, far_in, (c_send, c_recv, far_send, far_recv))
    outs = []

    def save(src, dst, index):
        copy = pltpu.make_async_copy(src, dst, out_sem.at[index])
        copy.start()
        outs.append(copy)

    def over(count, step, body):
        def loop(i, carry):
            body(pl.ds(pl.multiple_of(i * step, step), step), i)
            return carry

        lax.fori_loop(0, count // step, loop, 0)

    entry_barrier(place)
    cot_own = pltpu.make_async_copy(cot_ref, ag_cot.slot(0), out_sem.at[17])
    cot_own.start()
    weights.start(QK)

    def first_norm(r, i):
        value = normalized(x_ref[r, :].astype(F32))
        normed_all[r, :] = (value * params_ref[0:1, :] + params_ref[2:3, :]).astype(BF)

    over(tokens, 16, first_norm)
    ag_normed.start()
    weights.start(V)
    weights.forward(QK, 0)
    ag_normed.from_z()
    ag_normed.from_y()
    for i in range(1, len(place.masks)):
        weights.forward(QK, i)
    weights.start(G)
    ag_normed.from_zy()
    ag_cot.start(cot_ref)
    weights.forward(V, 0)
    for s in (0, 2, 4, 6):
        ag_normed.chip(s)
    save(normed_all, normed_out, 0)
    weights.finish(QK)

    def make_qk(r, i):
        qkv[r, : 2 * head_k] = dot_nn(normed_all[r, :], w[QK]).astype(BF)

    over(rows_all, tile, make_qk)
    save(w.at[QK], w_out.at[QK], 1)
    for i in range(1, len(place.masks)):
        weights.forward(V, i)
    weights.start(O)
    ag_cot.from_z()
    ag_cot.from_y()
    weights.forward(G, 0)
    weights.finish(V)

    def make_v(r, i):
        qkv[r, 2 * head_k :] = dot_nn(normed_all[r, :], w[V]).astype(BF)

    over(rows_all, tile, make_v)
    save(w.at[V], w_out.at[V], 2)
    save(qkv, qkv_out, 3)
    for i in range(1, len(place.masks)):
        weights.forward(G, i)
    weights.start(FG)

    def retention(r, i):
        start = pl.multiple_of((i // 2) * length, length)
        seq = pl.ds(start, length)
        scores = dot_nt(qkv[r, :head_k], qkv[seq, head_k : 2 * head_k])
        decays = decay_tile(
            place.t, cum_row_ref[pl.ds(i // 2, 1), :], cum_col_ref[r, :], (i % 2) * tile, tile, length, tokens
        )
        weighted = (scores * decays * scale).astype(BF)
        mixed[r, :] = dot_nn(weighted, qkv[seq, 2 * head_k :])

    over(rows_all, tile, retention)
    save(mixed, mixed_out, 4)
    ag_cot.from_zy()
    weights.forward(O, 0)
    weights.finish(G)

    def gating(r, i):
        gate = dot_nn(normed_all[r, :], w[G])
        gate_in[r, :] = gate
        value = mixed[r, :]
        center = value - jnp.mean(value, axis=-1, keepdims=True)
        spread = jnp.mean(center * center, axis=-1, keepdims=True)
        flat = center * lax.rsqrt(jnp.maximum(spread, GROUP_FLOOR)) * group_ref[...]
        gated[r, :] = (flat * (gate * lax.logistic(gate))).astype(BF)

    over(rows_all, tile, gating)
    save(w.at[G], w_out.at[G], 5)
    save(gate_in, gate_out, 6)
    for i in range(1, len(place.masks)):
        weights.forward(O, i)
    weights.start(FU)
    for s in (0, 2, 4, 6):
        ag_cot.chip(s)
    weights.forward(FG, 0)
    weights.finish(O)
    for b in (3, 2, 1, 0):
        branch.part(b, dot_nt(gated[b * tile : (b + 1) * tile, :], w[O]))
    save(w.at[O], w_out.at[O], 7)
    branch.pass_on(3)
    branch.pass_on(1)
    for i in range(1, len(place.masks)):
        weights.forward(FG, i)
    branch.pass_on(2)
    cot_own.wait()
    save(cot_all, cot_out, 8)
    weights.forward(FU, 0)
    branch.wait_own()

    def second_norm(r, i):
        value = x_ref[r, :].astype(F32) + branch.own(r)
        middle[r, :] = value
        ffn_in[r, :] = (normalized(value) * params_ref[1:2, :] + params_ref[3:4, :]).astype(BF)

    over(tokens, 16, second_norm)
    ag_two.start()
    weights.start(FD)
    save(middle, middle_out, 9)
    for i in range(1, len(place.masks)):
        weights.forward(FU, i)
    weights.finish(FG)
    weights.finish(FU)

    def feed(b):
        r = pl.ds(b * tile, tile)
        gate = dot_nn(ffn_in[r, :], w[FG])
        up = dot_nn(ffn_in[r, :], w[FU])
        gate_hidden[r, :] = gate
        up_hidden[r, :] = up
        hidden[r, :] = (gelu(gate) * up).astype(BF)

    ag_two.chip(0)
    feed(0)
    ag_two.from_z()
    ag_two.from_y()
    ag_two.chip(2)
    feed(1)
    ag_two.chip(4)
    feed(2)
    weights.forward(FD, 0)
    ag_two.from_zy()
    ag_two.chip(6)
    feed(3)
    save(w.at[FG], w_out.at[FG], 10)
    save(w.at[FU], w_out.at[FU], 11)
    save(ffn_in, ffn_in_out, 12)
    save(hidden, hidden_out, 13)
    for i in range(1, len(place.masks)):
        weights.forward(FD, i)
    weights.finish(FD)
    save(w.at[FD], w_out.at[FD], 14)
    size = gate_hidden.shape[1]

    def feed_back(r, i):
        back = dot_nn(cot_all[r, :], w[FD])
        gate = gate_hidden[r, :]
        value, slope = gelu_and_slope(gate)
        grads[r, :size] = (back * up_hidden[r, :] * slope).astype(BF)
        grads[r, size:] = (back * value).astype(BF)

    over(rows_all, tile, feed_back)
    save(grads, grads_out, 15)
    for copy in outs:
        copy.wait()
    for g in range(GROUPS):
        weights.sent(g)
    ag_normed.sent()
    ag_cot.sent(cot_ref)
    ag_two.sent()
    branch.sent()


ROOT = math.sqrt(2.0 / math.pi)


def gelu(v):
    return 0.5 * v * (1.0 + jnp.tanh(ROOT * (v + 0.044715 * v * v * v)))


def gelu_and_slope(v):
    inside = jnp.tanh(ROOT * (v + 0.044715 * v * v * v))
    slope = 0.5 * (1.0 + inside) + 0.5 * v * (1.0 - inside * inside) * ROOT * (1.0 + 3 * 0.044715 * v * v)
    return 0.5 * v * (1.0 + inside), slope


def forward_call(n_dp, x, cot, params, group, cum_row, cum_col, sources):
    tokens, width = x.shape
    rows_all = 8 * tokens
    cols = sources[0].shape[1] // 2
    masks = n_dp // 2 - 1
    vmem, hbm = pl.BlockSpec(memory_space=pltpu.VMEM), pl.BlockSpec(memory_space=pl.ANY)
    shape = jax.ShapeDtypeStruct
    outs = (
        shape((GROUPS, width, cols), BF),
        shape((rows_all, width), BF),
        shape((rows_all, 2 * cols), BF),
        shape((rows_all, cols), F32),
        shape((rows_all, cols), F32),
        shape((rows_all, width), BF),
        shape((rows_all, cols), BF),
        shape((rows_all, 2 * cols), BF),
        shape((rows_all, width), BF),
        shape((tokens, width), F32),
    )
    dma = pltpu.SemaphoreType.DMA
    scratch = [
        pltpu.VMEM((GROUPS, width, cols), BF),
        pltpu.VMEM((rows_all, width), BF),
        pltpu.VMEM((rows_all, width), BF),
        pltpu.VMEM((rows_all, width), BF),
        pltpu.VMEM((rows_all, 2 * cols), BF),
        pltpu.VMEM((rows_all, cols), F32),
        pltpu.VMEM((rows_all, cols), F32),
        pltpu.VMEM((rows_all, cols), BF),
        pltpu.VMEM((rows_all, cols), F32),
        pltpu.VMEM((rows_all, cols), F32),
        pltpu.VMEM((rows_all, cols), BF),
        pltpu.VMEM((rows_all, 2 * cols), BF),
        pltpu.VMEM((tokens, width), F32),
        pltpu.VMEM((4, tokens, width), F32),
        pltpu.VMEM((4, tokens, width), BF),
        pltpu.VMEM((4, tokens, width), BF),
        pltpu.VMEM((3, tokens, width), BF),
        pltpu.VMEM((3, tokens, width), BF),
        dma((GROUPS,)),
        dma((GROUPS, masks)),
        dma((GROUPS,)),
        dma((GROUPS,)),
        dma((GROUPS,)),
        dma((3, 7)),
        dma((3, 7)),
        dma((4,)),
        dma((4,)),
        dma((3,)),
        dma((3,)),
        dma((18,)),
    ]
    return pl.pallas_call(
        functools.partial(forward_kernel, n_dp),
        out_shape=outs,
        in_specs=[vmem, hbm, vmem, vmem, vmem, vmem] + [hbm] * GROUPS,
        out_specs=(hbm,) * len(outs),
        scratch_shapes=scratch,
        compiler_params=pltpu.CompilerParams(
            collective_id=1, has_side_effects=True, vmem_limit_bytes=64_000_000
        ),
    )(x, cot, params, group, cum_row, cum_col, *sources)


def layer_norm(values, gain_row, bias_row):
    center = values - jnp.mean(values, axis=-1, keepdims=True)
    spread = jnp.mean(center * center, axis=-1, keepdims=True)
    return center * lax.rsqrt(spread + EPSILON) * gain_row + bias_row


def group_norm(values, gain_rows):
    center = values - jnp.mean(values, axis=-1, keepdims=True)
    spread = jnp.mean(center * center, axis=-1, keepdims=True)
    return center * lax.rsqrt(jnp.maximum(spread, GROUP_FLOOR)) * gain_rows


def gated_product(gate_hidden, up_hidden):
    return jax.nn.gelu(gate_hidden) * up_hidden


def after(value, *others):
    return lax.optimization_barrier((value, *others))[0]


def per_device(
    n_dp,
    n_tensor,
    inputs,
    cotangent,
    log_decay,
    query_weight,
    key_weight,
    value_weight,
    gate_weight,
    out_weight,
    group_gain,
    norm_gains,
    norm_biases,
    ffn_gate_weight,
    ffn_up_weight,
    ffn_down_weight,
):
    d = lax.axis_index("dp")
    t = lax.axis_index("tensor")
    z = (d // PAIR) % 2
    rest = [1 << i for i in range(2, n_dp.bit_length() - 1)] + [1]
    tokens, width = inputs.shape
    block = width // n_dp
    length = tokens * n_tensor
    head_k = query_weight.shape[1] // 2
    head_v = value_weight.shape[1] // 2
    hidden_dev = ffn_gate_weight.shape[1] // 2
    scale_factor = 1.0 / math.sqrt(head_k)

    def swap_dp(value, bit):
        return lax.ppermute(value, "dp", [(i, i ^ bit) for i in range(n_dp)])

    def swap_t(value, bit):
        return lax.ppermute(value, "tensor", [(i, i ^ bit) for i in range(n_tensor)])

    def dp_of(p):
        out = (p & 1) * PAIR
        for k, bit in enumerate(rest):
            out = out + ((d // bit) % 2 ^ ((p >> (k + 1)) & 1)) * bit
        return out

    def position_of(q):
        out = (q // PAIR) & 1
        for k, bit in enumerate(rest):
            out = out + ((d // bit) % 2 ^ ((q // bit) & 1)) * (2 << k)
        return out

    def permuted(value):
        return jnp.concatenate(
            [lax.dynamic_slice_in_dim(value, dp_of(p) * block, block, 1) for p in range(n_dp)], axis=1
        )

    def natural(value):
        return jnp.concatenate(
            [lax.dynamic_slice_in_dim(value, position_of(q) * block, block, 1) for q in range(n_dp)], axis=1
        )

    def half(value, which, axis):
        size = value.shape[axis] // 2
        return lax.dynamic_slice_in_dim(value, which * size, size, axis)

    def ordered(mine, theirs):
        return jnp.where(z == 0, mine, theirs), jnp.where(z == 0, theirs, mine)

    def gather_small(value):
        got = swap_dp(value, PAIR)
        blocks = list(ordered(value, got))
        for bit in rest:
            more = swap_dp(jnp.stack(blocks), bit)
            blocks = blocks + [more[i] for i in range(len(blocks))]
        return blocks

    small = jnp.concatenate([norm_gains, norm_biases, group_gain], axis=1)
    small_blocks = gather_small(small)
    gains_float = jnp.concatenate([b[:, :block] for b in small_blocks], axis=1).astype(F32)
    biases_float = jnp.concatenate([b[:, block : 2 * block] for b in small_blocks], axis=1).astype(F32)
    group_stack = jnp.stack([lax.dynamic_index_in_dim(b[:, 2 * block :], z, 0, False) for b in small_blocks])
    group_float = jnp.concatenate(
        [lax.dynamic_index_in_dim(group_stack, position_of(q), 0, False) for q in range(n_dp)]
    ).astype(F32)[None]

    decay_mine = lax.dynamic_index_in_dim(log_decay, z, 0, True)
    decay_theirs = swap_dp(lax.dynamic_index_in_dim(log_decay, 1 - z, 0, True), PAIR)
    cumul = jnp.cumsum(jnp.concatenate([decay_mine, decay_theirs], axis=0), axis=1)
    chunk_of = [t ^ j for j in range(n_tensor)]
    cumul = jnp.concatenate([lax.dynamic_slice_in_dim(cumul, c * tokens, tokens, 1) for c in chunk_of], axis=1)
    positions = jnp.concatenate([c * tokens + jnp.arange(tokens) for c in chunk_of])
    causal = (positions[:, None] >= positions[None, :])[None]
    decays = jnp.where(causal, jnp.exp(jnp.where(causal, cumul[:, :, None] - cumul[:, None, :], 0.0)), 0.0)

    def interleaved(first, second):
        parts = [half(first, 0, 1), half(second, 0, 1), half(first, 1, 1), half(second, 1, 1)]
        return jnp.concatenate(parts, axis=1)

    sources = [
        interleaved(query_weight, key_weight),
        value_weight,
        gate_weight,
        out_weight.T,
        ffn_gate_weight,
        ffn_up_weight,
        ffn_down_weight.T,
    ]

    def gather_tokens(own):
        zr = swap_dp(own, PAIR)
        yr = swap_t(own, 2)
        zy = swap_t(zr, 2)
        near = [own, yr, zr, zy]
        return jnp.concatenate([v for a in near for v in (a, swap_t(a, 1))], axis=0)

    def scatter_tokens(part):
        part = part.reshape(4, 2, tokens, width)
        near = [part[b, 0].astype(F32) + swap_t(part[b, 1].astype(BF), 1).astype(F32) for b in range(4)]
        zr = (near[2] + swap_t(near[3].astype(BF), 2).astype(F32)).astype(BF)
        return near[0] + swap_t(near[1].astype(BF), 2).astype(F32) + swap_dp(zr, PAIR).astype(F32)

    inputs_perm, cot = permuted(inputs), permuted(cotangent)
    inputs_float = inputs_perm.astype(F32)
    params = jnp.concatenate([gains_float, biases_float], axis=0)
    full, normed_all, qkv, gate_in, mixed, ffn_in, hidden, grad_gate_up, cot_all, middle = forward_call(
        n_dp, inputs_perm, cot, params, group_float, cumul, cumul.reshape(-1, 1), sources
    )
    qkvg_full = jnp.concatenate([full[QK], full[V], full[G]], axis=1)
    out_full, down_full = full[O], full[FD]
    gate_up_full = jnp.concatenate([full[FG], full[FU]], axis=1)
    q_end, k_end = head_k, 2 * head_k
    queries = qkv[:, :q_end].reshape(2, length, head_k)
    keys = qkv[:, q_end:k_end].reshape(2, length, head_k)
    values = qkv[:, k_end:].reshape(2, length, head_v)
    scores = jnp.einsum("ztk,zsk->zts", queries, keys, preferred_element_type=F32)
    scores_w = (scores * decays * scale_factor).astype(BF)
    flat_norm = group_norm(mixed, group_float)
    silu_gate = jax.nn.silu(gate_in)
    gated = (flat_norm * silu_gate).astype(BF)

    def reduce_rows(left, right, previous):
        count = width // 2
        send = dot_tn(left[:, count:], right).astype(BF)
        keep = dot_tn(left[:, :count], right)
        for k, bit in enumerate(reversed(rest)):
            got = swap_dp(after(send, *previous), bit)
            keep = keep + got.astype(F32)
            count //= 2
            if k + 1 < len(rest):
                send, keep = keep[count:].astype(BF), keep[:count]
        send = half(keep, 1 - z, 0).astype(BF)
        got = swap_dp(send, PAIR)
        return half(keep, z, 0), got.astype(F32)

    def both(mine, theirs, axis):
        first, second = ordered(mine, theirs)
        return jnp.concatenate([first, second], axis=axis)

    grad_normed_two = scatter_tokens(dot_nt(grad_gate_up, gate_up_full).astype(BF))
    down_mine, down_theirs = reduce_rows(cot_all, hidden, ())
    gu_mine, gu_theirs = reduce_rows(ffn_in, grad_gate_up, ())
    ffn_out = scatter_tokens(dot_nt(hidden, down_full).astype(BF))
    layer_out = natural((middle + ffn_out).astype(BF))
    unused, pull_second = jax.vjp(layer_norm, middle, gains_float[1], biases_float[1])
    grad_mid_norm, grad_gain_two, grad_bias_two = pull_second(grad_normed_two)
    grad_middle = cot.astype(F32) + grad_mid_norm
    branch_all = gather_tokens(grad_middle.astype(BF))

    grad_gated = dot_nn(branch_all, out_full)
    out_mine, out_theirs = reduce_rows(branch_all, gated, ())
    unused, pull_silu = jax.vjp(jax.nn.silu, gate_in)
    (grad_gate_in,) = pull_silu(grad_gated * flat_norm)
    grad_gate_in = grad_gate_in.astype(BF)
    unused, pull_group = jax.vjp(group_norm, mixed, group_float)
    grad_mixed, group_gain_grad = pull_group(grad_gated * silu_gate)
    grad_mixed = grad_mixed.astype(BF).reshape(2, length, head_v)
    grad_weights = jnp.einsum("zte,zse->zts", grad_mixed, values, preferred_element_type=F32)
    score_gradient = (grad_weights * decays * scale_factor).astype(BF)
    grad_values = jnp.einsum("zts,zte->zse", scores_w, grad_mixed, preferred_element_type=F32)
    grad_queries = jnp.einsum("zts,zsk->ztk", score_gradient, keys, preferred_element_type=F32)
    grad_keys = jnp.einsum("zts,ztk->zsk", score_gradient, queries, preferred_element_type=F32)
    grad_qkvg = jnp.concatenate(
        [
            grad_queries.astype(BF).reshape(2 * length, head_k),
            grad_keys.astype(BF).reshape(2 * length, head_k),
            grad_values.astype(BF).reshape(2 * length, head_v),
            grad_gate_in,
        ],
        axis=1,
    )
    qkvg_mine, qkvg_theirs = reduce_rows(normed_all, grad_qkvg, ())
    grad_normed = scatter_tokens(dot_nt(grad_qkvg, qkvg_full).astype(BF))
    unused, pull_first = jax.vjp(layer_norm, inputs_float, gains_float[0], biases_float[0])
    grad_in_norm, grad_gain_one, grad_bias_one = pull_first(grad_normed)
    input_grad = natural((grad_middle + grad_in_norm).astype(BF))

    norm_rows = natural(jnp.stack([grad_gain_one, grad_gain_two, grad_bias_one, grad_bias_two], axis=0))
    zero = jnp.zeros_like(group_gain_grad)
    group_rows = both(group_gain_grad, zero, 0)
    group_flat = group_rows.reshape(1, -1)
    sums = jnp.concatenate([norm_rows.reshape(1, -1), group_flat], axis=1).reshape(-1, 128)
    for bit in [PAIR] + rest:
        sums = sums + swap_dp(sums, bit)
    sums = sums.reshape(-1)
    norm_sums, group_sums = sums[: 4 * width], sums[4 * width :].reshape(2, head_v)
    norm_sums = norm_sums.reshape(-1, 128)
    for bit in (1, 2):
        norm_sums = norm_sums + swap_t(norm_sums, bit)
    cols = width // (n_dp * n_tensor)
    norm_mine = lax.dynamic_slice_in_dim(norm_sums.reshape(4, width), (d * n_tensor + t) * cols, cols, 1)
    norm_gain_grad, norm_bias_grad = norm_mine[:2], norm_mine[2:]
    group_cols = head_v // n_dp
    group_gain_out = lax.dynamic_slice_in_dim(group_sums, d * group_cols, group_cols, 1)

    def split(value, sizes):
        out, start = [], 0
        for size in sizes:
            out.append(value[:, start : start + size])
            start += size
        return out

    sizes = (head_k, head_k, head_v, head_v)
    query_grad, key_grad, value_grad, gate_grad = (
        both(a, b, 1) for a, b in zip(split(qkvg_mine, sizes), split(qkvg_theirs, sizes), strict=True)
    )
    sizes = (hidden_dev, hidden_dev)
    ffn_gate_grad, ffn_up_grad = (
        both(a, b, 1) for a, b in zip(split(gu_mine, sizes), split(gu_theirs, sizes), strict=True)
    )
    ffn_down_grad = both(down_mine, down_theirs, 1).T
    out_weight_grad = both(out_mine, out_theirs, 1).T
    return (
        layer_out,
        input_grad,
        query_grad,
        key_grad,
        value_grad,
        gate_grad,
        out_weight_grad,
        group_gain_out,
        norm_gain_grad,
        norm_bias_grad,
        ffn_gate_grad,
        ffn_up_grad,
        ffn_down_grad,
    )


def solution(mesh):
    tokens = P(("dp", "tensor"), None)
    rows, cols, norms = P("dp", "tensor"), P("tensor", "dp"), P(None, "dp")
    sums = P(None, ("dp", "tensor"))
    in_specs = (tokens, tokens, cols, rows, rows, rows, rows, cols, cols, norms, norms, rows, rows, cols)
    out_specs = (tokens, tokens, rows, rows, rows, rows, cols, cols, sums, sums, rows, rows, cols)
    body = functools.partial(per_device, mesh.shape["dp"], mesh.shape["tensor"])
    return jax.shard_map(body, mesh=mesh, in_specs=in_specs, out_specs=out_specs, check_vma=False)
```

```python
import functools
import math

import jax
import jax.numpy as jnp
from jax import lax
from jax.experimental import pallas as pl
from jax.experimental.pallas import tpu as pltpu
from jax.sharding import PartitionSpec as P

EPSILON = 1e-05
GROUP_FLOOR = 1.0
BF = jnp.bfloat16
F32 = jnp.float32
PAIR = 2
MESH = pl.DeviceIdType.MESH
QK, V, G, O, FG, FU, FD = range(7)
GROUPS = 7


def dot_nn(a, b):
    return lax.dot_general(a, b, (((1,), (0,)), ((), ())), preferred_element_type=F32)


def dot_nt(a, b):
    return lax.dot_general(a, b, (((1,), (1,)), ((), ())), preferred_element_type=F32)


def dot_tn(a, b):
    return lax.dot_general(a, b, (((0,), (0,)), ((), ())), preferred_element_type=F32)


def flip(index, bit):
    return index + bit - 2 * bit * ((index // bit) % 2)


class Place:
    def __init__(self, n_dp):
        self.n_dp = n_dp
        self.d = lax.axis_index("dp")
        self.t = lax.axis_index("tensor")
        self.z = (self.d // PAIR) % 2
        self.rest = [1 << i for i in range(2, n_dp.bit_length() - 1)] + [1]
        self.inner = self.rest[:-1]
        self.masks = []
        for pick in range(1, 1 << (1 + len(self.inner))):
            bits = [PAIR] * (pick & 1) + [b for k, b in enumerate(self.inner) if (pick >> (k + 1)) & 1]
            self.masks.append((bits, pick & ~1, pick & 1))
        half = n_dp // 2
        self.pairs = self.masks + [([1], half, 0)] + [(bits + [1], above + half, flips) for bits, above, flips in self.masks]

    def peer(self, bits):
        out = self.d
        for bit in bits:
            out = flip(out, bit)
        return {"dp": out}

    def x_peer(self):
        return {"dp": flip(self.d, 1)}

    def z_peer(self):
        return {"dp": flip(self.d, PAIR)}

    def y_peer(self):
        return {"tensor": flip(self.t, 2)}

    def c_peer(self):
        return {"tensor": flip(self.t, 1)}

    def everyone(self, far):
        near = [self.x_peer(), self.y_peer(), self.c_peer()]
        if far:
            return near[1:] + [self.peer(bits) for bits, _, _ in self.pairs]
        return near + [self.peer(bits) for bits, _, _ in self.masks]


def entry_barrier(place, far=False):
    barrier = pltpu.get_barrier_semaphore()
    peers = place.everyone(far)
    for peer in peers:
        pl.semaphore_signal(barrier, inc=1, device_id=peer, device_id_type=MESH)
    pl.semaphore_wait(barrier, len(peers))


def remote(src, dst, send, recv, peer):
    return pltpu.make_async_remote_copy(
        src_ref=src, dst_ref=dst, send_sem=send, recv_sem=recv, device_id=peer, device_id_type=MESH
    )


class Weights:
    def __init__(self, place, sources, full, sems):
        self.place, self.sources, self.full = place, sources, full
        self.z_send, self.z_recv, self.x_send, self.x_recv, self.local = sems
        self.block = sources[0].shape[0]
        self.cols = sources[0].shape[1] // 2
        self.half = place.n_dp // 2

    def rows(self, position, count=1):
        return pl.ds(pl.multiple_of(position * self.block, self.block), count * self.block)

    def source(self, g, half):
        return self.sources[g].at[:, pl.ds(pl.multiple_of(half * self.cols, self.cols), self.cols)]

    def start(self, g):
        place = self.place
        z = place.z
        own = pltpu.make_async_copy(self.source(g, z), self.full.at[g, self.rows(z), :], self.local.at[g])
        own.start()
        for i, (bits, above, flips) in enumerate(place.masks):
            half = 1 - z if flips else z
            remote(
                self.source(g, half),
                self.full.at[g, self.rows(z + above), :],
                self.z_send.at[g],
                self.z_recv.at[g, i],
                place.peer(bits),
            ).start()
        remote(
            self.source(g, z),
            self.full.at[g, self.rows(z + self.half), :],
            self.x_send.at[g],
            self.x_recv.at[g],
            place.x_peer(),
        ).start()

    def forward(self, g, i):
        place = self.place
        bits, above, flips = place.masks[i]
        position = (1 - place.z if flips else place.z) + above
        here = self.full.at[g, self.rows(position), :]
        remote(here, here, self.z_send.at[g], self.z_recv.at[g, i], place.peer(bits)).wait_recv()
        remote(
            here,
            self.full.at[g, self.rows(position + self.half), :],
            self.x_send.at[g],
            self.x_recv.at[g],
            place.x_peer(),
        ).start()

    def forward_all(self, g):
        for i in range(len(self.place.masks)):
            self.forward(g, i)

    def finish(self, g):
        z = self.place.z
        pltpu.make_async_copy(self.source(g, z), self.full.at[g, self.rows(z), :], self.local.at[g]).wait()
        there = self.full.at[g, self.rows(self.half, self.half), :]
        remote(there, there, self.x_send.at[g], self.x_recv.at[g], self.place.x_peer()).wait_recv()

    def sent(self, g):
        there = self.full.at[g, self.rows(self.half, self.half), :]
        remote(there, there, self.x_send.at[g], self.x_recv.at[g], self.place.x_peer()).wait_send()
        count = self.half - 1
        those = self.full.at[g, self.rows(0, count), :]
        remote(those, those, self.z_send.at[g], self.z_recv.at[g, 0], self.place.x_peer()).wait_send()


class Gather:
    def __init__(self, place, buffer, send, recv):
        self.place, self.buffer = place, buffer
        self.send, self.recv = send, recv
        self.tokens = buffer.shape[0] // 8
        self.peers = {1: place.c_peer(), 2: place.y_peer(), 4: place.z_peer()}

    def slot(self, s):
        return self.buffer.at[pl.ds(s * self.tokens, self.tokens), :]

    def copy(self, source, bit, src=None):
        s = source + bit
        return remote(self.slot(source) if src is None else src, self.slot(s), self.send.at[s - 1], self.recv.at[s - 1], self.peers[bit])

    def start(self, src=None):
        for bit in (4, 2, 1):
            self.copy(0, bit, src).start()

    def from_z(self):
        self.copy(0, 4).wait_recv()
        self.copy(4, 2).start()
        self.copy(4, 1).start()

    def from_y(self):
        self.copy(0, 2).wait_recv()
        self.copy(2, 1).start()

    def from_zy(self):
        self.copy(4, 2).wait_recv()
        self.copy(6, 1).start()

    def chip(self, source):
        self.copy(source, 1).wait_recv()

    def sent(self, src=None):
        self.copy(0, 4, src).wait_send()
        self.copy(0, 2, src).wait_send()
        self.copy(0, 1, src).wait_send()
        self.copy(4, 2).wait_send()
        self.copy(4, 1).wait_send()
        self.copy(2, 1).wait_send()
        self.copy(6, 1).wait_send()


class Scatter:
    def __init__(self, place, keep, c_out, c_in, far_out, far_in, sems):
        self.place = place
        self.keep, self.c_out, self.c_in, self.far_out, self.far_in = keep, c_out, c_in, far_out, far_in
        self.c_send, self.c_recv, self.far_send, self.far_recv = sems
        self.tokens = c_out.shape[1]

    def part(self, b, value):
        self.keep[b] = value[: self.tokens].astype(self.keep.dtype)
        self.c_out[b] = value[self.tokens :].astype(BF)
        self.c_copy(b).start()

    def c_copy(self, b):
        return remote(self.c_out.at[b], self.c_in.at[b], self.c_send.at[b], self.c_recv.at[b], self.place.c_peer())

    def far_copy(self, b):
        peer = self.place.z_peer() if b == 2 else self.place.y_peer()
        return remote(
            self.far_source(b), self.far_in.at[b - 1], self.far_send.at[b - 1], self.far_recv.at[b - 1], peer
        )

    def far_source(self, b):
        return self.keep.at[b] if self.far_out is None else self.far_out.at[b - 1]

    def rows(self, body, step=16):
        def loop(i, carry):
            body(pl.ds(pl.multiple_of(i * step, step), step))
            return carry

        lax.fori_loop(0, self.tokens // step, loop, 0)

    def pass_on(self, b):
        self.c_copy(b).wait_recv()
        if b == 2:
            self.far_copy(3).wait_recv()

        def body(r):
            total = self.keep[b, r, :].astype(F32) + self.c_in[b, r, :].astype(F32)
            if b == 2:
                total = total + self.far_in[2, r, :].astype(F32)
            self.far_source(b)[r, :] = total.astype(BF)

        self.rows(body)
        self.far_copy(b).start()

    def wait_own(self):
        self.c_copy(0).wait_recv()
        self.far_copy(1).wait_recv()
        self.far_copy(2).wait_recv()

    def own(self, r):
        return (
            self.keep[0, r, :].astype(F32)
            + self.c_in[0, r, :].astype(F32)
            + self.far_in[0, r, :].astype(F32)
            + self.far_in[1, r, :].astype(F32)
        )

    def sent(self):
        for b in range(4):
            self.c_copy(b).wait_send()
        for b in (3, 2, 1):
            self.far_copy(b).wait_send()


def normalized(value):
    center = value - jnp.mean(value, axis=-1, keepdims=True)
    spread = jnp.mean(center * center, axis=-1, keepdims=True)
    return center * lax.rsqrt(spread + EPSILON)


def decay_tile(t, cumul_rows, cumul_cols, first, rows, length, tokens):
    index = lax.broadcasted_iota(jnp.int32, (rows, length), 0) + first
    other = lax.broadcasted_iota(jnp.int32, (rows, length), 1)
    at = ((index // tokens) ^ t) * tokens + index % tokens
    to = ((other // tokens) ^ t) * tokens + other % tokens
    causal = at >= to
    return jnp.where(causal, jnp.exp(jnp.where(causal, cumul_cols - cumul_rows, 0.0)), 0.0)


def forward_kernel(
    n_dp,
    x_ref,
    cot_ref,
    params_ref,
    group_ref,
    cum_row_ref,
    cum_col_ref,
    s_qk,
    s_v,
    s_g,
    s_o,
    s_fg,
    s_fu,
    s_fd,
    w_out,
    normed_out,
    qkv_out,
    gate_out,
    mixed_out,
    ffn_in_out,
    hidden_out,
    grads_out,
    cot_out,
    middle_out,
    w,
    normed_all,
    cot_all,
    ffn_in,
    qkv,
    gate_in,
    mixed,
    gated,
    gate_hidden,
    up_hidden,
    hidden,
    grads,
    middle,
    keep,
    c_out,
    c_in,
    far_out,
    far_in,
    z_send,
    z_recv,
    x_send,
    x_recv,
    w_local,
    ag_send,
    ag_recv,
    c_send,
    c_recv,
    far_send,
    far_recv,
    out_sem,
):
    place = Place(n_dp)
    tokens, width = x_ref.shape
    rows_all = 8 * tokens
    length = rows_all // 2
    head_k = qkv.shape[1] // 4
    scale = 1.0 / math.sqrt(head_k)
    tile = 2 * tokens
    weights = Weights(place, [s_qk, s_v, s_g, s_o, s_fg, s_fu, s_fd], w, (z_send, z_recv, x_send, x_recv, w_local))
    ag_normed = Gather(place, normed_all, ag_send.at[0], ag_recv.at[0])
    ag_cot = Gather(place, cot_all, ag_send.at[1], ag_recv.at[1])
    ag_two = Gather(place, ffn_in, ag_send.at[2], ag_recv.at[2])
    branch = Scatter(place, keep, c_out, c_in, far_out, far_in, (c_send, c_recv, far_send, far_recv))
    outs = []

    def save(src, dst, index):
        copy = pltpu.make_async_copy(src, dst, out_sem.at[index])
        copy.start()
        outs.append(copy)

    def over(count, step, body):
        def loop(i, carry):
            body(pl.ds(pl.multiple_of(i * step, step), step), i)
            return carry

        lax.fori_loop(0, count // step, loop, 0)

    entry_barrier(place)
    cot_own = pltpu.make_async_copy(cot_ref, ag_cot.slot(0), out_sem.at[17])
    cot_own.start()
    weights.start(QK)

    def first_norm(r, i):
        value = normalized(x_ref[r, :].astype(F32))
        normed_all[r, :] = (value * params_ref[0:1, :] + params_ref[2:3, :]).astype(BF)

    over(tokens, 16, first_norm)
    ag_normed.start()
    weights.start(V)
    weights.forward(QK, 0)
    ag_normed.from_z()
    ag_normed.from_y()
    for i in range(1, len(place.masks)):
        weights.forward(QK, i)
    weights.start(G)
    ag_normed.from_zy()
    ag_cot.start(cot_ref)
    weights.forward(V, 0)
    for s in (0, 2, 4, 6):
        ag_normed.chip(s)
    save(normed_all, normed_out, 0)
    weights.finish(QK)

    def make_qk(r, i):
        qkv[r, : 2 * head_k] = dot_nn(normed_all[r, :], w[QK]).astype(BF)

    over(rows_all, tile, make_qk)
    save(w.at[QK], w_out.at[QK], 1)
    for i in range(1, len(place.masks)):
        weights.forward(V, i)
    weights.start(O)
    ag_cot.from_z()
    ag_cot.from_y()
    weights.forward(G, 0)
    weights.finish(V)

    def make_v(r, i):
        qkv[r, 2 * head_k :] = dot_nn(normed_all[r, :], w[V]).astype(BF)

    over(rows_all, tile, make_v)
    save(w.at[V], w_out.at[V], 2)
    save(qkv, qkv_out, 3)
    for i in range(1, len(place.masks)):
        weights.forward(G, i)
    weights.start(FG)

    def retention(r, i):
        start = pl.multiple_of((i // 2) * length, length)
        seq = pl.ds(start, length)
        scores = dot_nt(qkv[r, :head_k], qkv[seq, head_k : 2 * head_k])
        decays = decay_tile(
            place.t, cum_row_ref[pl.ds(i // 2, 1), :], cum_col_ref[r, :], (i % 2) * tile, tile, length, tokens
        )
        weighted = (scores * decays * scale).astype(BF)
        mixed[r, :] = dot_nn(weighted, qkv[seq, 2 * head_k :])

    over(rows_all, tile, retention)
    save(mixed, mixed_out, 4)
    ag_cot.from_zy()
    weights.forward(O, 0)
    weights.finish(G)

    def gating(r, i):
        gate = dot_nn(normed_all[r, :], w[G])
        gate_in[r, :] = gate
        value = mixed[r, :]
        center = value - jnp.mean(value, axis=-1, keepdims=True)
        spread = jnp.mean(center * center, axis=-1, keepdims=True)
        flat = center * lax.rsqrt(jnp.maximum(spread, GROUP_FLOOR)) * group_ref[...]
        gated[r, :] = (flat * (gate * lax.logistic(gate))).astype(BF)

    over(rows_all, tile, gating)
    save(w.at[G], w_out.at[G], 5)
    save(gate_in, gate_out, 6)
    for i in range(1, len(place.masks)):
        weights.forward(O, i)
    weights.start(FU)
    for s in (0, 2, 4, 6):
        ag_cot.chip(s)
    weights.forward(FG, 0)
    weights.finish(O)
    for b in (3, 2, 1, 0):
        branch.part(b, dot_nt(gated[b * tile : (b + 1) * tile, :], w[O]))
    save(w.at[O], w_out.at[O], 7)
    branch.pass_on(3)
    branch.pass_on(1)
    for i in range(1, len(place.masks)):
        weights.forward(FG, i)
    branch.pass_on(2)
    cot_own.wait()
    save(cot_all, cot_out, 8)
    weights.forward(FU, 0)
    branch.wait_own()

    def second_norm(r, i):
        value = x_ref[r, :].astype(F32) + branch.own(r)
        middle[r, :] = value
        ffn_in[r, :] = (normalized(value) * params_ref[1:2, :] + params_ref[3:4, :]).astype(BF)

    over(tokens, 16, second_norm)
    ag_two.start()
    weights.start(FD)
    save(middle, middle_out, 9)
    for i in range(1, len(place.masks)):
        weights.forward(FU, i)
    weights.finish(FG)
    weights.finish(FU)

    def feed(b):
        r = pl.ds(b * tile, tile)
        gate = dot_nn(ffn_in[r, :], w[FG])
        up = dot_nn(ffn_in[r, :], w[FU])
        gate_hidden[r, :] = gate
        up_hidden[r, :] = up
        hidden[r, :] = (gelu(gate) * up).astype(BF)

    ag_two.chip(0)
    feed(0)
    ag_two.from_z()
    ag_two.from_y()
    ag_two.chip(2)
    feed(1)
    ag_two.chip(4)
    feed(2)
    weights.forward(FD, 0)
    ag_two.from_zy()
    ag_two.chip(6)
    feed(3)
    save(w.at[FG], w_out.at[FG], 10)
    save(w.at[FU], w_out.at[FU], 11)
    save(ffn_in, ffn_in_out, 12)
    save(hidden, hidden_out, 13)
    for i in range(1, len(place.masks)):
        weights.forward(FD, i)
    weights.finish(FD)
    save(w.at[FD], w_out.at[FD], 14)
    size = gate_hidden.shape[1]

    def feed_back(r, i):
        back = dot_nn(cot_all[r, :], w[FD])
        gate = gate_hidden[r, :]
        value, slope = gelu_and_slope(gate)
        grads[r, :size] = (back * up_hidden[r, :] * slope).astype(BF)
        grads[r, size:] = (back * value).astype(BF)

    over(rows_all, tile, feed_back)
    save(grads, grads_out, 15)
    for copy in outs:
        copy.wait()
    for g in range(GROUPS):
        weights.sent(g)
    ag_normed.sent()
    ag_cot.sent(cot_ref)
    ag_two.sent()
    branch.sent()


ROOT = math.sqrt(2.0 / math.pi)


def gelu(v):
    return 0.5 * v * (1.0 + jnp.tanh(ROOT * (v + 0.044715 * v * v * v)))


def gelu_and_slope(v):
    inside = jnp.tanh(ROOT * (v + 0.044715 * v * v * v))
    slope = 0.5 * (1.0 + inside) + 0.5 * v * (1.0 - inside * inside) * ROOT * (1.0 + 3 * 0.044715 * v * v)
    return 0.5 * v * (1.0 + inside), slope


def forward_call(n_dp, x, cot, params, group, cum_row, cum_col, sources):
    tokens, width = x.shape
    rows_all = 8 * tokens
    cols = sources[0].shape[1] // 2
    masks = n_dp // 2 - 1
    vmem, hbm = pl.BlockSpec(memory_space=pltpu.VMEM), pl.BlockSpec(memory_space=pl.ANY)
    shape = jax.ShapeDtypeStruct
    outs = (
        shape((GROUPS, width, cols), BF),
        shape((rows_all, width), BF),
        shape((rows_all, 2 * cols), BF),
        shape((rows_all, cols), F32),
        shape((rows_all, cols), F32),
        shape((rows_all, width), BF),
        shape((rows_all, cols), BF),
        shape((rows_all, 2 * cols), BF),
        shape((rows_all, width), BF),
        shape((tokens, width), F32),
    )
    dma = pltpu.SemaphoreType.DMA
    scratch = [
        pltpu.VMEM((GROUPS, width, cols), BF),
        pltpu.VMEM((rows_all, width), BF),
        pltpu.VMEM((rows_all, width), BF),
        pltpu.VMEM((rows_all, width), BF),
        pltpu.VMEM((rows_all, 2 * cols), BF),
        pltpu.VMEM((rows_all, cols), F32),
        pltpu.VMEM((rows_all, cols), F32),
        pltpu.VMEM((rows_all, cols), BF),
        pltpu.VMEM((rows_all, cols), F32),
        pltpu.VMEM((rows_all, cols), F32),
        pltpu.VMEM((rows_all, cols), BF),
        pltpu.VMEM((rows_all, 2 * cols), BF),
        pltpu.VMEM((tokens, width), F32),
        pltpu.VMEM((4, tokens, width), F32),
        pltpu.VMEM((4, tokens, width), BF),
        pltpu.VMEM((4, tokens, width), BF),
        pltpu.VMEM((3, tokens, width), BF),
        pltpu.VMEM((3, tokens, width), BF),
        dma((GROUPS,)),
        dma((GROUPS, masks)),
        dma((GROUPS,)),
        dma((GROUPS,)),
        dma((GROUPS,)),
        dma((3, 7)),
        dma((3, 7)),
        dma((4,)),
        dma((4,)),
        dma((3,)),
        dma((3,)),
        dma((18,)),
    ]
    return pl.pallas_call(
        functools.partial(forward_kernel, n_dp),
        out_shape=outs,
        in_specs=[vmem, hbm, vmem, vmem, vmem, vmem] + [hbm] * GROUPS,
        out_specs=(hbm,) * len(outs),
        scratch_shapes=scratch,
        compiler_params=pltpu.CompilerParams(
            collective_id=1, has_side_effects=True, vmem_limit_bytes=64_000_000
        ),
    )(x, cot, params, group, cum_row, cum_col, *sources)


class Reduce:
    def __init__(self, place, keep, x_out, x_in, z_in, own_out, sems, own_sem):
        self.place = place
        self.keep, self.x_out, self.x_in, self.z_in, self.own_out = keep, x_out, x_in, z_in, own_out
        self.x_send, self.x_recv, self.z_send, self.z_recv = sems
        self.own_sem = own_sem
        self.block = z_in.shape[2]
        self.half = place.n_dp // 2
        z = place.z
        self.targets = [
            ((1 - z if flips else z) + above, i, place.peer(bits)) for i, (bits, above, flips) in enumerate(place.masks)
        ]
        self.targets.reverse()

    def rows(self, position):
        return pl.ds(pl.multiple_of(position * self.block, self.block), self.block)

    def x_copy(self, g, ring, position):
        return remote(
            self.x_out.at[ring, self.rows(position), :],
            self.x_in.at[g, self.rows(position), :],
            self.x_send.at[g],
            self.x_recv.at[g, position],
            self.place.x_peer(),
        )

    def z_copy(self, g, position, i, peer):
        return remote(
            self.keep.at[g, self.rows(position), :],
            self.z_in.at[g, i],
            self.z_send.at[g],
            self.z_recv.at[g, i],
            peer,
        )

    def product(self, g, ring, left, right, col, step):
        width = left.shape[1] // 2
        cols = self.keep.shape[2]

        def upper(i, carry):
            at = pl.multiple_of(i * step, step)
            value = dot_tn(left[:, pl.ds(pl.multiple_of(width + at, step), step)], right[:, col : col + cols])
            self.x_out[ring, pl.ds(at, step), :] = value.astype(BF)
            return carry

        lax.fori_loop(0, width // step, upper, 0)
        for position, _, _ in self.targets:
            self.x_copy(g, ring, position).start()
        self.x_copy(g, ring, self.place.z).start()

        def lower(i, carry):
            at = pl.ds(pl.multiple_of(i * step, step), step)
            self.keep[g, at, :] = dot_tn(left[:, at], right[:, col : col + cols]).astype(BF)
            return carry

        lax.fori_loop(0, width // step, lower, 0)

    def x_sent(self, g, ring):
        whole = self.x_out.at[ring]
        remote(whole, whole, self.x_send.at[g], self.x_recv.at[g, 0], self.place.x_peer()).wait_send()

    def add(self, g, ring, position):
        self.x_copy(g, ring, position).wait_recv()
        step = min(64, self.block)

        def body(i, carry):
            r = pl.ds(pl.multiple_of(position * self.block + i * step, step), step)
            self.keep[g, r, :] = (self.keep[g, r, :].astype(F32) + self.x_in[g, r, :].astype(F32)).astype(BF)
            return carry

        lax.fori_loop(0, self.block // step, body, 0)

    def own_copy(self, g):
        return pltpu.make_async_copy(
            self.keep.at[g, self.rows(self.place.z), :], self.own_out.at[g], self.own_sem.at[g]
        )

    def pass_on(self, g, ring):
        for position, i, peer in self.targets:
            self.add(g, ring, position)
            self.z_copy(g, position, i, peer).start()
        self.add(g, ring, self.place.z)
        self.own_copy(g).start()

    def finish(self, g):
        self.own_copy(g).wait()
        for position, i, peer in self.targets:
            self.z_copy(g, position, i, peer).wait()


def norm_back(value, grad, gain):
    center = value - jnp.mean(value, axis=-1, keepdims=True)
    spread = jnp.mean(center * center, axis=-1, keepdims=True)
    r = lax.rsqrt(spread + EPSILON)
    hat = center * r
    scaled = grad * gain
    back = r * (
        scaled - jnp.mean(scaled, axis=-1, keepdims=True) - hat * jnp.mean(scaled * hat, axis=-1, keepdims=True)
    )
    return back, jnp.sum(grad * hat, axis=0, keepdims=True), jnp.sum(grad, axis=0, keepdims=True)


def backward_kernel(
    n_dp,
    x_ref,
    params_ref,
    group_ref,
    cum_row_ref,
    cum_col_ref,
    w_ref,
    normed_ref,
    qkv_ref,
    gate_ref,
    mixed_ref,
    ffn_in_ref,
    hidden_ref,
    grads_ref,
    cot_ref,
    middle_ref,
    layer_out,
    input_grad_out,
    own_out,
    z_in,
    sums_out,
    w,
    tokens_a,
    ffn_in,
    branch_all,
    slim,
    qkv,
    gate_in,
    mixed,
    gated,
    middle,
    grad_middle,
    sums,
    sums_in,
    group_sum,
    payload,
    payload_in,
    keep,
    c_out,
    c_in,
    far_in,
    c_in_two,
    far_in_two,
    dw_keep,
    x_out,
    x_in,
    ag_send,
    ag_recv,
    c_send,
    c_recv,
    far_send,
    far_recv,
    x_send,
    x_recv,
    z_send,
    z_recv,
    load_sem,
    own_sem,
    sum_send,
    sum_recv,
    pay_send,
    pay_recv,
):
    place = Place(n_dp)
    tokens, width = x_ref.shape
    rows_all = 8 * tokens
    length = rows_all // 2
    cols = gated.shape[1]
    head_k = cols // 2
    scale = 1.0 / math.sqrt(head_k)
    tile = 2 * tokens
    step = min(512, width // 2)
    block = z_in.shape[2]
    ag = Gather(place, branch_all, ag_send, ag_recv)

    def scatter(k, c, far):
        return Scatter(place, keep, c_out, c, None, far, (c_send.at[k], c_recv.at[k], far_send.at[k], far_recv.at[k]))

    rs_two = scatter(0, c_in, far_in)
    rs_out = scatter(1, c_in_two, far_in_two)
    rs_one = scatter(2, c_in, far_in)
    dw = Reduce(place, dw_keep, x_out, x_in, z_in, own_out, (x_send, x_recv, z_send, z_recv), own_sem)
    result = ffn_in.at[:tokens, :]
    weighted = ffn_in.at[tokens : tokens + length, :length]
    score_back = ffn_in.at[tokens : tokens + length, length : 2 * length]
    ring = {FD: 0, FG: 1, FU: 2, O: 3, QK: 0, V: 1, G: 2}

    def load(src, dst, index):
        copy = pltpu.make_async_copy(src, dst, load_sem.at[index])
        copy.start()
        return copy

    def over(count, size, body):
        def loop(i, carry):
            body(pl.ds(pl.multiple_of(i * size, size), size), i)
            return carry

        lax.fori_loop(0, count // size, loop, 0)

    in_grads = load(grads_ref, slim.at[:, : 2 * cols], 0)
    in_fg = load(w_ref.at[FG], w.at[0], 1)
    in_fu = load(w_ref.at[FU], w.at[1], 2)
    in_cot = load(cot_ref, tokens_a, 3)
    in_hidden = load(hidden_ref, slim.at[:, 2 * cols :], 4)
    in_ffn = load(ffn_in_ref, ffn_in, 5)
    in_middle = load(middle_ref, middle, 6)
    in_mixed = load(mixed_ref, mixed, 7)
    in_gate = load(gate_ref, gate_in, 8)
    in_o = load(w_ref.at[O], w.at[2], 9)
    in_qkv = load(qkv_ref, qkv, 10)
    sums[...] = jnp.zeros_like(sums)
    group_sum[...] = jnp.zeros_like(group_sum)
    entry_barrier(place, True)
    in_grads.wait()
    in_fg.wait()
    in_fu.wait()
    for b in (3, 2, 1, 0):
        r = slice(b * tile, (b + 1) * tile)
        rs_two.part(b, dot_nt(slim[r, :cols], w[0]) + dot_nt(slim[r, cols : 2 * cols], w[1]))
    in_fd = load(w_ref.at[FD], w.at[0], 1)
    in_qk = load(w_ref.at[QK], w.at[1], 2)
    rs_two.pass_on(3)
    rs_two.pass_on(1)
    in_cot.wait()
    in_hidden.wait()
    dw.product(FD, ring[FD], tokens_a, slim, 2 * cols, step)
    in_ffn.wait()
    dw.product(FG, ring[FG], ffn_in, slim, 0, step)
    rs_two.pass_on(2)
    dw.product(FU, ring[FU], ffn_in, slim, cols, step)
    in_mixed.wait()
    in_gate.wait()

    def gating(r, i):
        value = mixed[r, :]
        center = value - jnp.mean(value, axis=-1, keepdims=True)
        spread = jnp.mean(center * center, axis=-1, keepdims=True)
        gate = gate_in[r, :]
        flat = center * lax.rsqrt(jnp.maximum(spread, GROUP_FLOOR)) * group_ref[...]
        gated[r, :] = (flat * (gate * lax.logistic(gate))).astype(BF)

    over(rows_all, tokens, gating)
    in_middle.wait()
    rs_two.wait_own()

    def second_back(r, i):
        back, gain_sum, bias_sum = norm_back(middle[r, :], rs_two.own(r), params_ref[1:2, :])
        total = tokens_a[r, :].astype(F32) + back
        grad_middle[r, :] = total
        branch_all[r, :] = total.astype(BF)
        sums[1:2, :] += gain_sum
        sums[3:4, :] += bias_sum

    over(tokens, 16, second_back)
    ag.start()
    in_normed = load(normed_ref, tokens_a, 3)
    rs_two.sent()
    in_fd.wait()
    for b in (3, 2, 1, 0):
        rs_out.part(b, dot_nt(slim[b * tile : (b + 1) * tile, 2 * cols :], w[0]))
    in_v = load(w_ref.at[V], w.at[0], 1)
    dw.pass_on(FD, ring[FD])
    ag.from_z()
    ag.from_y()
    rs_out.pass_on(3)
    rs_out.pass_on(1)
    in_o.wait()
    in_qkv.wait()

    def gating_back(b):
        r = pl.ds(b * tile, tile)
        back = dot_nn(branch_all[r, :], w[2])
        value = mixed[r, :]
        center = value - jnp.mean(value, axis=-1, keepdims=True)
        spread = jnp.mean(center * center, axis=-1, keepdims=True)
        inverse = lax.rsqrt(jnp.maximum(spread, GROUP_FLOOR))
        hat = center * inverse
        gate = gate_in[r, :]
        sigmoid = lax.logistic(gate)
        flat = hat * group_ref[...]
        slope = sigmoid * (1.0 + gate * (1.0 - sigmoid))
        slim[r, 2 * cols :] = (back * flat * slope).astype(BF)
        grad = back * (gate * sigmoid)
        group_sum[...] += jnp.sum(grad * hat, axis=0, keepdims=True)
        scaled = grad * group_ref[...]
        live = jnp.where(spread > GROUP_FLOOR, 1.0, jnp.where(spread == GROUP_FLOOR, 0.5, 0.0))
        moment = jnp.mean(scaled * hat, axis=-1, keepdims=True) * live
        mixed_back = inverse * (scaled - jnp.mean(scaled, axis=-1, keepdims=True) - hat * moment)
        slim[r, cols : 2 * cols] = mixed_back.astype(BF)

    def sequence_back(s):
        seq = pl.ds(s * length, length)

        def body(i, carry):
            r = pl.ds(pl.multiple_of(s * length + i * tile, tile), tile)
            at = pl.ds(pl.multiple_of(i * tile, tile), tile)
            scores = dot_nt(qkv[r, :head_k], qkv[seq, head_k : 2 * head_k])
            decays = decay_tile(
                place.t, cum_row_ref[s : s + 1, :], cum_col_ref[r, :], i * tile, tile, length, tokens
            )
            weighted[at, :] = (scores * decays * scale).astype(BF)
            back = dot_nt(slim[r, cols : 2 * cols], qkv[seq, 2 * head_k :])
            grad = (back * decays * scale).astype(BF)
            score_back[at, :] = grad
            slim[r, :head_k] = dot_nn(grad, qkv[seq, head_k : 2 * head_k]).astype(BF)
            return carry

        lax.fori_loop(0, length // tile, body, 0)
        slim[seq, head_k : 2 * head_k] = dot_tn(score_back[...], qkv[seq, :head_k]).astype(BF)
        slim[seq, cols : 2 * cols] = dot_tn(weighted[...], slim[seq, cols : 2 * cols]).astype(BF)

    ag.chip(0)
    gating_back(0)
    ag.chip(2)
    gating_back(1)
    sequence_back(0)
    ag.from_zy()
    rs_out.pass_on(2)
    ag.chip(4)
    gating_back(2)
    ag.chip(6)
    gating_back(3)
    in_g = load(w_ref.at[G], w.at[2], 9)
    dw.product(O, ring[O], branch_all, gated, 0, step)
    sequence_back(1)
    dw.pass_on(FG, ring[FG])
    in_normed.wait()
    dw.x_sent(FD, ring[FD])
    dw.product(QK, ring[QK], tokens_a, slim, 0, step)
    rs_out.wait_own()

    def finish_out(r, i):
        result[r, :] = (middle[r, :] + rs_out.own(r)).astype(BF)

    over(tokens, 16, finish_out)
    out_layer = load(result, layer_out, 4)
    rs_out.sent()
    in_qk.wait()
    in_v.wait()
    in_g.wait()
    for b in (3, 2, 1, 0):
        r = slice(b * tile, (b + 1) * tile)
        total = dot_nt(slim[r, :cols], w[1]) + dot_nt(slim[r, cols : 2 * cols], w[0])
        rs_one.part(b, total + dot_nt(slim[r, 2 * cols :], w[2]))
    dw.x_sent(FG, ring[FG])
    dw.product(V, ring[V], tokens_a, slim, cols, step)
    rs_one.pass_on(3)
    rs_one.pass_on(1)
    dw.pass_on(FU, ring[FU])
    dw.x_sent(FU, ring[FU])
    dw.product(G, ring[G], tokens_a, slim, 2 * cols, step)
    rs_one.pass_on(2)
    dw.pass_on(O, ring[O])
    out_layer.wait()
    rs_one.wait_own()

    def first_back(r, i):
        back, gain_sum, bias_sum = norm_back(x_ref[r, :].astype(F32), rs_one.own(r), params_ref[0:1, :])
        result[r, :] = (grad_middle[r, :] + back).astype(BF)
        sums[0:1, :] += gain_sum
        sums[2:3, :] += bias_sum

    over(tokens, 16, first_back)
    out_grad = load(result, input_grad_out, 4)

    def sum_copy(k, peer):
        return remote(sums, sums_in.at[k], sum_send.at[k], sum_recv.at[k], peer)

    for k, peer in enumerate((place.c_peer(), place.y_peer())):
        sum_copy(k, peer).start()
        sum_copy(k, peer).wait()
        sums[...] += sums_in[k]
    pieces = cols // block
    for p in range(n_dp):
        payload[p, 0:4, :] = sums[0:4, p * block : (p + 1) * block]
        for k in range(pieces):
            payload[p, 4 + k : 5 + k, :] = group_sum[0:1, k * block : (k + 1) * block]
    pay = []
    for j, (bits, above, flips) in enumerate(place.pairs):
        position = (1 - place.z if flips else place.z) + above
        copy = remote(payload.at[position], payload_in.at[j], pay_send.at[j], pay_recv.at[j], place.peer(bits))
        copy.start()
        pay.append(copy)
    dw.pass_on(QK, ring[QK])
    for copy in pay:
        copy.wait()
    mine = payload[place.z]
    other = jnp.zeros_like(mine)
    for j, (bits, above, flips) in enumerate(place.pairs):
        if flips:
            other = other + payload_in[j]
        else:
            mine = mine + payload_in[j]
    sums_out[0] = mine
    sums_out[1] = other
    dw.pass_on(V, ring[V])
    dw.pass_on(G, ring[G])
    out_grad.wait()
    for g in (O, QK, V, G):
        dw.x_sent(g, ring[g])
    ag.sent()
    rs_one.sent()
    for g in (FD, FG, FU, O, QK, V, G):
        dw.finish(g)


def backward_call(n_dp, x, params, group, cum_row, cum_col, saved):
    tokens, width = x.shape
    rows_all = 8 * tokens
    w = saved[0]
    cols = w.shape[2]
    block = width // n_dp
    masks = n_dp // 2 - 1
    vmem, hbm = pl.BlockSpec(memory_space=pltpu.VMEM), pl.BlockSpec(memory_space=pl.ANY)
    shape = jax.ShapeDtypeStruct
    pay_rows = -(-(4 + cols // block) // 8) * 8
    outs = (
        shape((tokens, width), BF),
        shape((tokens, width), BF),
        shape((GROUPS, block, cols), BF),
        shape((GROUPS, masks, block, cols), BF),
        shape((2, pay_rows, block), F32),
    )
    dma = pltpu.SemaphoreType.DMA
    scratch = [
        pltpu.VMEM((3, width, cols), BF),
        pltpu.VMEM((rows_all, width), BF),
        pltpu.VMEM((rows_all, width), BF),
        pltpu.VMEM((rows_all, width), BF),
        pltpu.VMEM((rows_all, 3 * cols), BF),
        pltpu.VMEM((rows_all, 2 * cols), BF),
        pltpu.VMEM((rows_all, cols), F32),
        pltpu.VMEM((rows_all, cols), F32),
        pltpu.VMEM((rows_all, cols), BF),
        pltpu.VMEM((tokens, width), F32),
        pltpu.VMEM((tokens, width), F32),
        pltpu.VMEM((8, width), F32),
        pltpu.VMEM((2, 8, width), F32),
        pltpu.VMEM((1, cols), F32),
        pltpu.VMEM((n_dp, pay_rows, block), F32),
        pltpu.VMEM((n_dp - 1, pay_rows, block), F32),
        pltpu.VMEM((4, tokens, width), BF),
        pltpu.VMEM((4, tokens, width), BF),
        pltpu.VMEM((4, tokens, width), BF),
        pltpu.VMEM((3, tokens, width), BF),
        pltpu.VMEM((4, tokens, width), BF),
        pltpu.VMEM((3, tokens, width), BF),
        pltpu.VMEM((GROUPS, width // 2, cols), BF),
        pltpu.VMEM((4, width // 2, cols), BF),
        pltpu.VMEM((GROUPS, width // 2, cols), BF),
        dma((7,)),
        dma((7,)),
        dma((3, 4)),
        dma((3, 4)),
        dma((3, 3)),
        dma((3, 3)),
        dma((GROUPS,)),
        dma((GROUPS, n_dp // 2)),
        dma((GROUPS,)),
        dma((GROUPS, masks)),
        dma((11,)),
        dma((GROUPS,)),
        dma((2,)),
        dma((2,)),
        dma((n_dp - 1,)),
        dma((n_dp - 1,)),
    ]
    return pl.pallas_call(
        functools.partial(backward_kernel, n_dp),
        out_shape=outs,
        in_specs=[vmem] * 5 + [hbm] * len(saved),
        out_specs=(hbm,) * 4 + (vmem,),
        scratch_shapes=scratch,
        compiler_params=pltpu.CompilerParams(
            collective_id=2, has_side_effects=True, vmem_limit_bytes=67_000_000
        ),
    )(x, params, group, cum_row, cum_col, *saved)


def per_device(
    n_dp,
    n_tensor,
    inputs,
    cotangent,
    log_decay,
    query_weight,
    key_weight,
    value_weight,
    gate_weight,
    out_weight,
    group_gain,
    norm_gains,
    norm_biases,
    ffn_gate_weight,
    ffn_up_weight,
    ffn_down_weight,
):
    d = lax.axis_index("dp")
    t = lax.axis_index("tensor")
    z = (d // PAIR) % 2
    rest = [1 << i for i in range(2, n_dp.bit_length() - 1)] + [1]
    tokens, width = inputs.shape
    block = width // n_dp
    length = tokens * n_tensor
    head_k = query_weight.shape[1] // 2
    head_v = value_weight.shape[1] // 2
    hidden_dev = ffn_gate_weight.shape[1] // 2
    def swap_dp(value, bit):
        return lax.ppermute(value, "dp", [(i, i ^ bit) for i in range(n_dp)])

    def dp_of(p):
        out = (p & 1) * PAIR
        for k, bit in enumerate(rest):
            out = out + ((d // bit) % 2 ^ ((p >> (k + 1)) & 1)) * bit
        return out

    def position_of(q):
        out = (q // PAIR) & 1
        for k, bit in enumerate(rest):
            out = out + ((d // bit) % 2 ^ ((q // bit) & 1)) * (2 << k)
        return out

    def permuted(value):
        return jnp.concatenate(
            [lax.dynamic_slice_in_dim(value, dp_of(p) * block, block, 1) for p in range(n_dp)], axis=1
        )

    def natural(value):
        return jnp.concatenate(
            [lax.dynamic_slice_in_dim(value, position_of(q) * block, block, 1) for q in range(n_dp)], axis=1
        )

    def half(value, which, axis):
        size = value.shape[axis] // 2
        return lax.dynamic_slice_in_dim(value, which * size, size, axis)

    def ordered(mine, theirs):
        return jnp.where(z == 0, mine, theirs), jnp.where(z == 0, theirs, mine)

    def gather_small(value):
        got = swap_dp(value, PAIR)
        blocks = list(ordered(value, got))
        for bit in rest:
            more = swap_dp(jnp.stack(blocks), bit)
            blocks = blocks + [more[i] for i in range(len(blocks))]
        return blocks

    small = jnp.concatenate([norm_gains, norm_biases, group_gain], axis=1)
    small_blocks = gather_small(small)
    gains_float = jnp.concatenate([b[:, :block] for b in small_blocks], axis=1).astype(F32)
    biases_float = jnp.concatenate([b[:, block : 2 * block] for b in small_blocks], axis=1).astype(F32)
    group_stack = jnp.stack([lax.dynamic_index_in_dim(b[:, 2 * block :], z, 0, False) for b in small_blocks])
    group_float = jnp.concatenate(
        [lax.dynamic_index_in_dim(group_stack, position_of(q), 0, False) for q in range(n_dp)]
    ).astype(F32)[None]

    decay_mine = lax.dynamic_index_in_dim(log_decay, z, 0, True)
    decay_theirs = swap_dp(lax.dynamic_index_in_dim(log_decay, 1 - z, 0, True), PAIR)
    cumul = jnp.cumsum(jnp.concatenate([decay_mine, decay_theirs], axis=0), axis=1)
    chunk_of = [t ^ j for j in range(n_tensor)]
    cumul = jnp.concatenate([lax.dynamic_slice_in_dim(cumul, c * tokens, tokens, 1) for c in chunk_of], axis=1)

    def interleaved(first, second):
        parts = [half(first, 0, 1), half(second, 0, 1), half(first, 1, 1), half(second, 1, 1)]
        return jnp.concatenate(parts, axis=1)

    sources = [
        interleaved(query_weight, key_weight),
        value_weight,
        gate_weight,
        out_weight.T,
        ffn_gate_weight,
        ffn_up_weight,
        ffn_down_weight.T,
    ]

    inputs_perm, cot = permuted(inputs), permuted(cotangent)
    params = jnp.concatenate([gains_float, biases_float], axis=0)
    cum_col = cumul.reshape(-1, 1)
    saved = forward_call(n_dp, inputs_perm, cot, params, group_float, cumul, cum_col, sources)
    layer_perm, grad_perm, own, others, sums = backward_call(
        n_dp, inputs_perm, params, group_float, cumul, cum_col, saved
    )
    layer_out, input_grad = natural(layer_perm), natural(grad_perm)

    flips = [i % 2 == 0 for i in range(others.shape[1])]

    def total(g):
        mine = own[g].astype(F32)
        theirs = jnp.zeros_like(mine)
        for i, flipped in enumerate(flips):
            if flipped:
                theirs = theirs + others[g, i].astype(F32)
            else:
                mine = mine + others[g, i].astype(F32)
        return mine, theirs

    def both(mine, theirs, axis):
        first, second = ordered(mine, theirs)
        return jnp.concatenate([first, second], axis=axis)

    norm_both = sums[0, :4] + sums[1, :4]
    pieces = head_v // block
    group_both = both(sums[0, 4 : 4 + pieces].reshape(1, head_v), sums[1, 4 : 4 + pieces].reshape(1, head_v), 0)
    group_cols = head_v // n_dp
    group_gain_out = lax.dynamic_slice_in_dim(group_both, d * group_cols, group_cols, 1)
    norm_mine = lax.dynamic_slice_in_dim(norm_both, t * (block // n_tensor), block // n_tensor, 1)
    norm_gain_grad, norm_bias_grad = norm_mine[:2], norm_mine[2:]
    qk_mine, qk_theirs = total(QK)
    query_grad = both(qk_mine[:, :head_k], qk_theirs[:, :head_k], 1)
    key_grad = both(qk_mine[:, head_k:], qk_theirs[:, head_k:], 1)
    value_grad, gate_grad, ffn_gate_grad, ffn_up_grad = (both(*total(g), 1) for g in (V, G, FG, FU))
    out_weight_grad, ffn_down_grad = (both(*total(g), 1).T for g in (O, FD))
    return (
        layer_out,
        input_grad,
        query_grad,
        key_grad,
        value_grad,
        gate_grad,
        out_weight_grad,
        group_gain_out,
        norm_gain_grad,
        norm_bias_grad,
        ffn_gate_grad,
        ffn_up_grad,
        ffn_down_grad,
    )


def solution(mesh):
    tokens = P(("dp", "tensor"), None)
    rows, cols, norms = P("dp", "tensor"), P("tensor", "dp"), P(None, "dp")
    sums = P(None, ("dp", "tensor"))
    in_specs = (tokens, tokens, cols, rows, rows, rows, rows, cols, cols, norms, norms, rows, rows, cols)
    out_specs = (tokens, tokens, rows, rows, rows, rows, cols, cols, sums, sums, rows, rows, cols)
    body = functools.partial(per_device, mesh.shape["dp"], mesh.shape["tensor"])
    return jax.shard_map(body, mesh=mesh, in_specs=in_specs, out_specs=out_specs, check_vma=False)
```

```python
import functools
import math

import jax
import jax.numpy as jnp
from jax import lax
from jax.experimental import pallas as pl
from jax.experimental.pallas import tpu as pltpu
from jax.sharding import PartitionSpec as P

EPSILON = 1e-05
GROUP_FLOOR = 1.0
BF = jnp.bfloat16
F32 = jnp.float32
PAIR = 2
MESH = pl.DeviceIdType.MESH
QK, V, G, O, FG, FU, FD = range(7)
GROUPS = 7


def dot_nn(a, b):
    return lax.dot_general(a, b, (((1,), (0,)), ((), ())), preferred_element_type=F32)


def dot_nt(a, b):
    return lax.dot_general(a, b, (((1,), (1,)), ((), ())), preferred_element_type=F32)


def dot_tn(a, b):
    return lax.dot_general(a, b, (((0,), (0,)), ((), ())), preferred_element_type=F32)


def flip(index, bit):
    return index + bit - 2 * bit * ((index // bit) % 2)


class Place:
    def __init__(self, n_dp):
        self.n_dp = n_dp
        self.d = lax.axis_index("dp")
        self.t = lax.axis_index("tensor")
        self.z = (self.d // PAIR) % 2
        self.rest = [1 << i for i in range(2, n_dp.bit_length() - 1)] + [1]
        self.inner = self.rest[:-1]
        self.masks = []
        for pick in range(1, 1 << (1 + len(self.inner))):
            bits = [PAIR] * (pick & 1) + [b for k, b in enumerate(self.inner) if (pick >> (k + 1)) & 1]
            self.masks.append((bits, pick & ~1, pick & 1))
        half = n_dp // 2
        self.pairs = self.masks + [([1], half, 0)] + [(bits + [1], above + half, flips) for bits, above, flips in self.masks]

    def slot(self, above, flips):
        return next((j for j, pair in enumerate(self.pairs) if pair[1:] == (above, flips)), None)

    def dp_of(self, p):
        out = (p & 1) * PAIR
        for k, bit in enumerate(self.rest):
            here = (self.d // bit) % 2
            out = out + (1 - here if (p >> (k + 1)) & 1 else here) * bit
        return out

    def peer(self, bits):
        out = self.d
        for bit in bits:
            out = flip(out, bit)
        return {"dp": out}

    def x_peer(self):
        return {"dp": flip(self.d, 1)}

    def z_peer(self):
        return {"dp": flip(self.d, PAIR)}

    def y_peer(self):
        return {"tensor": flip(self.t, 2)}

    def c_peer(self):
        return {"tensor": flip(self.t, 1)}

    def everyone(self, far):
        near = [self.x_peer(), self.y_peer(), self.c_peer()]
        if far:
            return near[1:] + [self.peer(bits) for bits, _, _ in self.pairs]
        return near + [self.peer(bits) for bits, _, _ in self.masks]


def entry_barrier(place, far=False):
    barrier = pltpu.get_barrier_semaphore()
    peers = place.everyone(far)
    for peer in peers:
        pl.semaphore_signal(barrier, inc=1, device_id=peer, device_id_type=MESH)
    pl.semaphore_wait(barrier, len(peers))


def column_copies(place, src, dst, sem, block, back=False):
    if block % 128:
        return [pltpu.make_async_copy(src, dst, sem)]
    out = []
    for p in range(place.n_dp):
        natural = pl.ds(pl.multiple_of(place.dp_of(p) * block, block), block)
        here = pl.ds(p * block, block)
        a, b = (here, natural) if back else (natural, here)
        out.append(pltpu.make_async_copy(src.at[:, a], dst.at[:, b], sem))
    return out


def remote(src, dst, send, recv, peer):
    return pltpu.make_async_remote_copy(
        src_ref=src, dst_ref=dst, send_sem=send, recv_sem=recv, device_id=peer, device_id_type=MESH
    )


class Weights:
    def __init__(self, place, sources, full, sems):
        self.place, self.sources, self.full = place, sources, full
        self.z_send, self.z_recv, self.x_send, self.x_recv, self.local = sems
        self.block = sources[0].shape[0]
        self.cols = sources[0].shape[1] // 2
        self.half = place.n_dp // 2

    def rows(self, position, count=1):
        return pl.ds(pl.multiple_of(position * self.block, self.block), count * self.block)

    def source(self, g, half):
        return self.sources[g].at[:, pl.ds(pl.multiple_of(half * self.cols, self.cols), self.cols)]

    def start(self, g):
        place = self.place
        z = place.z
        own = pltpu.make_async_copy(self.source(g, z), self.full.at[g, self.rows(z), :], self.local.at[g])
        own.start()
        remote(
            self.source(g, z),
            self.full.at[g, self.rows(z + self.half), :],
            self.x_send.at[g],
            self.x_recv.at[g],
            place.x_peer(),
        ).start()
        for i, (bits, above, flips) in reversed(list(enumerate(place.masks))):
            half = 1 - z if flips else z
            remote(
                self.source(g, half),
                self.full.at[g, self.rows(z + above), :],
                self.z_send.at[g],
                self.z_recv.at[g, i],
                place.peer(bits),
            ).start()

    def forward(self, g, i):
        place = self.place
        bits, above, flips = place.masks[i]
        position = (1 - place.z if flips else place.z) + above
        here = self.full.at[g, self.rows(position), :]
        remote(here, here, self.z_send.at[g], self.z_recv.at[g, i], place.peer(bits)).wait_recv()
        remote(
            here,
            self.full.at[g, self.rows(position + self.half), :],
            self.x_send.at[g],
            self.x_recv.at[g],
            place.x_peer(),
        ).start()

    def forward_all(self, g):
        for i in range(len(self.place.masks)):
            self.forward(g, i)

    def finish(self, g):
        z = self.place.z
        pltpu.make_async_copy(self.source(g, z), self.full.at[g, self.rows(z), :], self.local.at[g]).wait()
        there = self.full.at[g, self.rows(self.half, self.half), :]
        remote(there, there, self.x_send.at[g], self.x_recv.at[g], self.place.x_peer()).wait_recv()

    def sent(self, g):
        there = self.full.at[g, self.rows(self.half, self.half), :]
        remote(there, there, self.x_send.at[g], self.x_recv.at[g], self.place.x_peer()).wait_send()
        count = self.half - 1
        those = self.full.at[g, self.rows(0, count), :]
        remote(those, those, self.z_send.at[g], self.z_recv.at[g, 0], self.place.x_peer()).wait_send()


class Gather:
    def __init__(self, place, buffer, send, recv):
        self.place, self.buffer = place, buffer
        self.send, self.recv = send, recv
        self.tokens = buffer.shape[0] // 8
        self.peers = {1: place.c_peer(), 2: place.y_peer(), 4: place.z_peer()}

    def slot(self, s):
        return self.buffer.at[pl.ds(pl.multiple_of(s * self.tokens, self.tokens), self.tokens), :]

    def copy(self, source, bit, src=None):
        s = source + bit
        return remote(self.slot(source) if src is None else src, self.slot(s), self.send.at[s - 1], self.recv.at[s - 1], self.peers[bit])

    def start(self, src=None):
        for bit in (4, 2, 1):
            self.copy(0, bit, src).start()

    def from_z(self):
        self.copy(0, 4).wait_recv()
        self.copy(4, 2).start()
        self.copy(4, 1).start()

    def from_y(self):
        self.copy(0, 2).wait_recv()
        self.copy(2, 1).start()

    def from_zy(self):
        self.copy(4, 2).wait_recv()
        self.copy(6, 1).start()

    def chip(self, source):
        self.copy(source, 1).wait_recv()

    def sent(self, src=None):
        self.copy(0, 4, src).wait_send()
        self.copy(0, 2, src).wait_send()
        self.copy(0, 1, src).wait_send()
        self.copy(4, 2).wait_send()
        self.copy(4, 1).wait_send()
        self.copy(2, 1).wait_send()
        self.copy(6, 1).wait_send()


class Scatter:
    def __init__(self, place, keep, c_out, c_in, far_out, far_in, sems):
        self.place = place
        self.keep, self.c_out, self.c_in, self.far_out, self.far_in = keep, c_out, c_in, far_out, far_in
        self.c_send, self.c_recv, self.far_send, self.far_recv = sems
        self.tokens = c_out.shape[1]

    def part(self, b, value):
        self.keep[b] = value[: self.tokens].astype(self.keep.dtype)
        self.c_out[b] = value[self.tokens :].astype(BF)
        self.c_copy(b).start()

    def c_copy(self, b):
        return remote(self.c_out.at[b], self.c_in.at[b], self.c_send.at[b], self.c_recv.at[b], self.place.c_peer())

    def far_copy(self, b):
        peer = self.place.z_peer() if b == 2 else self.place.y_peer()
        return remote(
            self.far_source(b), self.far_in.at[b - 1], self.far_send.at[b - 1], self.far_recv.at[b - 1], peer
        )

    def far_source(self, b):
        return self.keep.at[b] if self.far_out is None else self.far_out.at[b - 1]

    def rows(self, body, step=16):
        def loop(i, carry):
            body(pl.ds(pl.multiple_of(i * step, step), step))
            return carry

        lax.fori_loop(0, self.tokens // step, loop, 0)

    def pass_on(self, b):
        self.c_copy(b).wait_recv()
        if b == 2:
            self.far_copy(3).wait_recv()

        def body(r):
            total = self.keep[b, r, :].astype(F32) + self.c_in[b, r, :].astype(F32)
            if b == 2:
                total = total + self.far_in[2, r, :].astype(F32)
            self.far_source(b)[r, :] = total.astype(BF)

        self.rows(body)
        self.far_copy(b).start()

    def wait_own(self):
        self.c_copy(0).wait_recv()
        self.far_copy(1).wait_recv()
        self.far_copy(2).wait_recv()

    def own(self, r):
        return (
            self.keep[0, r, :].astype(F32)
            + self.c_in[0, r, :].astype(F32)
            + self.far_in[0, r, :].astype(F32)
            + self.far_in[1, r, :].astype(F32)
        )

    def sent(self):
        for b in range(4):
            self.c_copy(b).wait_send()
        for b in (3, 2, 1):
            self.far_copy(b).wait_send()


def normalized(value):
    center = value - jnp.mean(value, axis=-1, keepdims=True)
    spread = jnp.mean(center * center, axis=-1, keepdims=True)
    return center * lax.rsqrt(spread + EPSILON)


def decay_tile(t, cumul_rows, cumul_here, first, rows, length, tokens):
    square = (rows, rows)
    same = lax.broadcasted_iota(jnp.int32, square, 0) == lax.broadcasted_iota(jnp.int32, square, 1)
    cumul_cols = jnp.sum(jnp.where(same, cumul_here, 0.0), axis=1, keepdims=True)
    index = lax.broadcasted_iota(jnp.int32, (rows, length), 0) + first
    other = lax.broadcasted_iota(jnp.int32, (rows, length), 1)
    at = ((index // tokens) ^ t) * tokens + index % tokens
    to = ((other // tokens) ^ t) * tokens + other % tokens
    causal = at >= to
    return jnp.where(causal, jnp.exp(jnp.where(causal, cumul_cols - cumul_rows, 0.0)), 0.0)


def spread_small(place, own, others, params, group, cumul, block):
    pieces = group.shape[1] // block
    steps = cumul.shape[1] // block
    first = place.z == 0

    def of(above, flips, rows):
        j = place.slot(above, flips)
        return own[rows, :] if j is None else others[j, rows, :]

    head = slice(0, 4)
    for p in range(place.n_dp):
        same, flipped = of(p & ~1, 0, head), of(p & ~1, 1, head)
        params[head, p * block : (p + 1) * block] = jnp.where(place.z == p % 2, same, flipped)

    def head_rows(above, flips, at, count):
        one = of(above, flips, slice(at, at + count))
        two = of(above, flips, slice(at + count, at + 2 * count))
        return jnp.where(first, one, two)

    total = head_rows(0, 0, 4, pieces)
    for bits, above, flips in place.pairs:
        total = total + head_rows(above, flips, 4, pieces)
    for k in range(pieces):
        group[0:1, k * block : (k + 1) * block] = total[k : k + 1, :]
    at = 4 + 2 * pieces
    for row, flips in ((0, 0), (1, 1)):
        value = head_rows(0, flips, at, steps)
        for k in range(steps):
            cumul[row : row + 1, k * block : (k + 1) * block] = value[k : k + 1, :]


def forward_kernel(
    n_dp,
    x_hbm,
    cot_hbm,
    small_ref,
    s_qk,
    s_v,
    s_g,
    s_o,
    s_fg,
    s_fu,
    s_fd,
    w_out,
    normed_out,
    qkv_out,
    gate_out,
    mixed_out,
    ffn_in_out,
    hidden_out,
    grads_out,
    cot_out,
    middle_out,
    params_out,
    group_out,
    cumul_out,
    small_in,
    params_ref,
    group_ref,
    cum_row_ref,
    x_ref,
    w,
    normed_all,
    cot_all,
    ffn_in,
    qkv,
    gate_in,
    mixed,
    gated,
    gate_hidden,
    up_hidden,
    hidden,
    grads,
    middle,
    keep,
    c_out,
    c_in,
    far_out,
    far_in,
    z_send,
    z_recv,
    x_send,
    x_recv,
    w_local,
    ag_send,
    ag_recv,
    c_send,
    c_recv,
    far_send,
    far_recv,
    out_sem,
    small_send,
    small_recv,
):
    place = Place(n_dp)
    tokens, width = x_ref.shape
    block = width // n_dp
    rows_all = 8 * tokens
    length = rows_all // 2
    head_k = qkv.shape[1] // 4
    scale = 1.0 / math.sqrt(head_k)
    tile = 2 * tokens
    weights = Weights(place, [s_qk, s_v, s_g, s_o, s_fg, s_fu, s_fd], w, (z_send, z_recv, x_send, x_recv, w_local))
    ag_normed = Gather(place, normed_all, ag_send.at[0], ag_recv.at[0])
    ag_cot = Gather(place, cot_all, ag_send.at[1], ag_recv.at[1])
    ag_two = Gather(place, ffn_in, ag_send.at[2], ag_recv.at[2])
    branch = Scatter(place, keep, c_out, c_in, far_out, far_in, (c_send, c_recv, far_send, far_recv))
    outs = []

    def save(src, dst, index):
        copy = pltpu.make_async_copy(src, dst, out_sem.at[index])
        copy.start()
        outs.append(copy)

    def over(count, step, body):
        def loop(i, carry):
            body(pl.ds(pl.multiple_of(i * step, step), step), i)
            return carry

        lax.fori_loop(0, count // step, loop, 0)

    for copy in column_copies(place, x_hbm, x_ref, out_sem.at[16], block):
        copy.start()
    for copy in column_copies(place, cot_hbm, ag_cot.slot(0), out_sem.at[17], block):
        copy.start()
    entry_barrier(place, True)
    small = []
    for j, (bits, above, flips) in enumerate(place.pairs):
        copy = remote(small_ref, small_in.at[j], small_send.at[j], small_recv.at[j], place.peer(bits))
        copy.start()
        small.append(copy)
    weights.start(QK)
    pltpu.make_async_copy(x_hbm, x_ref, out_sem.at[16]).wait()
    for copy in small:
        copy.wait()
    spread_small(place, small_ref, small_in, params_ref, group_ref, cum_row_ref, block)

    def first_norm(r, i):
        value = normalized(x_ref[r, :].astype(F32))
        normed_all[r, :] = (value * params_ref[0:1, :] + params_ref[2:3, :]).astype(BF)

    over(tokens, 16, first_norm)
    ag_normed.start()
    save(params_ref, params_out, 18)
    save(group_ref, group_out, 19)
    save(cum_row_ref, cumul_out, 20)
    pltpu.make_async_copy(cot_hbm, ag_cot.slot(0), out_sem.at[17]).wait()
    weights.start(V)
    weights.start(G)
    weights.forward_all(QK)
    ag_normed.from_z()
    ag_normed.from_y()
    ag_cot.start()
    weights.start(O)
    ag_normed.from_zy()
    for s in (0, 2, 4, 6):
        ag_normed.chip(s)
    save(normed_all, normed_out, 0)
    weights.finish(QK)

    def make_qk(r, i):
        qkv[r, : 2 * head_k] = dot_nn(normed_all[r, :], w[QK]).astype(BF)

    over(rows_all, tile, make_qk)
    save(w.at[QK], w_out.at[QK], 1)
    weights.start(FG)
    weights.forward_all(V)
    weights.finish(V)

    def make_v(r, i):
        qkv[r, 2 * head_k :] = dot_nn(normed_all[r, :], w[V]).astype(BF)

    over(rows_all, tile, make_v)
    save(w.at[V], w_out.at[V], 2)
    save(qkv, qkv_out, 3)
    weights.start(FU)

    def retention(r, i):
        start = pl.multiple_of((i // 2) * length, length)
        seq = pl.ds(start, length)
        scores = dot_nt(qkv[r, :head_k], qkv[seq, head_k : 2 * head_k])
        here = cum_row_ref[pl.ds(i // 2, 1), pl.ds(pl.multiple_of((i % 2) * tile, tile), tile)]
        decays = decay_tile(
            place.t, cum_row_ref[pl.ds(i // 2, 1), :], here, (i % 2) * tile, tile, length, tokens
        )
        weighted = (scores * decays * scale).astype(BF)
        mixed[r, :] = dot_nn(weighted, qkv[seq, 2 * head_k :])

    over(rows_all, tile, retention)
    save(mixed, mixed_out, 4)
    weights.forward_all(G)
    ag_cot.from_z()
    ag_cot.from_y()
    weights.finish(G)

    def gating(r, i):
        gate = dot_nn(normed_all[r, :], w[G])
        gate_in[r, :] = gate
        value = mixed[r, :]
        center = value - jnp.mean(value, axis=-1, keepdims=True)
        spread = jnp.mean(center * center, axis=-1, keepdims=True)
        flat = center * lax.rsqrt(jnp.maximum(spread, GROUP_FLOOR)) * group_ref[...]
        gated[r, :] = (flat * (gate * lax.logistic(gate))).astype(BF)

    over(rows_all, tile, gating)
    save(w.at[G], w_out.at[G], 5)
    save(gate_in, gate_out, 6)
    weights.forward_all(O)
    ag_cot.from_zy()
    weights.finish(O)

    def branch_part(i, carry):
        r = pl.ds(pl.multiple_of((3 - i) * tile, tile), tile)
        branch.part(3 - i, dot_nt(gated[r, :], w[O]))
        return carry

    lax.fori_loop(0, 4, branch_part, 0)
    save(w.at[O], w_out.at[O], 7)
    branch.pass_on(3)
    branch.pass_on(1)
    for s in (0, 2, 4, 6):
        ag_cot.chip(s)
    save(cot_all, cot_out, 8)
    weights.forward_all(FG)
    branch.pass_on(2)
    weights.start(FD)
    weights.forward(FU, 0)
    branch.wait_own()

    def second_norm(r, i):
        value = x_ref[r, :].astype(F32) + branch.own(r)
        middle[r, :] = value
        ffn_in[r, :] = (normalized(value) * params_ref[1:2, :] + params_ref[3:4, :]).astype(BF)

    over(tokens, 16, second_norm)
    ag_two.start()
    save(middle, middle_out, 9)
    for i in range(1, len(place.masks)):
        weights.forward(FU, i)
    weights.finish(FG)
    weights.finish(FU)

    def feed(b):
        r = pl.ds(pl.multiple_of(b * tile, tile), tile)
        gate = dot_nn(ffn_in[r, :], w[FG])
        up = dot_nn(ffn_in[r, :], w[FU])
        gate_hidden[r, :] = gate
        up_hidden[r, :] = up
        hidden[r, :] = (gelu(gate) * up).astype(BF)

    ag_two.from_z()
    ag_two.from_y()

    def feed_chips(b, carry):
        ag_two.chip(2 * b)
        feed(b)
        return carry

    lax.fori_loop(0, 3, feed_chips, 0)
    weights.forward(FD, len(place.masks) - 1)
    ag_two.from_zy()
    lax.fori_loop(3, 4, feed_chips, 0)
    save(w.at[FG], w_out.at[FG], 10)
    save(w.at[FU], w_out.at[FU], 11)
    save(ffn_in, ffn_in_out, 12)
    save(hidden, hidden_out, 13)
    for i in reversed(range(len(place.masks) - 1)):
        weights.forward(FD, i)
    weights.finish(FD)
    save(w.at[FD], w_out.at[FD], 14)
    size = gate_hidden.shape[1]

    def feed_back(r, i):
        back = dot_nn(cot_all[r, :], w[FD])
        gate = gate_hidden[r, :]
        value, slope = gelu_and_slope(gate)
        grads[r, :size] = (back * up_hidden[r, :] * slope).astype(BF)
        grads[r, size:] = (back * value).astype(BF)

    over(rows_all, tile, feed_back)
    save(grads, grads_out, 15)
    for copy in outs:
        copy.wait()
    for g in range(GROUPS):
        weights.sent(g)
    ag_normed.sent()
    ag_cot.sent()
    ag_two.sent()
    branch.sent()


ROOT = math.sqrt(2.0 / math.pi)


def gelu(v):
    return 0.5 * v * (1.0 + jnp.tanh(ROOT * (v + 0.044715 * v * v * v)))


def gelu_and_slope(v):
    inside = jnp.tanh(ROOT * (v + 0.044715 * v * v * v))
    slope = 0.5 * (1.0 + inside) + 0.5 * v * (1.0 - inside * inside) * ROOT * (1.0 + 3 * 0.044715 * v * v)
    return 0.5 * v * (1.0 + inside), slope


def forward_call(n_dp, x, cot, small, sources):
    tokens, width = x.shape
    length = 4 * tokens
    rows_all = 8 * tokens
    cols = sources[0].shape[1] // 2
    masks = n_dp // 2 - 1
    vmem, hbm = pl.BlockSpec(memory_space=pltpu.VMEM), pl.BlockSpec(memory_space=pl.ANY)
    shape = jax.ShapeDtypeStruct
    outs = (
        shape((GROUPS, width, cols), BF),
        shape((rows_all, width), BF),
        shape((rows_all, 2 * cols), BF),
        shape((rows_all, cols), F32),
        shape((rows_all, cols), F32),
        shape((rows_all, width), BF),
        shape((rows_all, cols), BF),
        shape((rows_all, 2 * cols), BF),
        shape((rows_all, width), BF),
        shape((tokens, width), F32),
        shape((8, width), F32),
        shape((1, cols), F32),
        shape((2, length), F32),
    )
    dma = pltpu.SemaphoreType.DMA
    scratch = [
        pltpu.VMEM((n_dp - 1, *small.shape), F32),
        pltpu.VMEM((8, width), F32),
        pltpu.VMEM((1, cols), F32),
        pltpu.VMEM((2, length), F32),
        pltpu.VMEM((tokens, width), BF),
        pltpu.VMEM((GROUPS, width, cols), BF),
        pltpu.VMEM((rows_all, width), BF),
        pltpu.VMEM((rows_all, width), BF),
        pltpu.VMEM((rows_all, width), BF),
        pltpu.VMEM((rows_all, 2 * cols), BF),
        pltpu.VMEM((rows_all, cols), F32),
        pltpu.VMEM((rows_all, cols), F32),
        pltpu.VMEM((rows_all, cols), BF),
        pltpu.VMEM((rows_all, cols), F32),
        pltpu.VMEM((rows_all, cols), F32),
        pltpu.VMEM((rows_all, cols), BF),
        pltpu.VMEM((rows_all, 2 * cols), BF),
        pltpu.VMEM((tokens, width), F32),
        pltpu.VMEM((4, tokens, width), F32),
        pltpu.VMEM((4, tokens, width), BF),
        pltpu.VMEM((4, tokens, width), BF),
        pltpu.VMEM((3, tokens, width), BF),
        pltpu.VMEM((3, tokens, width), BF),
        dma((GROUPS,)),
        dma((GROUPS, masks)),
        dma((GROUPS,)),
        dma((GROUPS,)),
        dma((GROUPS,)),
        dma((3, 7)),
        dma((3, 7)),
        dma((4,)),
        dma((4,)),
        dma((3,)),
        dma((3,)),
        dma((21,)),
        dma((n_dp - 1,)),
        dma((n_dp - 1,)),
    ]
    return pl.pallas_call(
        functools.partial(forward_kernel, n_dp),
        out_shape=outs,
        in_specs=[hbm, hbm, vmem] + [hbm] * GROUPS,
        out_specs=(hbm,) * len(outs),
        scratch_shapes=scratch,
        compiler_params=pltpu.CompilerParams(
            collective_id=1, has_side_effects=True, vmem_limit_bytes=64_000_000
        ),
    )(x, cot, small, *sources)


class Reduce:
    def __init__(self, place, keep, x_out, x_in, z_in, own_out, sems, own_sem):
        self.place = place
        self.keep, self.x_out, self.x_in, self.z_in, self.own_out = keep, x_out, x_in, z_in, own_out
        self.x_send, self.x_recv, self.z_send, self.z_recv = sems
        self.own_sem = own_sem
        self.block = z_in.shape[2]
        self.half = place.n_dp // 2
        z = place.z
        self.targets = [
            ((1 - z if flips else z) + above, i, place.peer(bits)) for i, (bits, above, flips) in enumerate(place.masks)
        ]
        self.targets.reverse()

    def rows(self, position):
        return pl.ds(pl.multiple_of(position * self.block, self.block), self.block)

    def x_copy(self, g, ring, position):
        return remote(
            self.x_out.at[ring, self.rows(position), :],
            self.x_in.at[g, self.rows(position), :],
            self.x_send.at[g],
            self.x_recv.at[g, position],
            self.place.x_peer(),
        )

    def z_copy(self, g, position, i, peer):
        return remote(
            self.keep.at[g, self.rows(position), :],
            self.z_in.at[g, i],
            self.z_send.at[g],
            self.z_recv.at[g, i],
            peer,
        )

    def upper(self, g, ring, left, right, col, step):
        width = left.shape[1] // 2
        cols = self.keep.shape[2]

        def body(i, carry):
            at = pl.multiple_of(i * step, step)
            value = dot_tn(left[:, pl.ds(pl.multiple_of(width + at, step), step)], right[:, col : col + cols])
            self.x_out[ring, pl.ds(at, step), :] = value.astype(BF)
            return carry

        lax.fori_loop(0, width // step, body, 0)
        for position, _, _ in self.targets:
            self.x_copy(g, ring, position).start()
        self.x_copy(g, ring, self.place.z).start()

    def lower(self, g, left, right, col, step):
        width = left.shape[1] // 2
        cols = self.keep.shape[2]

        def body(i, carry):
            at = pl.ds(pl.multiple_of(i * step, step), step)
            self.keep[g, at, :] = dot_tn(left[:, at], right[:, col : col + cols]).astype(BF)
            return carry

        lax.fori_loop(0, width // step, body, 0)

    def x_sent(self, g, ring):
        whole = self.x_out.at[ring]
        remote(whole, whole, self.x_send.at[g], self.x_recv.at[g, 0], self.place.x_peer()).wait_send()

    def add(self, g, ring, position):
        self.x_copy(g, ring, position).wait_recv()
        step = min(64, self.block)

        def body(i, carry):
            r = pl.ds(pl.multiple_of(position * self.block + i * step, step), step)
            self.keep[g, r, :] = (self.keep[g, r, :].astype(F32) + self.x_in[g, r, :].astype(F32)).astype(BF)
            return carry

        lax.fori_loop(0, self.block // step, body, 0)

    def own_copy(self, g):
        return pltpu.make_async_copy(
            self.keep.at[g, self.rows(self.place.z), :], self.own_out.at[g], self.own_sem.at[g]
        )

    def pass_on(self, g, ring):
        for position, i, peer in self.targets:
            self.add(g, ring, position)
            self.z_copy(g, position, i, peer).start()
        self.add(g, ring, self.place.z)
        self.own_copy(g).start()

    def finish(self, g):
        self.own_copy(g).wait()
        for position, i, peer in self.targets:
            self.z_copy(g, position, i, peer).wait()


def norm_back(value, grad, gain):
    center = value - jnp.mean(value, axis=-1, keepdims=True)
    spread = jnp.mean(center * center, axis=-1, keepdims=True)
    r = lax.rsqrt(spread + EPSILON)
    hat = center * r
    scaled = grad * gain
    back = r * (
        scaled - jnp.mean(scaled, axis=-1, keepdims=True) - hat * jnp.mean(scaled * hat, axis=-1, keepdims=True)
    )
    return back, jnp.sum(grad * hat, axis=0, keepdims=True), jnp.sum(grad, axis=0, keepdims=True)


def backward_kernel(
    n_dp,
    x_hbm,
    params_ref,
    group_ref,
    cum_row_ref,
    w_ref,
    normed_ref,
    qkv_ref,
    gate_ref,
    mixed_ref,
    ffn_in_ref,
    hidden_ref,
    grads_ref,
    cot_ref,
    middle_ref,
    layer_out,
    input_grad_out,
    own_out,
    z_in,
    sums_out,
    w,
    tokens_a,
    ffn_in,
    branch_all,
    slim,
    qkv,
    gate_in,
    mixed,
    gated,
    x_ref,
    middle,
    grad_middle,
    sums,
    sums_in,
    group_sum,
    payload,
    payload_in,
    keep,
    c_out,
    c_in,
    far_in,
    c_in_two,
    far_in_two,
    dw_keep,
    x_out,
    x_in,
    ag_send,
    ag_recv,
    c_send,
    c_recv,
    far_send,
    far_recv,
    x_send,
    x_recv,
    z_send,
    z_recv,
    load_sem,
    own_sem,
    sum_send,
    sum_recv,
    pay_send,
    pay_recv,
):
    place = Place(n_dp)
    tokens, width = x_ref.shape
    rows_all = 8 * tokens
    length = rows_all // 2
    cols = gated.shape[1]
    head_k = cols // 2
    scale = 1.0 / math.sqrt(head_k)
    tile = 2 * tokens
    step = min(512, width // 2)
    block = z_in.shape[2]
    ag = Gather(place, branch_all, ag_send, ag_recv)

    def scatter(k, c, far):
        return Scatter(place, keep, c_out, c, None, far, (c_send.at[k], c_recv.at[k], far_send.at[k], far_recv.at[k]))

    rs_two = scatter(0, c_in, far_in)
    rs_out = scatter(1, c_in_two, far_in_two)
    rs_one = scatter(2, c_in, far_in)
    dw = Reduce(place, dw_keep, x_out, x_in, z_in, own_out, (x_send, x_recv, z_send, z_recv), own_sem)
    result = ffn_in.at[:tokens, :]
    weighted = ffn_in.at[tokens : tokens + length, :length]
    score_back = ffn_in.at[tokens : tokens + length, length : 2 * length]
    ring = {FD: 0, FG: 1, FU: 2, O: 3, QK: 0, V: 1, G: 2}

    def load(src, dst, index):
        copy = pltpu.make_async_copy(src, dst, load_sem.at[index])
        copy.start()
        return copy

    def over(count, size, body):
        def loop(i, carry):
            body(pl.ds(pl.multiple_of(i * size, size), size), i)
            return carry

        lax.fori_loop(0, count // size, loop, 0)

    in_cot = load(cot_ref, tokens_a, 3)
    in_hidden = load(hidden_ref, slim.at[:, 2 * cols :], 4)
    in_grads = load(grads_ref, slim.at[:, : 2 * cols], 0)
    in_fg = load(w_ref.at[FG], w.at[0], 1)
    in_fu = load(w_ref.at[FU], w.at[1], 2)
    in_ffn = load(ffn_in_ref, ffn_in, 5)
    in_middle = load(middle_ref, middle, 6)
    in_mixed = load(mixed_ref, mixed, 7)
    in_gate = load(gate_ref, gate_in, 8)
    in_o = load(w_ref.at[O], w.at[2], 9)
    in_qkv = load(qkv_ref, qkv, 10)
    for copy in column_copies(place, x_hbm, x_ref, load_sem.at[11], block):
        copy.start()
    sums[...] = jnp.zeros_like(sums)
    group_sum[...] = jnp.zeros_like(group_sum)
    entry_barrier(place, True)
    in_cot.wait()
    in_hidden.wait()
    dw.upper(FD, ring[FD], tokens_a, slim, 2 * cols, step)
    in_grads.wait()
    in_fg.wait()
    in_fu.wait()

    def rows_of(i):
        return 3 - i, pl.ds(pl.multiple_of((3 - i) * tile, tile), tile)

    def two_part(i, carry):
        b, r = rows_of(i)
        rs_two.part(b, dot_nt(slim[r, :cols], w[0]) + dot_nt(slim[r, cols : 2 * cols], w[1]))
        return carry

    lax.fori_loop(0, 4, two_part, 0)
    in_fd = load(w_ref.at[FD], w.at[0], 1)
    in_qk = load(w_ref.at[QK], w.at[1], 2)
    rs_two.pass_on(3)
    rs_two.pass_on(1)
    in_ffn.wait()
    dw.upper(FG, ring[FG], ffn_in, slim, 0, step)
    dw.upper(FU, ring[FU], ffn_in, slim, cols, step)
    dw.lower(FD, tokens_a, slim, 2 * cols, step)
    dw.lower(FG, ffn_in, slim, 0, step)
    rs_two.pass_on(2)
    dw.lower(FU, ffn_in, slim, cols, step)
    in_mixed.wait()
    in_gate.wait()

    def gating(r, i):
        value = mixed[r, :]
        center = value - jnp.mean(value, axis=-1, keepdims=True)
        spread = jnp.mean(center * center, axis=-1, keepdims=True)
        gate = gate_in[r, :]
        flat = center * lax.rsqrt(jnp.maximum(spread, GROUP_FLOOR)) * group_ref[...]
        gated[r, :] = (flat * (gate * lax.logistic(gate))).astype(BF)

    over(rows_all, tokens, gating)
    in_middle.wait()
    rs_two.wait_own()

    def second_back(r, i):
        back, gain_sum, bias_sum = norm_back(middle[r, :], rs_two.own(r), params_ref[1:2, :])
        total = tokens_a[r, :].astype(F32) + back
        grad_middle[r, :] = total
        branch_all[r, :] = total.astype(BF)
        sums[1:2, :] += gain_sum
        sums[3:4, :] += bias_sum

    over(tokens, 16, second_back)
    ag.start()
    in_normed = load(normed_ref, tokens_a, 3)
    rs_two.sent()
    in_fd.wait()
    dw.pass_on(FD, ring[FD])

    def out_part(i, carry):
        b, r = rows_of(i)
        rs_out.part(b, dot_nt(slim[r, 2 * cols :], w[0]))
        return carry

    lax.fori_loop(0, 4, out_part, 0)
    in_v = load(w_ref.at[V], w.at[0], 1)
    ag.from_z()
    ag.from_y()
    rs_out.pass_on(3)
    rs_out.pass_on(1)
    in_o.wait()
    in_qkv.wait()

    def gating_back(b):
        r = pl.ds(pl.multiple_of(b * tile, tile), tile)
        back = dot_nn(branch_all[r, :], w[2])
        value = mixed[r, :]
        center = value - jnp.mean(value, axis=-1, keepdims=True)
        spread = jnp.mean(center * center, axis=-1, keepdims=True)
        inverse = lax.rsqrt(jnp.maximum(spread, GROUP_FLOOR))
        hat = center * inverse
        gate = gate_in[r, :]
        sigmoid = lax.logistic(gate)
        flat = hat * group_ref[...]
        slope = sigmoid * (1.0 + gate * (1.0 - sigmoid))
        slim[r, 2 * cols :] = (back * flat * slope).astype(BF)
        grad = back * (gate * sigmoid)
        group_sum[...] += jnp.sum(grad * hat, axis=0, keepdims=True)
        scaled = grad * group_ref[...]
        live = jnp.where(spread > GROUP_FLOOR, 1.0, jnp.where(spread == GROUP_FLOOR, 0.5, 0.0))
        moment = jnp.mean(scaled * hat, axis=-1, keepdims=True) * live
        mixed_back = inverse * (scaled - jnp.mean(scaled, axis=-1, keepdims=True) - hat * moment)
        slim[r, cols : 2 * cols] = mixed_back.astype(BF)

    def sequence_back(s):
        seq = pl.ds(pl.multiple_of(s * length, length), length)

        def body(i, carry):
            r = pl.ds(pl.multiple_of(s * length + i * tile, tile), tile)
            at = pl.ds(pl.multiple_of(i * tile, tile), tile)
            scores = dot_nt(qkv[r, :head_k], qkv[seq, head_k : 2 * head_k])
            here = cum_row_ref[pl.ds(s, 1), at]
            decays = decay_tile(
                place.t, cum_row_ref[pl.ds(s, 1), :], here, i * tile, tile, length, tokens
            )
            weighted[at, :] = (scores * decays * scale).astype(BF)
            back = dot_nt(slim[r, cols : 2 * cols], qkv[seq, 2 * head_k :])
            grad = (back * decays * scale).astype(BF)
            score_back[at, :] = grad
            slim[r, :head_k] = dot_nn(grad, qkv[seq, head_k : 2 * head_k]).astype(BF)
            return carry

        lax.fori_loop(0, length // tile, body, 0)
        slim[seq, head_k : 2 * head_k] = dot_tn(score_back[...], qkv[seq, :head_k]).astype(BF)
        slim[seq, cols : 2 * cols] = dot_tn(weighted[...], slim[seq, cols : 2 * cols]).astype(BF)


    def gating_chips(b, carry):
        ag.chip(2 * b)
        gating_back(b)
        return carry

    lax.fori_loop(0, 2, gating_chips, 0)
    dw.pass_on(FG, ring[FG])
    ag.from_zy()
    lax.fori_loop(2, 4, gating_chips, 0)
    in_g = load(w_ref.at[G], w.at[2], 9)
    dw.upper(O, ring[O], branch_all, gated, 0, step)

    def sequences(s, carry):
        sequence_back(s)
        return carry

    lax.fori_loop(0, 2, sequences, 0)
    in_normed.wait()
    dw.x_sent(FD, ring[FD])
    dw.upper(QK, ring[QK], tokens_a, slim, 0, step)
    dw.x_sent(FG, ring[FG])
    dw.upper(V, ring[V], tokens_a, slim, cols, step)
    dw.lower(O, branch_all, gated, 0, step)
    rs_out.pass_on(2)
    dw.pass_on(FU, ring[FU])
    dw.x_sent(FU, ring[FU])
    dw.upper(G, ring[G], tokens_a, slim, 2 * cols, step)
    dw.lower(QK, tokens_a, slim, 0, step)
    dw.lower(V, tokens_a, slim, cols, step)
    dw.lower(G, tokens_a, slim, 2 * cols, step)
    rs_out.wait_own()

    def finish_out(r, i):
        result[r, :] = (middle[r, :] + rs_out.own(r)).astype(BF)

    over(tokens, 16, finish_out)
    out_layer = load(result, layer_out, 4)
    rs_out.sent()
    in_qk.wait()
    in_v.wait()
    in_g.wait()

    def one_part(i, carry):
        b, r = rows_of(i)
        total = dot_nt(slim[r, :cols], w[1]) + dot_nt(slim[r, cols : 2 * cols], w[0])
        rs_one.part(b, total + dot_nt(slim[r, 2 * cols :], w[2]))
        return carry

    lax.fori_loop(0, 4, one_part, 0)
    rs_one.pass_on(3)
    rs_one.pass_on(1)
    dw.pass_on(O, ring[O])
    rs_one.pass_on(2)
    dw.pass_on(QK, ring[QK])
    out_layer.wait()
    rs_one.wait_own()

    pltpu.make_async_copy(x_hbm, x_ref, load_sem.at[11]).wait()

    def first_back(r, i):
        back, gain_sum, bias_sum = norm_back(x_ref[r, :].astype(F32), rs_one.own(r), params_ref[0:1, :])
        result[r, :] = (grad_middle[r, :] + back).astype(BF)
        sums[0:1, :] += gain_sum
        sums[2:3, :] += bias_sum

    over(tokens, 16, first_back)
    out_grad = load(result, input_grad_out, 4)

    def sum_copy(k, peer):
        return remote(sums, sums_in.at[k], sum_send.at[k], sum_recv.at[k], peer)

    for k, peer in enumerate((place.c_peer(), place.y_peer())):
        sum_copy(k, peer).start()
        sum_copy(k, peer).wait()
        sums[...] += sums_in[k]
    pieces = cols // block
    for p in range(n_dp):
        payload[p, 0:4, :] = sums[0:4, p * block : (p + 1) * block]
        for k in range(pieces):
            payload[p, 4 + k : 5 + k, :] = group_sum[0:1, k * block : (k + 1) * block]
    pay = []
    for j, (bits, above, flips) in enumerate(place.pairs):
        position = (1 - place.z if flips else place.z) + above
        copy = remote(payload.at[position], payload_in.at[j], pay_send.at[j], pay_recv.at[j], place.peer(bits))
        copy.start()
        pay.append(copy)
    dw.pass_on(V, ring[V])
    for copy in pay:
        copy.wait()
    mine = payload[place.z]
    other = jnp.zeros_like(mine)
    for j, (bits, above, flips) in enumerate(place.pairs):
        if flips:
            other = other + payload_in[j]
        else:
            mine = mine + payload_in[j]
    sums_out[0] = mine
    sums_out[1] = other
    dw.pass_on(G, ring[G])
    out_grad.wait()
    for g in (O, QK, V, G):
        dw.x_sent(g, ring[g])
    ag.sent()
    rs_one.sent()
    for g in (FD, FG, FU, O, QK, V, G):
        dw.finish(g)


def backward_call(n_dp, x, params, group, cum_row, saved):
    tokens, width = x.shape
    rows_all = 8 * tokens
    w = saved[0]
    cols = w.shape[2]
    block = width // n_dp
    masks = n_dp // 2 - 1
    vmem, hbm = pl.BlockSpec(memory_space=pltpu.VMEM), pl.BlockSpec(memory_space=pl.ANY)
    shape = jax.ShapeDtypeStruct
    pay_rows = -(-(4 + cols // block) // 8) * 8
    outs = (
        shape((tokens, width), BF),
        shape((tokens, width), BF),
        shape((GROUPS, block, cols), BF),
        shape((GROUPS, masks, block, cols), BF),
        shape((2, pay_rows, block), F32),
    )
    dma = pltpu.SemaphoreType.DMA
    scratch = [
        pltpu.VMEM((3, width, cols), BF),
        pltpu.VMEM((rows_all, width), BF),
        pltpu.VMEM((rows_all, width), BF),
        pltpu.VMEM((rows_all, width), BF),
        pltpu.VMEM((rows_all, 3 * cols), BF),
        pltpu.VMEM((rows_all, 2 * cols), BF),
        pltpu.VMEM((rows_all, cols), F32),
        pltpu.VMEM((rows_all, cols), F32),
        pltpu.VMEM((rows_all, cols), BF),
        pltpu.VMEM((tokens, width), BF),
        pltpu.VMEM((tokens, width), F32),
        pltpu.VMEM((tokens, width), F32),
        pltpu.VMEM((8, width), F32),
        pltpu.VMEM((2, 8, width), F32),
        pltpu.VMEM((1, cols), F32),
        pltpu.VMEM((n_dp, pay_rows, block), F32),
        pltpu.VMEM((n_dp - 1, pay_rows, block), F32),
        pltpu.VMEM((4, tokens, width), BF),
        pltpu.VMEM((4, tokens, width), BF),
        pltpu.VMEM((4, tokens, width), BF),
        pltpu.VMEM((3, tokens, width), BF),
        pltpu.VMEM((4, tokens, width), BF),
        pltpu.VMEM((3, tokens, width), BF),
        pltpu.VMEM((GROUPS, width // 2, cols), BF),
        pltpu.VMEM((4, width // 2, cols), BF),
        pltpu.VMEM((GROUPS, width // 2, cols), BF),
        dma((7,)),
        dma((7,)),
        dma((3, 4)),
        dma((3, 4)),
        dma((3, 3)),
        dma((3, 3)),
        dma((GROUPS,)),
        dma((GROUPS, n_dp // 2)),
        dma((GROUPS,)),
        dma((GROUPS, masks)),
        dma((12,)),
        dma((GROUPS,)),
        dma((2,)),
        dma((2,)),
        dma((n_dp - 1,)),
        dma((n_dp - 1,)),
    ]
    return pl.pallas_call(
        functools.partial(backward_kernel, n_dp),
        out_shape=outs,
        in_specs=[hbm, vmem, vmem, vmem] + [hbm] * len(saved),
        out_specs=(hbm,) * 4 + (vmem,),
        scratch_shapes=scratch,
        compiler_params=pltpu.CompilerParams(
            collective_id=2, has_side_effects=True, vmem_limit_bytes=67_000_000
        ),
    )(x, params, group, cum_row, *saved)


def finish_kernel(
    n_dp,
    own_ref,
    others_ref,
    layer_ref,
    grad_ref,
    sums_ref,
    layer_out,
    input_grad,
    query_grad,
    key_grad,
    value_grad,
    gate_grad,
    out_grad,
    group_grad,
    gain_grad,
    bias_grad,
    ffn_gate_grad,
    ffn_up_grad,
    ffn_down_grad,
    own,
    others,
    rows,
    wide,
    tall,
    in_sem,
    out_sem,
    row_sem,
):
    place = Place(n_dp)
    z = place.z
    block, cols = own.shape[1:]
    loads = []
    for g in (FD, FG, FU, O, QK, V, G):
        pair = (
            pltpu.make_async_copy(own_ref.at[g], own.at[g], in_sem.at[0, g]),
            pltpu.make_async_copy(others_ref.at[g], others.at[g], in_sem.at[1, g]),
        )
        for copy in pair:
            copy.start()
        loads.append((g, pair))
    row_loads = [
        pltpu.make_async_copy(layer_ref, rows.at[0], row_sem.at[0]),
        pltpu.make_async_copy(grad_ref, rows.at[1], row_sem.at[1]),
    ]
    for copy in row_loads:
        copy.start()
    outs = []

    def save(src, dst, index):
        copy = pltpu.make_async_copy(src, dst, out_sem.at[index])
        copy.start()
        outs.append(copy)

    wide_at = {FG: 0, FU: 1, V: 2, G: 3, QK: 4}
    tall_at = {FD: 0, O: 1}
    targets = {FG: ffn_gate_grad, FU: ffn_up_grad, V: value_grad, G: gate_grad, FD: ffn_down_grad, O: out_grad}
    for g, pair in loads:
        for copy in pair:
            copy.wait()
        mine = own[g].astype(F32)
        theirs = None
        for i, (bits, above, flips) in enumerate(place.masks):
            value = others[g, i].astype(F32)
            if not flips:
                mine = mine + value
            else:
                theirs = value if theirs is None else theirs + value
        if g in tall_at:
            k = tall_at[g]
            tall[k, pl.ds(pl.multiple_of(z * cols, cols), cols), :] = mine.T
            tall[k, pl.ds(pl.multiple_of((1 - z) * cols, cols), cols), :] = theirs.T
            save(tall.at[k], targets[g], k)
            continue
        k = wide_at[g]
        if g == QK:
            half = cols // 2
            for which, dst in ((0, query_grad), (1, key_grad)):
                part = slice(which * half, (which + 1) * half)
                at = which * cols
                wide[k, :, pl.ds(pl.multiple_of(at + z * half, half), half)] = mine[:, part]
                wide[k, :, pl.ds(pl.multiple_of(at + (1 - z) * half, half), half)] = theirs[:, part]
                save(wide.at[k, :, pl.ds(at, cols)], dst, 2 + which)
            continue
        wide[k, :, pl.ds(pl.multiple_of(z * cols, cols), cols)] = mine
        wide[k, :, pl.ds(pl.multiple_of((1 - z) * cols, cols), cols)] = theirs
        save(wide.at[k], targets[g], 4 + k)
    for k, dst in ((0, layer_out), (1, input_grad)):
        row_loads[k].wait()
        for copy in column_copies(place, rows.at[k], dst, row_sem.at[k], block, True):
            copy.start()
    norm = sums_ref[0, 0:4, :] + sums_ref[1, 0:4, :]
    piece = gain_grad.shape[1]
    mine = norm[:, :piece]
    for k in range(1, block // piece):
        mine = jnp.where(place.t == k, norm[:, k * piece : (k + 1) * piece], mine)
    gain_grad[...] = mine[0:2, :]
    bias_grad[...] = mine[2:4, :]
    piece = group_grad.shape[1]
    here = place.d % (block // piece)
    row = place.d // (block // piece)

    def group_of(which):
        value = sums_ref[which, 4:5, :]
        for k in range(1, cols // block):
            value = jnp.where(row == k, sums_ref[which, 4 + k : 5 + k, :], value)
        out = value[:, :piece]
        for k in range(1, block // piece):
            out = jnp.where(here == k, value[:, k * piece : (k + 1) * piece], out)
        return out

    same, other = group_of(0), group_of(1)
    group_grad[0:1, :] = jnp.where(z == 0, same, other)
    group_grad[1:2, :] = jnp.where(z == 0, other, same)
    for copy in outs:
        copy.wait()
    for k, dst in ((0, layer_out), (1, input_grad)):
        pltpu.make_async_copy(rows.at[k], dst, row_sem.at[k]).wait()


def finish_call(n_dp, n_tensor, own, others, layer, grad, sums):
    tokens, width = layer.shape
    block, cols = own.shape[1:]
    masks = others.shape[1]
    vmem, hbm = pl.BlockSpec(memory_space=pltpu.VMEM), pl.BlockSpec(memory_space=pl.ANY)
    shape = jax.ShapeDtypeStruct
    rows, wide, tall = shape((tokens, width), BF), shape((block, 2 * cols), F32), shape((2 * cols, block), F32)
    thin, norm = shape((block, cols), F32), shape((2, width // (n_dp * n_tensor)), F32)
    outs = (rows, rows, thin, thin, wide, wide, tall, shape((2, cols // n_dp), F32), norm, norm, wide, wide, tall)
    specs = [vmem if o.shape[0] == 2 else hbm for o in outs]
    dma = pltpu.SemaphoreType.DMA
    return pl.pallas_call(
        functools.partial(finish_kernel, n_dp),
        out_shape=outs,
        in_specs=[hbm, hbm, hbm, hbm, vmem],
        out_specs=tuple(specs),
        scratch_shapes=[
            pltpu.VMEM((GROUPS, block, cols), BF),
            pltpu.VMEM((GROUPS, masks, block, cols), BF),
            pltpu.VMEM((2, tokens, width), BF),
            pltpu.VMEM((5, block, 2 * cols), F32),
            pltpu.VMEM((2, 2 * cols, block), F32),
            dma((2, GROUPS)),
            dma((8,)),
            dma((2,)),
        ],
        compiler_params=pltpu.CompilerParams(vmem_limit_bytes=67_000_000),
    )(own, others, layer, grad, sums)


def per_device(
    n_dp,
    n_tensor,
    inputs,
    cotangent,
    log_decay,
    query_weight,
    key_weight,
    value_weight,
    gate_weight,
    out_weight,
    group_gain,
    norm_gains,
    norm_biases,
    ffn_gate_weight,
    ffn_up_weight,
    ffn_down_weight,
):
    place = Place(n_dp)
    d, t = place.d, place.t
    tokens, width = inputs.shape
    block = width // n_dp
    head_v = value_weight.shape[1] // 2

    def position_of(q):
        out = (q // PAIR) & 1
        for k, bit in enumerate(place.rest):
            out = out + ((d // bit) % 2 ^ ((q // bit) & 1)) * (2 << k)
        return out

    def moved(value, index):
        if block % 128 == 0:
            return value
        return jnp.concatenate(
            [lax.dynamic_slice_in_dim(value, index(p) * block, block, 1) for p in range(n_dp)], axis=1
        )

    def half(value, which, axis):
        size = value.shape[axis] // 2
        return lax.dynamic_slice_in_dim(value, which * size, size, axis)

    cumul = jnp.cumsum(log_decay, axis=1).reshape(2, n_tensor, tokens)
    for bit in (1, 2):
        swapped = jnp.concatenate([cumul[:, j ^ bit : (j ^ bit) + 1] for j in range(n_tensor)], axis=1)
        cumul = jnp.where((t // bit) % 2 == 1, swapped, cumul)
    spread = jnp.tile(group_gain.astype(F32), (1, n_dp))
    spread = jnp.where(lax.broadcasted_iota(jnp.int32, spread.shape, 1) // (head_v // n_dp) == d, spread, 0.0)
    parts = [norm_gains.astype(F32), norm_biases.astype(F32), spread, cumul]
    small = jnp.concatenate([part.reshape(-1, block) for part in parts], axis=0)
    small = jnp.pad(small, ((0, -small.shape[0] % 8), (0, 0)))

    def interleaved(first, second):
        parts = [half(first, 0, 1), half(second, 0, 1), half(first, 1, 1), half(second, 1, 1)]
        return jnp.concatenate(parts, axis=1)

    sources = [
        interleaved(query_weight, key_weight),
        value_weight,
        gate_weight,
        out_weight.T,
        ffn_gate_weight,
        ffn_up_weight,
        ffn_down_weight.T,
    ]

    x, cot = moved(inputs, place.dp_of), moved(cotangent, place.dp_of)
    *saved, params, group, cumul = forward_call(n_dp, x, cot, small, sources)
    layer, grad, own, others, sums = backward_call(n_dp, x, params, group, cumul, saved)
    outs = finish_call(n_dp, n_tensor, own, others, layer, grad, sums)
    return (moved(outs[0], position_of), moved(outs[1], position_of), *outs[2:])


def solution(mesh):
    tokens = P(("dp", "tensor"), None)
    rows, cols, norms = P("dp", "tensor"), P("tensor", "dp"), P(None, "dp")
    sums = P(None, ("dp", "tensor"))
    in_specs = (tokens, tokens, cols, rows, rows, rows, rows, cols, cols, norms, norms, rows, rows, cols)
    out_specs = (tokens, tokens, rows, rows, rows, rows, cols, cols, sums, sums, rows, rows, cols)
    body = functools.partial(per_device, mesh.shape["dp"], mesh.shape["tensor"])
    return jax.shard_map(body, mesh=mesh, in_specs=in_specs, out_specs=out_specs, check_vma=False)
```

```python
import functools
import math

import jax
import jax.numpy as jnp
from jax import lax
from jax.experimental import pallas as pl
from jax.experimental.pallas import tpu as pltpu
from jax.sharding import PartitionSpec as P

EPSILON = 1e-05
GROUP_FLOOR = 1.0
BF = jnp.bfloat16
F32 = jnp.float32
PAIR = 2
MESH = pl.DeviceIdType.MESH
QK, V, G, O, FG, FU, FD = range(7)
GROUPS = 7


FORWARD = (
    "x2", "x3", "x0", "s01", "s22", "s02", "s21", "s41", "s12", "x1", "f01", "s31", "small", "ln", "f22", "ns",
    "s03", "f41", "f02", "nfy", "s23", "f12", "x6", "s32", "s13", "f31", "s11", "nfz", "f21", "f03", "f32", "ks",
    "s33", "s53", "nfzy", "f11", "s43", "s51", "f23", "qk", "f13", "kfz", "f33", "v", "g", "f53", "kfy", "s52",
    "o", "p3", "f51", "p1", "s61", "x5", "f52", "s42", "p2", "f42", "s63", "kfzy", "x4", "f43", "ln2", "f61", "ts",
    "feedA", "tfy", "s62", "tfz", "feedB", "f63", "f62", "tfzy", "feedC", "feedD", "back",
)
BACKWARD = (
    "u6", "two", "a3", "l6", "s63", "a1", "a2", "l4", "u4", "lnb", "bs", "u5", "s60", "gat", "l5", "s43", "out",
    "bfz", "s53", "s61", "bfy", "gbA", "s40", "bfzy", "s52", "s41", "gbB", "u3", "seq0", "seq1", "o3", "u2", "l0",
    "s42", "s51", "s62", "l2", "u0", "s50", "o1", "l3", "o2", "s32", "u1", "s21", "s23", "s33", "s31", "outf",
    "one", "s30", "l1", "b3", "b1", "s22", "b2", "s02", "s13", "s01", "lna", "s00", "s10", "s11", "s03", "s20",
    "sc", "sy", "pay", "s12", "payw",
)


def dot_nn(a, b):
    return lax.dot_general(a, b, (((1,), (0,)), ((), ())), preferred_element_type=F32)


def dot_nt(a, b):
    return lax.dot_general(a, b, (((1,), (1,)), ((), ())), preferred_element_type=F32)


def dot_tn(a, b):
    return lax.dot_general(a, b, (((0,), (0,)), ((), ())), preferred_element_type=F32)


def flip(index, bit):
    return index + bit - 2 * bit * ((index // bit) % 2)


class Place:
    def __init__(self, n_dp):
        self.n_dp = n_dp
        self.d = lax.axis_index("dp")
        self.t = lax.axis_index("tensor")
        self.z = (self.d // PAIR) % 2
        self.rest = [1 << i for i in range(2, n_dp.bit_length() - 1)] + [1]
        self.inner = self.rest[:-1]
        self.masks = []
        for pick in range(1, 1 << (1 + len(self.inner))):
            bits = [PAIR] * (pick & 1) + [b for k, b in enumerate(self.inner) if (pick >> (k + 1)) & 1]
            self.masks.append((bits, pick & ~1, pick & 1))
        half = n_dp // 2
        self.pairs = self.masks + [([1], half, 0)] + [(bits + [1], above + half, flips) for bits, above, flips in self.masks]

    def slot(self, above, flips):
        return next((j for j, pair in enumerate(self.pairs) if pair[1:] == (above, flips)), None)

    def dp_of(self, p):
        out = (p & 1) * PAIR
        for k, bit in enumerate(self.rest):
            here = (self.d // bit) % 2
            out = out + (1 - here if (p >> (k + 1)) & 1 else here) * bit
        return out

    def peer(self, bits):
        out = self.d
        for bit in bits:
            out = flip(out, bit)
        return {"dp": out}

    def x_peer(self):
        return {"dp": flip(self.d, 1)}

    def z_peer(self):
        return {"dp": flip(self.d, PAIR)}

    def y_peer(self):
        return {"tensor": flip(self.t, 2)}

    def c_peer(self):
        return {"tensor": flip(self.t, 1)}

    def everyone(self, far):
        near = [self.x_peer(), self.y_peer(), self.c_peer()]
        if far:
            return near[1:] + [self.peer(bits) for bits, _, _ in self.pairs]
        return near + [self.peer(bits) for bits, _, _ in self.masks]


def entry_barrier(place, far=False):
    barrier = pltpu.get_barrier_semaphore()
    peers = place.everyone(far)
    for peer in peers:
        pl.semaphore_signal(barrier, inc=1, device_id=peer, device_id_type=MESH)
    pl.semaphore_wait(barrier, len(peers))


def column_copies(place, src, dst, sem, block, back=False):
    if block % 128:
        return [pltpu.make_async_copy(src, dst, sem)]
    out = []
    for p in range(place.n_dp):
        natural = pl.ds(pl.multiple_of(place.dp_of(p) * block, block), block)
        here = pl.ds(p * block, block)
        a, b = (here, natural) if back else (natural, here)
        out.append(pltpu.make_async_copy(src.at[:, a], dst.at[:, b], sem))
    return out


def remote(src, dst, send, recv, peer):
    return pltpu.make_async_remote_copy(
        src_ref=src, dst_ref=dst, send_sem=send, recv_sem=recv, device_id=peer, device_id_type=MESH
    )


class Weights:
    def __init__(self, place, sources, full, sems):
        self.place, self.sources, self.full = place, sources, full
        self.z_send, self.z_recv, self.x_send, self.x_recv, self.local = sems
        self.block = sources[0].shape[0]
        self.cols = sources[0].shape[1] // 2
        self.half = place.n_dp // 2

    def rows(self, position, count=1):
        return pl.ds(pl.multiple_of(position * self.block, self.block), count * self.block)

    def source(self, g, half):
        return self.sources[g].at[:, pl.ds(pl.multiple_of(half * self.cols, self.cols), self.cols)]

    def own(self, g):
        z = self.place.z
        pltpu.make_async_copy(self.source(g, z), self.full.at[g, self.rows(z), :], self.local.at[g]).start()
        remote(
            self.source(g, z),
            self.full.at[g, self.rows(z + self.half), :],
            self.x_send.at[g],
            self.x_recv.at[g],
            self.place.x_peer(),
        ).start()

    def some(self, third):
        count = len(self.place.masks)
        return reversed(range(third * count // 3, (third + 1) * count // 3))

    def start(self, g, third):
        z = self.place.z
        for i in self.some(third):
            bits, above, flips = self.place.masks[i]
            remote(
                self.source(g, 1 - z if flips else z),
                self.full.at[g, self.rows(z + above), :],
                self.z_send.at[g],
                self.z_recv.at[g, i],
                self.place.peer(bits),
            ).start()

    def forward(self, g, third):
        for i in self.some(third):
            bits, above, flips = self.place.masks[i]
            position = (1 - self.place.z if flips else self.place.z) + above
            here = self.full.at[g, self.rows(position), :]
            remote(here, here, self.z_send.at[g], self.z_recv.at[g, i], self.place.peer(bits)).wait_recv()
            remote(
                here,
                self.full.at[g, self.rows(position + self.half), :],
                self.x_send.at[g],
                self.x_recv.at[g],
                self.place.x_peer(),
            ).start()

    def finish(self, g):
        z = self.place.z
        pltpu.make_async_copy(self.source(g, z), self.full.at[g, self.rows(z), :], self.local.at[g]).wait()
        there = self.full.at[g, self.rows(self.half, self.half), :]
        remote(there, there, self.x_send.at[g], self.x_recv.at[g], self.place.x_peer()).wait_recv()

    def sent(self, g):
        there = self.full.at[g, self.rows(self.half, self.half), :]
        remote(there, there, self.x_send.at[g], self.x_recv.at[g], self.place.x_peer()).wait_send()
        count = self.half - 1
        those = self.full.at[g, self.rows(0, count), :]
        remote(those, those, self.z_send.at[g], self.z_recv.at[g, 0], self.place.x_peer()).wait_send()


class Gather:
    def __init__(self, place, buffer, send, recv):
        self.place, self.buffer = place, buffer
        self.send, self.recv = send, recv
        self.tokens = buffer.shape[0] // 8
        self.peers = {1: place.c_peer(), 2: place.y_peer(), 4: place.z_peer()}

    def slot(self, s):
        return self.buffer.at[pl.ds(pl.multiple_of(s * self.tokens, self.tokens), self.tokens), :]

    def copy(self, source, bit, src=None):
        s = source + bit
        return remote(self.slot(source) if src is None else src, self.slot(s), self.send.at[s - 1], self.recv.at[s - 1], self.peers[bit])

    def start(self, src=None):
        for bit in (4, 2, 1):
            self.copy(0, bit, src).start()

    def from_z(self):
        self.copy(0, 4).wait_recv()
        self.copy(4, 2).start()
        self.copy(4, 1).start()

    def from_y(self):
        self.copy(0, 2).wait_recv()
        self.copy(2, 1).start()

    def from_zy(self):
        self.copy(4, 2).wait_recv()
        self.copy(6, 1).start()

    def chip(self, source):
        self.copy(source, 1).wait_recv()

    def sent(self, src=None):
        self.copy(0, 4, src).wait_send()
        self.copy(0, 2, src).wait_send()
        self.copy(0, 1, src).wait_send()
        self.copy(4, 2).wait_send()
        self.copy(4, 1).wait_send()
        self.copy(2, 1).wait_send()
        self.copy(6, 1).wait_send()


class Scatter:
    def __init__(self, place, keep, c_out, c_in, far_out, far_in, sems):
        self.place = place
        self.keep, self.c_out, self.c_in, self.far_out, self.far_in = keep, c_out, c_in, far_out, far_in
        self.c_send, self.c_recv, self.far_send, self.far_recv = sems
        self.tokens = c_out.shape[1]

    def part(self, b, value):
        self.keep[b] = value[: self.tokens].astype(self.keep.dtype)
        self.c_out[b] = value[self.tokens :].astype(BF)
        self.c_copy(b).start()

    def c_copy(self, b):
        return remote(self.c_out.at[b], self.c_in.at[b], self.c_send.at[b], self.c_recv.at[b], self.place.c_peer())

    def far_copy(self, b):
        peer = self.place.z_peer() if b == 2 else self.place.y_peer()
        return remote(
            self.far_source(b), self.far_in.at[b - 1], self.far_send.at[b - 1], self.far_recv.at[b - 1], peer
        )

    def far_source(self, b):
        return self.keep.at[b] if self.far_out is None else self.far_out.at[b - 1]

    def rows(self, body, step=16):
        def loop(i, carry):
            body(pl.ds(pl.multiple_of(i * step, step), step))
            return carry

        lax.fori_loop(0, self.tokens // step, loop, 0)

    def pass_on(self, b):
        self.c_copy(b).wait_recv()
        if b == 2:
            self.far_copy(3).wait_recv()

        def body(r):
            total = self.keep[b, r, :].astype(F32) + self.c_in[b, r, :].astype(F32)
            if b == 2:
                total = total + self.far_in[2, r, :].astype(F32)
            self.far_source(b)[r, :] = total.astype(BF)

        self.rows(body)
        self.far_copy(b).start()

    def wait_own(self):
        self.c_copy(0).wait_recv()
        self.far_copy(1).wait_recv()
        self.far_copy(2).wait_recv()

    def own(self, r):
        return (
            self.keep[0, r, :].astype(F32)
            + self.c_in[0, r, :].astype(F32)
            + self.far_in[0, r, :].astype(F32)
            + self.far_in[1, r, :].astype(F32)
        )

    def sent(self):
        for b in range(4):
            self.c_copy(b).wait_send()
        for b in (3, 2, 1):
            self.far_copy(b).wait_send()


def normalized(value):
    center = value - jnp.mean(value, axis=-1, keepdims=True)
    spread = jnp.mean(center * center, axis=-1, keepdims=True)
    return center * lax.rsqrt(spread + EPSILON)


def decay_tile(t, cumul_rows, cumul_here, first, rows, length, tokens):
    square = (rows, rows)
    same = lax.broadcasted_iota(jnp.int32, square, 0) == lax.broadcasted_iota(jnp.int32, square, 1)
    cumul_cols = jnp.sum(jnp.where(same, cumul_here, 0.0), axis=1, keepdims=True)
    index = lax.broadcasted_iota(jnp.int32, (rows, length), 0) + first
    other = lax.broadcasted_iota(jnp.int32, (rows, length), 1)
    at = ((index // tokens) ^ t) * tokens + index % tokens
    to = ((other // tokens) ^ t) * tokens + other % tokens
    causal = at >= to
    return jnp.where(causal, jnp.exp(jnp.where(causal, cumul_cols - cumul_rows, 0.0)), 0.0)


def spread_small(place, own, others, params, group, cumul, block):
    pieces = group.shape[1] // block
    steps = cumul.shape[1] // block
    first = place.z == 0

    def of(above, flips, rows):
        j = place.slot(above, flips)
        return own[rows, :] if j is None else others[j, rows, :]

    head = slice(0, 4)
    for p in range(place.n_dp):
        same, flipped = of(p & ~1, 0, head), of(p & ~1, 1, head)
        params[head, p * block : (p + 1) * block] = jnp.where(place.z == p % 2, same, flipped)

    def head_rows(above, flips, at, count):
        one = of(above, flips, slice(at, at + count))
        two = of(above, flips, slice(at + count, at + 2 * count))
        return jnp.where(first, one, two)

    total = head_rows(0, 0, 4, pieces)
    for bits, above, flips in place.pairs:
        total = total + head_rows(above, flips, 4, pieces)
    for k in range(pieces):
        group[0:1, k * block : (k + 1) * block] = total[k : k + 1, :]
    at = 4 + 2 * pieces
    for row, flips in ((0, 0), (1, 1)):
        value = head_rows(0, flips, at, steps)
        for k in range(steps):
            cumul[row : row + 1, k * block : (k + 1) * block] = value[k : k + 1, :]


def forward_kernel(
    n_dp,
    x_hbm,
    cot_hbm,
    small_ref,
    s_qk,
    s_v,
    s_g,
    s_o,
    s_fg,
    s_fu,
    s_fd,
    w_out,
    normed_out,
    qkv_out,
    gate_out,
    mixed_out,
    ffn_in_out,
    hidden_out,
    grads_out,
    cot_out,
    middle_out,
    params_out,
    group_out,
    cumul_out,
    small_in,
    params_ref,
    group_ref,
    cum_row_ref,
    x_ref,
    w,
    normed_all,
    cot_all,
    ffn_in,
    qkv,
    gate_in,
    mixed,
    gated,
    gate_hidden,
    up_hidden,
    hidden,
    grads,
    middle,
    keep,
    c_out,
    c_in,
    far_out,
    far_in,
    z_send,
    z_recv,
    x_send,
    x_recv,
    w_local,
    ag_send,
    ag_recv,
    c_send,
    c_recv,
    far_send,
    far_recv,
    out_sem,
    small_send,
    small_recv,
):
    place = Place(n_dp)
    tokens, width = x_ref.shape
    block = width // n_dp
    rows_all = 8 * tokens
    length = rows_all // 2
    head_k = qkv.shape[1] // 4
    scale = 1.0 / math.sqrt(head_k)
    tile = 2 * tokens
    weights = Weights(place, [s_qk, s_v, s_g, s_o, s_fg, s_fu, s_fd], w, (z_send, z_recv, x_send, x_recv, w_local))
    ag_normed = Gather(place, normed_all, ag_send.at[0], ag_recv.at[0])
    ag_cot = Gather(place, cot_all, ag_send.at[1], ag_recv.at[1])
    ag_two = Gather(place, ffn_in, ag_send.at[2], ag_recv.at[2])
    branch = Scatter(place, keep, c_out, c_in, far_out, far_in, (c_send, c_recv, far_send, far_recv))
    outs = []

    def save(src, dst, index):
        copy = pltpu.make_async_copy(src, dst, out_sem.at[index])
        copy.start()
        outs.append(copy)

    def over(count, step, body):
        def loop(i, carry):
            body(pl.ds(pl.multiple_of(i * step, step), step), i)
            return carry

        lax.fori_loop(0, count // step, loop, 0)

    for copy in column_copies(place, x_hbm, x_ref, out_sem.at[16], block):
        copy.start()
    for copy in column_copies(place, cot_hbm, ag_cot.slot(0), out_sem.at[17], block):
        copy.start()
    entry_barrier(place, True)
    small = []
    for j, (bits, above, flips) in enumerate(place.pairs):
        copy = remote(small_ref, small_in.at[j], small_send.at[j], small_recv.at[j], place.peer(bits))
        copy.start()
        small.append(copy)
    size = gate_hidden.shape[1]

    def first_norm(r, i):
        value = normalized(x_ref[r, :].astype(F32))
        normed_all[r, :] = (value * params_ref[0:1, :] + params_ref[2:3, :]).astype(BF)

    def make_qk(r, i):
        qkv[r, : 2 * head_k] = dot_nn(normed_all[r, :], w[QK]).astype(BF)

    def make_v(r, i):
        qkv[r, 2 * head_k :] = dot_nn(normed_all[r, :], w[V]).astype(BF)

    def retention(r, i):
        start = pl.multiple_of((i // 2) * length, length)
        seq = pl.ds(start, length)
        scores = dot_nt(qkv[r, :head_k], qkv[seq, head_k : 2 * head_k])
        here = cum_row_ref[pl.ds(i // 2, 1), pl.ds(pl.multiple_of((i % 2) * tile, tile), tile)]
        decays = decay_tile(
            place.t, cum_row_ref[pl.ds(i // 2, 1), :], here, (i % 2) * tile, tile, length, tokens
        )
        weighted = (scores * decays * scale).astype(BF)
        mixed[r, :] = dot_nn(weighted, qkv[seq, 2 * head_k :])

    def gating(r, i):
        gate = dot_nn(normed_all[r, :], w[G])
        gate_in[r, :] = gate
        value = mixed[r, :]
        center = value - jnp.mean(value, axis=-1, keepdims=True)
        spread = jnp.mean(center * center, axis=-1, keepdims=True)
        flat = center * lax.rsqrt(jnp.maximum(spread, GROUP_FLOOR)) * group_ref[...]
        gated[r, :] = (flat * (gate * lax.logistic(gate))).astype(BF)

    def branch_part(i, carry):
        r = pl.ds(pl.multiple_of((3 - i) * tile, tile), tile)
        branch.part(3 - i, dot_nt(gated[r, :], w[O]))
        return carry

    def second_norm(r, i):
        value = x_ref[r, :].astype(F32) + branch.own(r)
        middle[r, :] = value
        ffn_in[r, :] = (normalized(value) * params_ref[1:2, :] + params_ref[3:4, :]).astype(BF)

    def feed(b):
        r = pl.ds(pl.multiple_of(b * tile, tile), tile)
        gate = dot_nn(ffn_in[r, :], w[FG])
        up = dot_nn(ffn_in[r, :], w[FU])
        gate_hidden[r, :] = gate
        up_hidden[r, :] = up
        hidden[r, :] = (gelu(gate) * up).astype(BF)

    def feed_back(r, i):
        back = dot_nn(cot_all[r, :], w[FD])
        gate = gate_hidden[r, :]
        value, slope = gelu_and_slope(gate)
        grads[r, :size] = (back * up_hidden[r, :] * slope).astype(BF)
        grads[r, size:] = (back * value).astype(BF)

    def small_step():
        pltpu.make_async_copy(x_hbm, x_ref, out_sem.at[16]).wait()
        for copy in small:
            copy.wait()
        spread_small(place, small_ref, small_in, params_ref, group_ref, cum_row_ref, block)

    def norm_step():
        over(tokens, 16, first_norm)

    def cot_start():
        pltpu.make_async_copy(cot_hbm, ag_cot.slot(0), out_sem.at[17]).wait()
        ag_cot.start()

    def chips(ag):
        lax.fori_loop(0, 4, lambda b, carry: (ag.chip(2 * b), carry)[1], 0)

    def qk_step():
        chips(ag_normed)
        weights.finish(QK)
        over(rows_all, tile, make_qk)
        save(normed_all, normed_out, 0)
        save(w.at[QK], w_out.at[QK], 1)
        save(params_ref, params_out, 18)
        save(group_ref, group_out, 19)
        save(cum_row_ref, cumul_out, 20)

    def v_step():
        weights.finish(V)
        over(rows_all, tile, make_v)
        over(rows_all, tile, retention)
        save(w.at[V], w_out.at[V], 2)
        save(qkv, qkv_out, 3)
        save(mixed, mixed_out, 4)

    def g_step():
        weights.finish(G)
        over(rows_all, tile, gating)
        save(w.at[G], w_out.at[G], 5)
        save(gate_in, gate_out, 6)

    def o_step():
        weights.finish(O)
        lax.fori_loop(0, 4, branch_part, 0)
        save(w.at[O], w_out.at[O], 7)

    def second_step():
        branch.wait_own()
        over(tokens, 16, second_norm)
        save(middle, middle_out, 9)

    def feed_step(b):
        if b == 0:
            weights.finish(FG)
            weights.finish(FU)
            save(w.at[FG], w_out.at[FG], 10)
            save(w.at[FU], w_out.at[FU], 11)

        def one(i, carry):
            ag_two.chip(2 * i)
            feed(i)
            return carry

        lax.fori_loop(b, b + 1, one, 0)

    def last_step():
        save(ffn_in, ffn_in_out, 12)
        save(hidden, hidden_out, 13)
        chips(ag_cot)
        save(cot_all, cot_out, 8)
        weights.finish(FD)
        save(w.at[FD], w_out.at[FD], 14)
        over(rows_all, tile, feed_back)
        save(grads, grads_out, 15)

    steps = {
        "small": small_step,
        "ln": norm_step,
        "ns": ag_normed.start,
        "nfz": ag_normed.from_z,
        "nfy": ag_normed.from_y,
        "nfzy": ag_normed.from_zy,
        "ks": cot_start,
        "kfz": ag_cot.from_z,
        "kfy": ag_cot.from_y,
        "kfzy": ag_cot.from_zy,
        "ts": ag_two.start,
        "tfz": ag_two.from_z,
        "tfy": ag_two.from_y,
        "tfzy": ag_two.from_zy,
        "qk": qk_step,
        "v": v_step,
        "g": g_step,
        "o": o_step,
        "p3": lambda: branch.pass_on(3),
        "p1": lambda: branch.pass_on(1),
        "p2": lambda: branch.pass_on(2),
        "ln2": second_step,
        "feedA": lambda: feed_step(0),
        "feedB": lambda: feed_step(1),
        "feedC": lambda: feed_step(2),
        "feedD": lambda: feed_step(3),
        "back": last_step,
    }
    for name in FORWARD:
        if name[1:].isdigit():
            g = int(name[1])
            if name[0] == "x":
                weights.own(g)
            elif name[0] == "s":
                weights.start(g, int(name[2]) - 1)
            elif name[0] == "f":
                weights.forward(g, int(name[2]) - 1)
            else:
                steps[name]()
        else:
            steps[name]()
    for copy in outs:
        copy.wait()
    for g in range(GROUPS):
        weights.sent(g)
    ag_normed.sent()
    ag_cot.sent()
    ag_two.sent()
    branch.sent()


ROOT = math.sqrt(2.0 / math.pi)


def gelu(v):
    return 0.5 * v * (1.0 + jnp.tanh(ROOT * (v + 0.044715 * v * v * v)))


def gelu_and_slope(v):
    inside = jnp.tanh(ROOT * (v + 0.044715 * v * v * v))
    slope = 0.5 * (1.0 + inside) + 0.5 * v * (1.0 - inside * inside) * ROOT * (1.0 + 3 * 0.044715 * v * v)
    return 0.5 * v * (1.0 + inside), slope


def forward_call(n_dp, x, cot, small, sources):
    tokens, width = x.shape
    length = 4 * tokens
    rows_all = 8 * tokens
    cols = sources[0].shape[1] // 2
    masks = n_dp // 2 - 1
    vmem, hbm = pl.BlockSpec(memory_space=pltpu.VMEM), pl.BlockSpec(memory_space=pl.ANY)
    shape = jax.ShapeDtypeStruct
    outs = (
        shape((GROUPS, width, cols), BF),
        shape((rows_all, width), BF),
        shape((rows_all, 2 * cols), BF),
        shape((rows_all, cols), F32),
        shape((rows_all, cols), F32),
        shape((rows_all, width), BF),
        shape((rows_all, cols), BF),
        shape((rows_all, 2 * cols), BF),
        shape((rows_all, width), BF),
        shape((tokens, width), F32),
        shape((8, width), F32),
        shape((1, cols), F32),
        shape((2, length), F32),
    )
    dma = pltpu.SemaphoreType.DMA
    scratch = [
        pltpu.VMEM((n_dp - 1, *small.shape), F32),
        pltpu.VMEM((8, width), F32),
        pltpu.VMEM((1, cols), F32),
        pltpu.VMEM((2, length), F32),
        pltpu.VMEM((tokens, width), BF),
        pltpu.VMEM((GROUPS, width, cols), BF),
        pltpu.VMEM((rows_all, width), BF),
        pltpu.VMEM((rows_all, width), BF),
        pltpu.VMEM((rows_all, width), BF),
        pltpu.VMEM((rows_all, 2 * cols), BF),
        pltpu.VMEM((rows_all, cols), F32),
        pltpu.VMEM((rows_all, cols), F32),
        pltpu.VMEM((rows_all, cols), BF),
        pltpu.VMEM((rows_all, cols), F32),
        pltpu.VMEM((rows_all, cols), F32),
        pltpu.VMEM((rows_all, cols), BF),
        pltpu.VMEM((rows_all, 2 * cols), BF),
        pltpu.VMEM((tokens, width), F32),
        pltpu.VMEM((4, tokens, width), F32),
        pltpu.VMEM((4, tokens, width), BF),
        pltpu.VMEM((4, tokens, width), BF),
        pltpu.VMEM((3, tokens, width), BF),
        pltpu.VMEM((3, tokens, width), BF),
        dma((GROUPS,)),
        dma((GROUPS, masks)),
        dma((GROUPS,)),
        dma((GROUPS,)),
        dma((GROUPS,)),
        dma((3, 7)),
        dma((3, 7)),
        dma((4,)),
        dma((4,)),
        dma((3,)),
        dma((3,)),
        dma((21,)),
        dma((n_dp - 1,)),
        dma((n_dp - 1,)),
    ]
    return pl.pallas_call(
        functools.partial(forward_kernel, n_dp),
        out_shape=outs,
        in_specs=[hbm, hbm, vmem] + [hbm] * GROUPS,
        out_specs=(hbm,) * len(outs),
        scratch_shapes=scratch,
        compiler_params=pltpu.CompilerParams(
            collective_id=1, has_side_effects=True, vmem_limit_bytes=64_000_000
        ),
    )(x, cot, small, *sources)


class Reduce:
    def __init__(self, place, keep, x_out, x_in, z_in, own_out, sems, own_sem):
        self.place = place
        self.keep, self.x_out, self.x_in, self.z_in, self.own_out = keep, x_out, x_in, z_in, own_out
        self.x_send, self.x_recv, self.z_send, self.z_recv = sems
        self.own_sem = own_sem
        self.block = z_in.shape[2]
        self.half = place.n_dp // 2
        z = place.z
        self.targets = [
            ((1 - z if flips else z) + above, i, place.peer(bits)) for i, (bits, above, flips) in enumerate(place.masks)
        ]
        self.targets.reverse()

    def rows(self, position):
        return pl.ds(pl.multiple_of(position * self.block, self.block), self.block)

    def x_copy(self, g, ring, position):
        return remote(
            self.x_out.at[ring, self.rows(position), :],
            self.x_in.at[g, self.rows(position), :],
            self.x_send.at[g],
            self.x_recv.at[g, position],
            self.place.x_peer(),
        )

    def z_copy(self, g, position, i, peer):
        return remote(
            self.keep.at[g, self.rows(position), :],
            self.z_in.at[g, i],
            self.z_send.at[g],
            self.z_recv.at[g, i],
            peer,
        )

    def upper(self, g, ring, left, right, col, step):
        width = left.shape[1] // 2
        cols = self.keep.shape[2]

        def body(i, carry):
            at = pl.multiple_of(i * step, step)
            value = dot_tn(left[:, pl.ds(pl.multiple_of(width + at, step), step)], right[:, col : col + cols])
            self.x_out[ring, pl.ds(at, step), :] = value.astype(BF)
            return carry

        lax.fori_loop(0, width // step, body, 0)
        for position, _, _ in self.targets:
            self.x_copy(g, ring, position).start()
        self.x_copy(g, ring, self.place.z).start()

    def lower(self, g, left, right, col, step):
        width = left.shape[1] // 2
        cols = self.keep.shape[2]

        def body(i, carry):
            at = pl.ds(pl.multiple_of(i * step, step), step)
            self.keep[g, at, :] = dot_tn(left[:, at], right[:, col : col + cols]).astype(BF)
            return carry

        lax.fori_loop(0, width // step, body, 0)

    def x_sent(self, g, ring):
        whole = self.x_out.at[ring]
        remote(whole, whole, self.x_send.at[g], self.x_recv.at[g, 0], self.place.x_peer()).wait_send()

    def add(self, g, ring, position):
        self.x_copy(g, ring, position).wait_recv()
        step = min(64, self.block)

        def body(i, carry):
            r = pl.ds(pl.multiple_of(position * self.block + i * step, step), step)
            self.keep[g, r, :] = (self.keep[g, r, :].astype(F32) + self.x_in[g, r, :].astype(F32)).astype(BF)
            return carry

        lax.fori_loop(0, self.block // step, body, 0)

    def own_copy(self, g):
        return pltpu.make_async_copy(
            self.keep.at[g, self.rows(self.place.z), :], self.own_out.at[g], self.own_sem.at[g]
        )

    def step(self, g, ring, third):
        if third == 0:
            self.add(g, ring, self.place.z)
            self.own_copy(g).start()
            return
        count = len(self.targets)
        for position, i, peer in self.targets[(3 - third) * count // 3 : (4 - third) * count // 3]:
            self.add(g, ring, position)
            self.z_copy(g, position, i, peer).start()

    def finish(self, g):
        self.own_copy(g).wait()
        for position, i, peer in self.targets:
            self.z_copy(g, position, i, peer).wait()


def norm_back(value, grad, gain):
    center = value - jnp.mean(value, axis=-1, keepdims=True)
    spread = jnp.mean(center * center, axis=-1, keepdims=True)
    r = lax.rsqrt(spread + EPSILON)
    hat = center * r
    scaled = grad * gain
    back = r * (
        scaled - jnp.mean(scaled, axis=-1, keepdims=True) - hat * jnp.mean(scaled * hat, axis=-1, keepdims=True)
    )
    return back, jnp.sum(grad * hat, axis=0, keepdims=True), jnp.sum(grad, axis=0, keepdims=True)


def backward_kernel(
    n_dp,
    x_hbm,
    params_ref,
    group_ref,
    cum_row_ref,
    w_ref,
    normed_ref,
    qkv_ref,
    gate_ref,
    mixed_ref,
    ffn_in_ref,
    hidden_ref,
    grads_ref,
    cot_ref,
    middle_ref,
    layer_out,
    input_grad_out,
    own_out,
    z_in,
    sums_out,
    w,
    tokens_a,
    ffn_in,
    branch_all,
    slim,
    qkv,
    gate_in,
    mixed,
    gated,
    x_ref,
    middle,
    grad_middle,
    sums,
    sums_in,
    group_sum,
    payload,
    payload_in,
    keep,
    c_out,
    c_in,
    far_in,
    c_in_two,
    far_in_two,
    dw_keep,
    x_out,
    x_in,
    ag_send,
    ag_recv,
    c_send,
    c_recv,
    far_send,
    far_recv,
    x_send,
    x_recv,
    z_send,
    z_recv,
    load_sem,
    own_sem,
    sum_send,
    sum_recv,
    pay_send,
    pay_recv,
):
    place = Place(n_dp)
    tokens, width = x_ref.shape
    rows_all = 8 * tokens
    length = rows_all // 2
    cols = gated.shape[1]
    head_k = cols // 2
    scale = 1.0 / math.sqrt(head_k)
    tile = 2 * tokens
    step = min(512, width // 2)
    block = z_in.shape[2]
    ag = Gather(place, branch_all, ag_send, ag_recv)

    def scatter(k, c, far):
        return Scatter(place, keep, c_out, c, None, far, (c_send.at[k], c_recv.at[k], far_send.at[k], far_recv.at[k]))

    rs_two = scatter(0, c_in, far_in)
    rs_out = scatter(1, c_in_two, far_in_two)
    rs_one = scatter(2, c_in, far_in)
    dw = Reduce(place, dw_keep, x_out, x_in, z_in, own_out, (x_send, x_recv, z_send, z_recv), own_sem)
    result = ffn_in.at[:tokens, :]
    weighted = ffn_in.at[tokens : tokens + length, :length]
    score_back = ffn_in.at[tokens : tokens + length, length : 2 * length]
    ring = {FD: 0, FG: 1, FU: 2, O: 3, G: 0, QK: 1, V: 2}

    def load(src, dst, index):
        copy = pltpu.make_async_copy(src, dst, load_sem.at[index])
        copy.start()
        return copy

    def over(count, size, body):
        def loop(i, carry):
            body(pl.ds(pl.multiple_of(i * size, size), size), i)
            return carry

        lax.fori_loop(0, count // size, loop, 0)

    in_cot = load(cot_ref, tokens_a, 3)
    in_hidden = load(hidden_ref, slim.at[:, 2 * cols :], 4)
    in_grads = load(grads_ref, slim.at[:, : 2 * cols], 0)
    in_fg = load(w_ref.at[FG], w.at[0], 1)
    in_fu = load(w_ref.at[FU], w.at[1], 2)
    in_ffn = load(ffn_in_ref, ffn_in, 5)
    in_middle = load(middle_ref, middle, 6)
    in_mixed = load(mixed_ref, mixed, 7)
    in_gate = load(gate_ref, gate_in, 8)
    in_o = load(w_ref.at[O], w.at[2], 9)
    in_qkv = load(qkv_ref, qkv, 10)
    for copy in column_copies(place, x_hbm, x_ref, load_sem.at[11], block):
        copy.start()
    sums[...] = jnp.zeros_like(sums)
    group_sum[...] = jnp.zeros_like(group_sum)
    entry_barrier(place, True)
    waited = []

    def ready(*copies):
        for copy in copies:
            if not any(copy is other for other in waited):
                waited.append(copy)
                copy.wait()

    def rows_of(i):
        return 3 - i, pl.ds(pl.multiple_of((3 - i) * tile, tile), tile)

    def two_part(i, carry):
        b, r = rows_of(i)
        rs_two.part(b, dot_nt(slim[r, :cols], w[0]) + dot_nt(slim[r, cols : 2 * cols], w[1]))
        return carry

    def gating(r, i):
        value = mixed[r, :]
        center = value - jnp.mean(value, axis=-1, keepdims=True)
        spread = jnp.mean(center * center, axis=-1, keepdims=True)
        gate = gate_in[r, :]
        flat = center * lax.rsqrt(jnp.maximum(spread, GROUP_FLOOR)) * group_ref[...]
        gated[r, :] = (flat * (gate * lax.logistic(gate))).astype(BF)

    def second_back(r, i):
        back, gain_sum, bias_sum = norm_back(middle[r, :], rs_two.own(r), params_ref[1:2, :])
        total = tokens_a[r, :].astype(F32) + back
        grad_middle[r, :] = total
        branch_all[r, :] = total.astype(BF)
        sums[1:2, :] += gain_sum
        sums[3:4, :] += bias_sum

    def out_part(i, carry):
        b, r = rows_of(i)
        rs_out.part(b, dot_nt(slim[r, 2 * cols :], w[0]))
        return carry

    def gating_back(b):
        r = pl.ds(pl.multiple_of(b * tile, tile), tile)
        back = dot_nn(branch_all[r, :], w[2])
        value = mixed[r, :]
        center = value - jnp.mean(value, axis=-1, keepdims=True)
        spread = jnp.mean(center * center, axis=-1, keepdims=True)
        inverse = lax.rsqrt(jnp.maximum(spread, GROUP_FLOOR))
        hat = center * inverse
        gate = gate_in[r, :]
        sigmoid = lax.logistic(gate)
        flat = hat * group_ref[...]
        slope = sigmoid * (1.0 + gate * (1.0 - sigmoid))
        slim[r, 2 * cols :] = (back * flat * slope).astype(BF)
        grad = back * (gate * sigmoid)
        group_sum[...] += jnp.sum(grad * hat, axis=0, keepdims=True)
        scaled = grad * group_ref[...]
        live = jnp.where(spread > GROUP_FLOOR, 1.0, jnp.where(spread == GROUP_FLOOR, 0.5, 0.0))
        moment = jnp.mean(scaled * hat, axis=-1, keepdims=True) * live
        mixed_back = inverse * (scaled - jnp.mean(scaled, axis=-1, keepdims=True) - hat * moment)
        slim[r, cols : 2 * cols] = mixed_back.astype(BF)

    def sequence_back(s):
        seq = pl.ds(pl.multiple_of(s * length, length), length)

        def body(i, carry):
            r = pl.ds(pl.multiple_of(s * length + i * tile, tile), tile)
            at = pl.ds(pl.multiple_of(i * tile, tile), tile)
            scores = dot_nt(qkv[r, :head_k], qkv[seq, head_k : 2 * head_k])
            here = cum_row_ref[pl.ds(s, 1), at]
            decays = decay_tile(
                place.t, cum_row_ref[pl.ds(s, 1), :], here, i * tile, tile, length, tokens
            )
            weighted[at, :] = (scores * decays * scale).astype(BF)
            back = dot_nt(slim[r, cols : 2 * cols], qkv[seq, 2 * head_k :])
            grad = (back * decays * scale).astype(BF)
            score_back[at, :] = grad
            slim[r, :head_k] = dot_nn(grad, qkv[seq, head_k : 2 * head_k]).astype(BF)
            return carry

        lax.fori_loop(0, length // tile, body, 0)
        slim[seq, head_k : 2 * head_k] = dot_tn(score_back[...], qkv[seq, :head_k]).astype(BF)
        slim[seq, cols : 2 * cols] = dot_tn(weighted[...], slim[seq, cols : 2 * cols]).astype(BF)


    def finish_out(r, i):
        result[r, :] = (middle[r, :] + rs_out.own(r)).astype(BF)

    def one_part(i, carry):
        b, r = rows_of(i)
        total = dot_nt(slim[r, :cols], w[1]) + dot_nt(slim[r, cols : 2 * cols], w[0])
        rs_one.part(b, total + dot_nt(slim[r, 2 * cols :], w[2]))
        return carry

    def first_back(r, i):
        back, gain_sum, bias_sum = norm_back(x_ref[r, :].astype(F32), rs_one.own(r), params_ref[0:1, :])
        result[r, :] = (grad_middle[r, :] + back).astype(BF)
        sums[0:1, :] += gain_sum
        sums[2:3, :] += bias_sum

    def sum_copy(k):
        peer = (place.c_peer(), place.y_peer())[k]
        return remote(sums, sums_in.at[k], sum_send.at[k], sum_recv.at[k], peer)

    pay = []
    for j, (bits, above, flips) in enumerate(place.pairs):
        position = (1 - place.z if flips else place.z) + above
        pay.append(remote(payload.at[position], payload_in.at[j], pay_send.at[j], pay_recv.at[j], place.peer(bits)))

    later = {}
    operands = {
        FD: (tokens_a, 2 * cols),
        FG: (ffn_in, 0),
        FU: (ffn_in, cols),
        O: (branch_all, None),
        QK: (tokens_a, 0),
        V: (tokens_a, cols),
        G: (tokens_a, 2 * cols),
    }

    def operands_of(g):
        ready(*{FD: (in_cot, in_hidden), FG: (in_ffn, in_grads), FU: (in_ffn, in_grads), O: ()}.get(g, (later.get(3),)))
        left, col = operands[g]
        return (left, gated, 0, step) if col is None else (left, slim, col, step)

    def two_step():
        ready(in_grads, in_fg, in_fu)
        lax.fori_loop(0, 4, two_part, 0)
        later[FD] = load(w_ref.at[FD], w.at[0], 1)
        later[QK] = load(w_ref.at[QK], w.at[1], 2)

    def gating_step():
        ready(in_mixed, in_gate)
        over(rows_all, tokens, gating)

    def second_step():
        ready(in_middle)
        rs_two.wait_own()
        over(tokens, 16, second_back)
        later[3] = load(normed_ref, tokens_a, 3)

    def out_step():
        rs_two.sent()
        ready(later[FD])
        lax.fori_loop(0, 4, out_part, 0)
        later[V] = load(w_ref.at[V], w.at[0], 1)

    def chip_step(first):
        ready(in_o, in_qkv)

        def chip(b, carry):
            ag.chip(2 * b)
            gating_back(b)
            return carry

        lax.fori_loop(first, first + 2, chip, 0)
        if first:
            later[G] = load(w_ref.at[G], w.at[2], 9)

    def sequence_step(s):
        lax.fori_loop(s, s + 1, lambda i, carry: (sequence_back(i), carry)[1], 0)

    def out_finish():
        rs_out.wait_own()
        over(tokens, 16, finish_out)
        later["layer"] = load(result, layer_out, 4)

    def one_step():
        rs_out.sent()
        ready(later[QK], later[V], later[G])
        lax.fori_loop(0, 4, one_part, 0)

    def first_step():
        pltpu.make_async_copy(x_hbm, x_ref, load_sem.at[11]).wait()
        ready(later["layer"])
        rs_one.wait_own()
        over(tokens, 16, first_back)
        later["grad"] = load(result, input_grad_out, 4)

    def sum_cores():
        sum_copy(0).start()

    def sum_chips():
        sum_copy(0).wait()
        sums[...] += sums_in[0]
        sum_copy(1).start()

    def pay_start():
        sum_copy(1).wait()
        sums[...] += sums_in[1]
        for p in range(n_dp):
            payload[p, 0:4, :] = sums[0:4, p * block : (p + 1) * block]
            for k in range(cols // block):
                payload[p, 4 + k : 5 + k, :] = group_sum[0:1, k * block : (k + 1) * block]
        for copy in pay:
            copy.start()

    def pay_finish():
        for copy in pay:
            copy.wait()
        mine = payload[place.z]
        other = jnp.zeros_like(mine)
        for j, (bits, above, flips) in enumerate(place.pairs):
            if flips:
                other = other + payload_in[j]
            else:
                mine = mine + payload_in[j]
        sums_out[0] = mine
        sums_out[1] = other

    before = {G: FD, QK: FG, V: FU}

    def upper(g):
        if g in before:
            dw.x_sent(before[g], ring[before[g]])
        dw.upper(g, ring[g], *operands_of(g))

    steps = {
        "two": two_step,
        "a3": lambda: rs_two.pass_on(3),
        "a1": lambda: rs_two.pass_on(1),
        "a2": lambda: rs_two.pass_on(2),
        "gat": gating_step,
        "lnb": second_step,
        "bs": ag.start,
        "bfz": ag.from_z,
        "bfy": ag.from_y,
        "bfzy": ag.from_zy,
        "out": out_step,
        "o3": lambda: rs_out.pass_on(3),
        "o1": lambda: rs_out.pass_on(1),
        "o2": lambda: rs_out.pass_on(2),
        "gbA": lambda: chip_step(0),
        "gbB": lambda: chip_step(2),
        "seq0": lambda: sequence_step(0),
        "seq1": lambda: sequence_step(1),
        "outf": out_finish,
        "one": one_step,
        "b3": lambda: rs_one.pass_on(3),
        "b1": lambda: rs_one.pass_on(1),
        "b2": lambda: rs_one.pass_on(2),
        "lna": first_step,
        "sc": sum_cores,
        "sy": sum_chips,
        "pay": pay_start,
        "payw": pay_finish,
    }
    for name in BACKWARD:
        if name in steps:
            steps[name]()
        elif name[0] == "u":
            upper(int(name[1]))
        elif name[0] == "l":
            dw.lower(int(name[1]), *operands_of(int(name[1])))
        else:
            dw.step(int(name[1]), ring[int(name[1])], int(name[2]))
    ready(later["grad"])
    for g in (O, G, QK, V):
        dw.x_sent(g, ring[g])
    ag.sent()
    rs_one.sent()
    for g in (FD, FG, FU, O, G, QK, V):
        dw.finish(g)


def backward_call(n_dp, x, params, group, cum_row, saved):
    tokens, width = x.shape
    rows_all = 8 * tokens
    w = saved[0]
    cols = w.shape[2]
    block = width // n_dp
    masks = n_dp // 2 - 1
    vmem, hbm = pl.BlockSpec(memory_space=pltpu.VMEM), pl.BlockSpec(memory_space=pl.ANY)
    shape = jax.ShapeDtypeStruct
    pay_rows = -(-(4 + cols // block) // 8) * 8
    outs = (
        shape((tokens, width), BF),
        shape((tokens, width), BF),
        shape((GROUPS, block, cols), BF),
        shape((GROUPS, masks, block, cols), BF),
        shape((2, pay_rows, block), F32),
    )
    dma = pltpu.SemaphoreType.DMA
    scratch = [
        pltpu.VMEM((3, width, cols), BF),
        pltpu.VMEM((rows_all, width), BF),
        pltpu.VMEM((rows_all, width), BF),
        pltpu.VMEM((rows_all, width), BF),
        pltpu.VMEM((rows_all, 3 * cols), BF),
        pltpu.VMEM((rows_all, 2 * cols), BF),
        pltpu.VMEM((rows_all, cols), F32),
        pltpu.VMEM((rows_all, cols), F32),
        pltpu.VMEM((rows_all, cols), BF),
        pltpu.VMEM((tokens, width), BF),
        pltpu.VMEM((tokens, width), F32),
        pltpu.VMEM((tokens, width), F32),
        pltpu.VMEM((8, width), F32),
        pltpu.VMEM((2, 8, width), F32),
        pltpu.VMEM((1, cols), F32),
        pltpu.VMEM((n_dp, pay_rows, block), F32),
        pltpu.VMEM((n_dp - 1, pay_rows, block), F32),
        pltpu.VMEM((4, tokens, width), BF),
        pltpu.VMEM((4, tokens, width), BF),
        pltpu.VMEM((4, tokens, width), BF),
        pltpu.VMEM((3, tokens, width), BF),
        pltpu.VMEM((4, tokens, width), BF),
        pltpu.VMEM((3, tokens, width), BF),
        pltpu.VMEM((GROUPS, width // 2, cols), BF),
        pltpu.VMEM((4, width // 2, cols), BF),
        pltpu.VMEM((GROUPS, width // 2, cols), BF),
        dma((7,)),
        dma((7,)),
        dma((3, 4)),
        dma((3, 4)),
        dma((3, 3)),
        dma((3, 3)),
        dma((GROUPS,)),
        dma((GROUPS, n_dp // 2)),
        dma((GROUPS,)),
        dma((GROUPS, masks)),
        dma((12,)),
        dma((GROUPS,)),
        dma((2,)),
        dma((2,)),
        dma((n_dp - 1,)),
        dma((n_dp - 1,)),
    ]
    return pl.pallas_call(
        functools.partial(backward_kernel, n_dp),
        out_shape=outs,
        in_specs=[hbm, vmem, vmem, vmem] + [hbm] * len(saved),
        out_specs=(hbm,) * 4 + (vmem,),
        scratch_shapes=scratch,
        compiler_params=pltpu.CompilerParams(
            collective_id=2, has_side_effects=True, vmem_limit_bytes=67_000_000
        ),
    )(x, params, group, cum_row, *saved)


def finish_kernel(
    n_dp,
    own_ref,
    others_ref,
    layer_ref,
    grad_ref,
    sums_ref,
    layer_out,
    input_grad,
    query_grad,
    key_grad,
    value_grad,
    gate_grad,
    out_grad,
    group_grad,
    gain_grad,
    bias_grad,
    ffn_gate_grad,
    ffn_up_grad,
    ffn_down_grad,
    own,
    others,
    rows,
    wide,
    tall,
    in_sem,
    out_sem,
    row_sem,
):
    place = Place(n_dp)
    z = place.z
    block, cols = own.shape[1:]
    loads = []
    for g in (FD, FG, FU, O, QK, V, G):
        pair = (
            pltpu.make_async_copy(own_ref.at[g], own.at[g], in_sem.at[0, g]),
            pltpu.make_async_copy(others_ref.at[g], others.at[g], in_sem.at[1, g]),
        )
        for copy in pair:
            copy.start()
        loads.append((g, pair))
    row_loads = [
        pltpu.make_async_copy(layer_ref, rows.at[0], row_sem.at[0]),
        pltpu.make_async_copy(grad_ref, rows.at[1], row_sem.at[1]),
    ]
    for copy in row_loads:
        copy.start()
    outs = []

    def save(src, dst, index):
        copy = pltpu.make_async_copy(src, dst, out_sem.at[index])
        copy.start()
        outs.append(copy)

    wide_at = {FG: 0, FU: 1, V: 2, G: 3, QK: 4}
    tall_at = {FD: 0, O: 1}
    targets = {FG: ffn_gate_grad, FU: ffn_up_grad, V: value_grad, G: gate_grad, FD: ffn_down_grad, O: out_grad}
    for g, pair in loads:
        for copy in pair:
            copy.wait()
        mine = own[g].astype(F32)
        theirs = None
        for i, (bits, above, flips) in enumerate(place.masks):
            value = others[g, i].astype(F32)
            if not flips:
                mine = mine + value
            else:
                theirs = value if theirs is None else theirs + value
        if g in tall_at:
            k = tall_at[g]
            tall[k, pl.ds(pl.multiple_of(z * cols, cols), cols), :] = mine.T
            tall[k, pl.ds(pl.multiple_of((1 - z) * cols, cols), cols), :] = theirs.T
            save(tall.at[k], targets[g], k)
            continue
        k = wide_at[g]
        if g == QK:
            half = cols // 2
            for which, dst in ((0, query_grad), (1, key_grad)):
                part = slice(which * half, (which + 1) * half)
                at = which * cols
                wide[k, :, pl.ds(pl.multiple_of(at + z * half, half), half)] = mine[:, part]
                wide[k, :, pl.ds(pl.multiple_of(at + (1 - z) * half, half), half)] = theirs[:, part]
                save(wide.at[k, :, pl.ds(at, cols)], dst, 2 + which)
            continue
        wide[k, :, pl.ds(pl.multiple_of(z * cols, cols), cols)] = mine
        wide[k, :, pl.ds(pl.multiple_of((1 - z) * cols, cols), cols)] = theirs
        save(wide.at[k], targets[g], 4 + k)
    for k, dst in ((0, layer_out), (1, input_grad)):
        row_loads[k].wait()
        for copy in column_copies(place, rows.at[k], dst, row_sem.at[k], block, True):
            copy.start()
    norm = sums_ref[0, 0:4, :] + sums_ref[1, 0:4, :]
    piece = gain_grad.shape[1]
    mine = norm[:, :piece]
    for k in range(1, block // piece):
        mine = jnp.where(place.t == k, norm[:, k * piece : (k + 1) * piece], mine)
    gain_grad[...] = mine[0:2, :]
    bias_grad[...] = mine[2:4, :]
    piece = group_grad.shape[1]
    here = place.d % (block // piece)
    row = place.d // (block // piece)

    def group_of(which):
        value = sums_ref[which, 4:5, :]
        for k in range(1, cols // block):
            value = jnp.where(row == k, sums_ref[which, 4 + k : 5 + k, :], value)
        out = value[:, :piece]
        for k in range(1, block // piece):
            out = jnp.where(here == k, value[:, k * piece : (k + 1) * piece], out)
        return out

    same, other = group_of(0), group_of(1)
    group_grad[0:1, :] = jnp.where(z == 0, same, other)
    group_grad[1:2, :] = jnp.where(z == 0, other, same)
    for copy in outs:
        copy.wait()
    for k, dst in ((0, layer_out), (1, input_grad)):
        pltpu.make_async_copy(rows.at[k], dst, row_sem.at[k]).wait()


def finish_call(n_dp, n_tensor, own, others, layer, grad, sums):
    tokens, width = layer.shape
    block, cols = own.shape[1:]
    masks = others.shape[1]
    vmem, hbm = pl.BlockSpec(memory_space=pltpu.VMEM), pl.BlockSpec(memory_space=pl.ANY)
    shape = jax.ShapeDtypeStruct
    rows, wide, tall = shape((tokens, width), BF), shape((block, 2 * cols), F32), shape((2 * cols, block), F32)
    thin, norm = shape((block, cols), F32), shape((2, width // (n_dp * n_tensor)), F32)
    outs = (rows, rows, thin, thin, wide, wide, tall, shape((2, cols // n_dp), F32), norm, norm, wide, wide, tall)
    specs = [vmem if o.shape[0] == 2 else hbm for o in outs]
    dma = pltpu.SemaphoreType.DMA
    return pl.pallas_call(
        functools.partial(finish_kernel, n_dp),
        out_shape=outs,
        in_specs=[hbm, hbm, hbm, hbm, vmem],
        out_specs=tuple(specs),
        scratch_shapes=[
            pltpu.VMEM((GROUPS, block, cols), BF),
            pltpu.VMEM((GROUPS, masks, block, cols), BF),
            pltpu.VMEM((2, tokens, width), BF),
            pltpu.VMEM((5, block, 2 * cols), F32),
            pltpu.VMEM((2, 2 * cols, block), F32),
            dma((2, GROUPS)),
            dma((8,)),
            dma((2,)),
        ],
        compiler_params=pltpu.CompilerParams(vmem_limit_bytes=67_000_000),
    )(own, others, layer, grad, sums)


def per_device(
    n_dp,
    n_tensor,
    inputs,
    cotangent,
    log_decay,
    query_weight,
    key_weight,
    value_weight,
    gate_weight,
    out_weight,
    group_gain,
    norm_gains,
    norm_biases,
    ffn_gate_weight,
    ffn_up_weight,
    ffn_down_weight,
):
    place = Place(n_dp)
    d, t = place.d, place.t
    tokens, width = inputs.shape
    block = width // n_dp
    head_v = value_weight.shape[1] // 2

    def position_of(q):
        out = (q // PAIR) & 1
        for k, bit in enumerate(place.rest):
            out = out + ((d // bit) % 2 ^ ((q // bit) & 1)) * (2 << k)
        return out

    def moved(value, index):
        if block % 128 == 0:
            return value
        return jnp.concatenate(
            [lax.dynamic_slice_in_dim(value, index(p) * block, block, 1) for p in range(n_dp)], axis=1
        )

    def half(value, which, axis):
        size = value.shape[axis] // 2
        return lax.dynamic_slice_in_dim(value, which * size, size, axis)

    cumul = jnp.cumsum(log_decay, axis=1).reshape(2, n_tensor, tokens)
    for bit in (1, 2):
        swapped = jnp.concatenate([cumul[:, j ^ bit : (j ^ bit) + 1] for j in range(n_tensor)], axis=1)
        cumul = jnp.where((t // bit) % 2 == 1, swapped, cumul)
    spread = jnp.tile(group_gain.astype(F32), (1, n_dp))
    spread = jnp.where(lax.broadcasted_iota(jnp.int32, spread.shape, 1) // (head_v // n_dp) == d, spread, 0.0)
    parts = [norm_gains.astype(F32), norm_biases.astype(F32), spread, cumul]
    small = jnp.concatenate([part.reshape(-1, block) for part in parts], axis=0)
    small = jnp.pad(small, ((0, -small.shape[0] % 8), (0, 0)))

    def interleaved(first, second):
        parts = [half(first, 0, 1), half(second, 0, 1), half(first, 1, 1), half(second, 1, 1)]
        return jnp.concatenate(parts, axis=1)

    sources = [
        interleaved(query_weight, key_weight),
        value_weight,
        gate_weight,
        out_weight.T,
        ffn_gate_weight,
        ffn_up_weight,
        ffn_down_weight.T,
    ]

    x, cot = moved(inputs, place.dp_of), moved(cotangent, place.dp_of)
    *saved, params, group, cumul = forward_call(n_dp, x, cot, small, sources)
    layer, grad, own, others, sums = backward_call(n_dp, x, params, group, cumul, saved)
    outs = finish_call(n_dp, n_tensor, own, others, layer, grad, sums)
    return (moved(outs[0], position_of), moved(outs[1], position_of), *outs[2:])


def solution(mesh):
    tokens = P(("dp", "tensor"), None)
    rows, cols, norms = P("dp", "tensor"), P("tensor", "dp"), P(None, "dp")
    sums = P(None, ("dp", "tensor"))
    in_specs = (tokens, tokens, cols, rows, rows, rows, rows, cols, cols, norms, norms, rows, rows, cols)
    out_specs = (tokens, tokens, rows, rows, rows, rows, cols, cols, sums, sums, rows, rows, cols)
    body = functools.partial(per_device, mesh.shape["dp"], mesh.shape["tensor"])
    return jax.shard_map(body, mesh=mesh, in_specs=in_specs, out_specs=out_specs, check_vma=False)
```

```python
import functools
import math

import jax
import jax.numpy as jnp
from jax import lax
from jax.experimental import pallas as pl
from jax.experimental.pallas import tpu as pltpu
from jax.sharding import PartitionSpec as P

EPSILON = 1e-05
GROUP_FLOOR = 1.0
BF = jnp.bfloat16
F32 = jnp.float32
PAIR = 2
MESH = pl.DeviceIdType.MESH
QK, V, G, O, FG, FU, FD = range(7)
GROUPS = 7


FORWARD = (
    "x2", "x3", "x0", "s01", "s22", "s02", "s21", "s41", "s12", "x1", "f01", "s31", "small", "ln", "f22", "ns",
    "s03", "f41", "f02", "nfy", "s23", "f12", "x6", "s32", "s13", "f31", "s11", "nfz", "f21", "f03", "f32", "ks",
    "s33", "s53", "nfzy", "f11", "s43", "s51", "f23", "qk", "f13", "kfz", "f33", "v", "g", "f53", "kfy", "s52",
    "o", "p3", "f51", "p1", "s61", "x5", "f52", "s42", "p2", "f42", "s63", "kfzy", "x4", "f43", "ln2", "f61", "ts",
    "feedA", "tfy", "s62", "tfz", "feedB", "f63", "f62", "tfzy", "feedC", "feedD", "back",
)
BACKWARD = (
    "u6", "two", "a3", "l6", "s63", "u4", "a1", "a2", "l4", "s43", "lnb", "bs", "gat", "out", "o3", "l5", "s42",
    "bfy", "u5", "s62", "s41", "bfz", "gbA", "s40", "o1", "o2", "bfzy", "s53", "s52", "gbB", "u3", "seq0", "l3",
    "s60", "s61", "seq1", "outf", "one", "s51", "s33", "u1", "u2", "s32", "b3", "b2", "u0", "s30", "l1", "l0",
    "s13", "s12", "b1", "s50", "lna", "s11", "l2", "sc", "s22", "s21", "sy", "s20", "pay", "s31", "s10", "s23",
    "s01", "s03", "s02", "payw", "s00",
)


def dot_nn(a, b):
    return lax.dot_general(a, b, (((1,), (0,)), ((), ())), preferred_element_type=F32)


def dot_nt(a, b):
    return lax.dot_general(a, b, (((1,), (1,)), ((), ())), preferred_element_type=F32)


def dot_tn(a, b):
    return lax.dot_general(a, b, (((0,), (0,)), ((), ())), preferred_element_type=F32)


def flip(index, bit):
    return index + bit - 2 * bit * ((index // bit) % 2)


class Place:
    def __init__(self, n_dp):
        self.n_dp = n_dp
        self.d = lax.axis_index("dp")
        self.t = lax.axis_index("tensor")
        self.z = (self.d // PAIR) % 2
        self.rest = [1 << i for i in range(2, n_dp.bit_length() - 1)] + [1]
        self.inner = self.rest[:-1]
        self.masks = []
        for pick in range(1, 1 << (1 + len(self.inner))):
            bits = [PAIR] * (pick & 1) + [b for k, b in enumerate(self.inner) if (pick >> (k + 1)) & 1]
            self.masks.append((bits, pick & ~1, pick & 1))
        half = n_dp // 2
        self.pairs = self.masks + [([1], half, 0)] + [(bits + [1], above + half, flips) for bits, above, flips in self.masks]

    def slot(self, above, flips):
        return next((j for j, pair in enumerate(self.pairs) if pair[1:] == (above, flips)), None)

    def dp_of(self, p):
        out = (p & 1) * PAIR
        for k, bit in enumerate(self.rest):
            here = (self.d // bit) % 2
            out = out + (1 - here if (p >> (k + 1)) & 1 else here) * bit
        return out

    def peer(self, bits):
        out = self.d
        for bit in bits:
            out = flip(out, bit)
        return {"dp": out}

    def x_peer(self):
        return {"dp": flip(self.d, 1)}

    def z_peer(self):
        return {"dp": flip(self.d, PAIR)}

    def y_peer(self):
        return {"tensor": flip(self.t, 2)}

    def c_peer(self):
        return {"tensor": flip(self.t, 1)}

    def everyone(self, far):
        near = [self.x_peer(), self.y_peer(), self.c_peer()]
        if far:
            return near[1:] + [self.peer(bits) for bits, _, _ in self.pairs]
        return near + [self.peer(bits) for bits, _, _ in self.masks]


def greet(place, far):
    barrier = pltpu.get_barrier_semaphore()
    for peer in place.everyone(far):
        pl.semaphore_signal(barrier, inc=1, device_id=peer, device_id_type=MESH)


def met(place, far):
    pl.semaphore_wait(pltpu.get_barrier_semaphore(), len(place.everyone(far)))


def entry_barrier(place, far=False):
    greet(place, far)
    met(place, far)


def column_copies(place, src, dst, sem, block, back=False):
    if block % 128:
        return [pltpu.make_async_copy(src, dst, sem)]
    out = []
    for p in range(place.n_dp):
        natural = pl.ds(pl.multiple_of(place.dp_of(p) * block, block), block)
        here = pl.ds(p * block, block)
        a, b = (here, natural) if back else (natural, here)
        out.append(pltpu.make_async_copy(src.at[:, a], dst.at[:, b], sem))
    return out


def remote(src, dst, send, recv, peer):
    return pltpu.make_async_remote_copy(
        src_ref=src, dst_ref=dst, send_sem=send, recv_sem=recv, device_id=peer, device_id_type=MESH
    )


class Weights:
    def __init__(self, place, sources, full, sems):
        self.place, self.sources, self.full = place, sources, full
        self.z_send, self.z_recv, self.x_send, self.x_recv, self.local = sems
        self.block = sources[-1].shape[0]
        self.cols = sources[-1].shape[1] // 2
        self.half = place.n_dp // 2

    def rows(self, position, count=1):
        return pl.ds(pl.multiple_of(position * self.block, self.block), count * self.block)

    def pairs(self, g, half, position):
        parts = self.sources[g] if isinstance(self.sources[g], tuple) else (self.sources[g],)
        count = self.cols // len(parts)
        for k, part in enumerate(parts):
            columns = pl.ds(pl.multiple_of(half * count, count), count)
            yield part.at[:, columns], self.full.at[g, self.rows(position), k * count : (k + 1) * count]

    def own(self, g):
        z = self.place.z
        for src, dst in self.pairs(g, z, z):
            pltpu.make_async_copy(src, dst, self.local.at[g]).start()
        for src, dst in self.pairs(g, z, z + self.half):
            remote(src, dst, self.x_send.at[g], self.x_recv.at[g], self.place.x_peer()).start()

    def some(self, third):
        count = len(self.place.masks)
        return reversed(range(third * count // 3, (third + 1) * count // 3))

    def start(self, g, third):
        z = self.place.z
        for i in self.some(third):
            bits, above, flips = self.place.masks[i]
            for src, dst in self.pairs(g, 1 - z if flips else z, z + above):
                remote(src, dst, self.z_send.at[g], self.z_recv.at[g, i], self.place.peer(bits)).start()

    def forward(self, g, third):
        for i in self.some(third):
            bits, above, flips = self.place.masks[i]
            position = (1 - self.place.z if flips else self.place.z) + above
            here = self.full.at[g, self.rows(position), :]
            remote(here, here, self.z_send.at[g], self.z_recv.at[g, i], self.place.peer(bits)).wait_recv()
            remote(
                here,
                self.full.at[g, self.rows(position + self.half), :],
                self.x_send.at[g],
                self.x_recv.at[g],
                self.place.x_peer(),
            ).start()

    def finish(self, g):
        z = self.place.z
        here = self.full.at[g, self.rows(z), :]
        pltpu.make_async_copy(here, here, self.local.at[g]).wait()
        there = self.full.at[g, self.rows(self.half, self.half), :]
        remote(there, there, self.x_send.at[g], self.x_recv.at[g], self.place.x_peer()).wait_recv()

    def sent(self, g):
        there = self.full.at[g, self.rows(self.half, self.half), :]
        remote(there, there, self.x_send.at[g], self.x_recv.at[g], self.place.x_peer()).wait_send()
        count = self.half - 1
        those = self.full.at[g, self.rows(0, count), :]
        remote(those, those, self.z_send.at[g], self.z_recv.at[g, 0], self.place.x_peer()).wait_send()


class Gather:
    def __init__(self, place, buffer, send, recv):
        self.place, self.buffer = place, buffer
        self.send, self.recv = send, recv
        self.tokens = buffer.shape[0] // 8
        self.peers = {1: place.c_peer(), 2: place.y_peer(), 4: place.z_peer()}

    def slot(self, s):
        return self.buffer.at[pl.ds(pl.multiple_of(s * self.tokens, self.tokens), self.tokens), :]

    def copy(self, source, bit, src=None):
        s = source + bit
        return remote(self.slot(source) if src is None else src, self.slot(s), self.send.at[s - 1], self.recv.at[s - 1], self.peers[bit])

    def start(self, src=None):
        for bit in (4, 2, 1):
            self.copy(0, bit, src).start()

    def from_z(self):
        self.copy(0, 4).wait_recv()
        self.copy(4, 2).start()
        self.copy(4, 1).start()

    def from_y(self):
        self.copy(0, 2).wait_recv()
        self.copy(2, 1).start()

    def from_zy(self):
        self.copy(4, 2).wait_recv()
        self.copy(6, 1).start()

    def chip(self, source):
        self.copy(source, 1).wait_recv()

    def sent(self, src=None):
        self.copy(0, 4, src).wait_send()
        self.copy(0, 2, src).wait_send()
        self.copy(0, 1, src).wait_send()
        self.copy(4, 2).wait_send()
        self.copy(4, 1).wait_send()
        self.copy(2, 1).wait_send()
        self.copy(6, 1).wait_send()


class Scatter:
    def __init__(self, place, keep, c_out, c_in, far_out, far_in, sems):
        self.place = place
        self.keep, self.c_out, self.c_in, self.far_out, self.far_in = keep, c_out, c_in, far_out, far_in
        self.c_send, self.c_recv, self.far_send, self.far_recv = sems
        self.tokens = c_out.shape[1]

    def part(self, b, value):
        self.keep[b] = value[: self.tokens].astype(self.keep.dtype)
        self.c_out[b] = value[self.tokens :].astype(BF)
        self.c_copy(b).start()

    def c_copy(self, b):
        return remote(self.c_out.at[b], self.c_in.at[b], self.c_send.at[b], self.c_recv.at[b], self.place.c_peer())

    def far_copy(self, b):
        peer = self.place.z_peer() if b == 2 else self.place.y_peer()
        return remote(
            self.far_source(b), self.far_in.at[b - 1], self.far_send.at[b - 1], self.far_recv.at[b - 1], peer
        )

    def far_source(self, b):
        return self.keep.at[b] if self.far_out is None else self.far_out.at[b - 1]

    def rows(self, body, step=16):
        def loop(i, carry):
            body(pl.ds(pl.multiple_of(i * step, step), step))
            return carry

        lax.fori_loop(0, self.tokens // step, loop, 0)

    def pass_on(self, b):
        self.c_copy(b).wait_recv()
        if b == 2:
            self.far_copy(3).wait_recv()

        def body(r):
            total = self.keep[b, r, :].astype(F32) + self.c_in[b, r, :].astype(F32)
            if b == 2:
                total = total + self.far_in[2, r, :].astype(F32)
            self.far_source(b)[r, :] = total.astype(BF)

        self.rows(body)
        self.far_copy(b).start()

    def wait_own(self):
        self.c_copy(0).wait_recv()
        self.far_copy(1).wait_recv()
        self.far_copy(2).wait_recv()

    def own(self, r):
        return (
            self.keep[0, r, :].astype(F32)
            + self.c_in[0, r, :].astype(F32)
            + self.far_in[0, r, :].astype(F32)
            + self.far_in[1, r, :].astype(F32)
        )

    def sent(self):
        for b in range(4):
            self.c_copy(b).wait_send()
        for b in (3, 2, 1):
            self.far_copy(b).wait_send()


def normalized(value):
    center = value - jnp.mean(value, axis=-1, keepdims=True)
    spread = jnp.mean(center * center, axis=-1, keepdims=True)
    return center * lax.rsqrt(spread + EPSILON)


def decay_tile(t, cumul_rows, cumul_here, first, rows, length, tokens):
    square = (rows, rows)
    same = lax.broadcasted_iota(jnp.int32, square, 0) == lax.broadcasted_iota(jnp.int32, square, 1)
    cumul_cols = jnp.sum(jnp.where(same, cumul_here, 0.0), axis=1, keepdims=True)
    index = lax.broadcasted_iota(jnp.int32, (rows, length), 0) + first
    other = lax.broadcasted_iota(jnp.int32, (rows, length), 1)
    at = ((index // tokens) ^ t) * tokens + index % tokens
    to = ((other // tokens) ^ t) * tokens + other % tokens
    causal = at >= to
    return jnp.where(causal, jnp.exp(jnp.where(causal, cumul_cols - cumul_rows, 0.0)), 0.0)


def pack_small(place, small, gains, biases, group, decay, tokens):
    block = small.shape[1]
    wide = place.n_dp * group.shape[1]
    length = decay.shape[1]
    small[...] = jnp.zeros_like(small)
    small[0:2, :] = gains[...].astype(F32)
    small[2:4, :] = biases[...].astype(F32)
    lane = lax.broadcasted_iota(jnp.int32, (2, wide), 1)
    tiled = jnp.concatenate([group[...].astype(F32)] * place.n_dp, axis=1)
    spread = jnp.where(lane // group.shape[1] == place.d, tiled, 0.0)
    at = 4
    for h in range(2):
        for k in range(wide // block):
            small[at : at + 1, :] = spread[h : h + 1, k * block : (k + 1) * block]
            at += 1
    total = decay[...]
    lane = lax.broadcasted_iota(jnp.int32, total.shape, 1)
    shift = 1
    while shift < length:
        total = total + jnp.where(lane >= shift, pltpu.roll(total, shift, 1), 0.0)
        shift *= 2
    for bit in (1, 2):
        pieces = [total[:, (j ^ bit) * tokens : ((j ^ bit) + 1) * tokens] for j in range(length // tokens)]
        total = jnp.where((place.t // bit) % 2 == 1, jnp.concatenate(pieces, axis=1), total)
    for h in range(2):
        for k in range(length // block):
            small[at : at + 1, :] = total[h : h + 1, k * block : (k + 1) * block]
            at += 1


def spread_small(place, own, others, params, group, cumul, block):
    pieces = group.shape[1] // block
    steps = cumul.shape[1] // block
    first = place.z == 0

    def of(above, flips, rows):
        j = place.slot(above, flips)
        return own[rows, :] if j is None else others[j, rows, :]

    head = slice(0, 4)
    for p in range(place.n_dp):
        same, flipped = of(p & ~1, 0, head), of(p & ~1, 1, head)
        params[head, p * block : (p + 1) * block] = jnp.where(place.z == p % 2, same, flipped)

    def head_rows(above, flips, at, count):
        one = of(above, flips, slice(at, at + count))
        two = of(above, flips, slice(at + count, at + 2 * count))
        return jnp.where(first, one, two)

    total = head_rows(0, 0, 4, pieces)
    for bits, above, flips in place.pairs:
        total = total + head_rows(above, flips, 4, pieces)
    for k in range(pieces):
        group[0:1, k * block : (k + 1) * block] = total[k : k + 1, :]
    at = 4 + 2 * pieces
    for row, flips in ((0, 0), (1, 1)):
        value = head_rows(0, flips, at, steps)
        for k in range(steps):
            cumul[row : row + 1, k * block : (k + 1) * block] = value[k : k + 1, :]


def forward_kernel(
    n_dp,
    x_hbm,
    cot_hbm,
    gains_ref,
    biases_ref,
    group_gain_ref,
    decay_ref,
    s_q,
    s_k,
    s_v,
    s_g,
    s_o,
    s_fg,
    s_fu,
    s_fd,
    w_out,
    normed_out,
    qkv_out,
    gate_out,
    mixed_out,
    ffn_in_out,
    hidden_out,
    grads_out,
    cot_out,
    middle_out,
    params_out,
    group_out,
    cumul_out,
    small_ref,
    small_in,
    turned,
    natural,
    params_ref,
    group_ref,
    cum_row_ref,
    x_ref,
    w,
    normed_all,
    cot_all,
    ffn_in,
    qkv,
    gate_in,
    mixed,
    gated,
    gate_hidden,
    up_hidden,
    hidden,
    grads,
    middle,
    keep,
    c_out,
    c_in,
    far_out,
    far_in,
    z_send,
    z_recv,
    x_send,
    x_recv,
    w_local,
    ag_send,
    ag_recv,
    c_send,
    c_recv,
    far_send,
    far_recv,
    out_sem,
    small_send,
    small_recv,
):
    place = Place(n_dp)
    tokens, width = x_ref.shape
    block = width // n_dp
    rows_all = 8 * tokens
    length = rows_all // 2
    head_k = qkv.shape[1] // 4
    scale = 1.0 / math.sqrt(head_k)
    tile = 2 * tokens
    weights = Weights(place, [(s_q, s_k), s_v, s_g, turned.at[0], s_fg, s_fu, turned.at[1]], w, (z_send, z_recv, x_send, x_recv, w_local))
    ag_normed = Gather(place, normed_all, ag_send.at[0], ag_recv.at[0])
    ag_cot = Gather(place, cot_all, ag_send.at[1], ag_recv.at[1])
    ag_two = Gather(place, ffn_in, ag_send.at[2], ag_recv.at[2])
    branch = Scatter(place, keep, c_out, c_in, far_out, far_in, (c_send, c_recv, far_send, far_recv))
    outs = []

    def save(src, dst, index):
        copy = pltpu.make_async_copy(src, dst, out_sem.at[index])
        copy.start()
        outs.append(copy)

    def over(count, step, body):
        def loop(i, carry):
            body(pl.ds(pl.multiple_of(i * step, step), step), i)
            return carry

        lax.fori_loop(0, count // step, loop, 0)

    for copy in column_copies(place, x_hbm, x_ref, out_sem.at[16], block):
        copy.start()
    for copy in column_copies(place, cot_hbm, ag_cot.slot(0), out_sem.at[17], block):
        copy.start()
    flat = [
        pltpu.make_async_copy(s_o, natural.at[0], out_sem.at[21]),
        pltpu.make_async_copy(s_fd, natural.at[1], out_sem.at[22]),
    ]
    for copy in flat:
        copy.start()
    greet(place, True)
    pack_small(place, small_ref, gains_ref, biases_ref, group_gain_ref, decay_ref, tokens)
    for k, copy in enumerate(flat):
        copy.wait()
        cols = w.shape[2]
        for j in range(2):
            turned[k, :, j * cols : (j + 1) * cols] = natural[k, j * cols : (j + 1) * cols, :].T
    met(place, True)
    small = []
    for j, (bits, above, flips) in enumerate(place.pairs):
        copy = remote(small_ref, small_in.at[j], small_send.at[j], small_recv.at[j], place.peer(bits))
        copy.start()
        small.append(copy)
    size = gate_hidden.shape[1]

    def first_norm(r, i):
        value = normalized(x_ref[r, :].astype(F32))
        normed_all[r, :] = (value * params_ref[0:1, :] + params_ref[2:3, :]).astype(BF)

    def make_qk(r, i):
        qkv[r, : 2 * head_k] = dot_nn(normed_all[r, :], w[QK]).astype(BF)

    def make_v(r, i):
        qkv[r, 2 * head_k :] = dot_nn(normed_all[r, :], w[V]).astype(BF)

    def retention(r, i):
        start = pl.multiple_of((i // 2) * length, length)
        seq = pl.ds(start, length)
        scores = dot_nt(qkv[r, :head_k], qkv[seq, head_k : 2 * head_k])
        here = cum_row_ref[pl.ds(i // 2, 1), pl.ds(pl.multiple_of((i % 2) * tile, tile), tile)]
        decays = decay_tile(
            place.t, cum_row_ref[pl.ds(i // 2, 1), :], here, (i % 2) * tile, tile, length, tokens
        )
        weighted = (scores * decays * scale).astype(BF)
        mixed[r, :] = dot_nn(weighted, qkv[seq, 2 * head_k :])

    def gating(r, i):
        gate = dot_nn(normed_all[r, :], w[G])
        gate_in[r, :] = gate
        value = mixed[r, :]
        center = value - jnp.mean(value, axis=-1, keepdims=True)
        spread = jnp.mean(center * center, axis=-1, keepdims=True)
        flat = center * lax.rsqrt(jnp.maximum(spread, GROUP_FLOOR)) * group_ref[...]
        gated[r, :] = (flat * (gate * lax.logistic(gate))).astype(BF)

    def branch_part(i, carry):
        r = pl.ds(pl.multiple_of((3 - i) * tile, tile), tile)
        branch.part(3 - i, dot_nt(gated[r, :], w[O]))
        return carry

    def second_norm(r, i):
        value = x_ref[r, :].astype(F32) + branch.own(r)
        middle[r, :] = value
        ffn_in[r, :] = (normalized(value) * params_ref[1:2, :] + params_ref[3:4, :]).astype(BF)

    def feed(b):
        r = pl.ds(pl.multiple_of(b * tile, tile), tile)
        gate = dot_nn(ffn_in[r, :], w[FG])
        up = dot_nn(ffn_in[r, :], w[FU])
        gate_hidden[r, :] = gate
        up_hidden[r, :] = up
        hidden[r, :] = (gelu(gate) * up).astype(BF)

    def feed_back(r, i):
        back = dot_nn(cot_all[r, :], w[FD])
        gate = gate_hidden[r, :]
        value, slope = gelu_and_slope(gate)
        grads[r, :size] = (back * up_hidden[r, :] * slope).astype(BF)
        grads[r, size:] = (back * value).astype(BF)

    def small_step():
        pltpu.make_async_copy(x_hbm, x_ref, out_sem.at[16]).wait()
        for copy in small:
            copy.wait()
        spread_small(place, small_ref, small_in, params_ref, group_ref, cum_row_ref, block)

    def norm_step():
        over(tokens, 16, first_norm)

    def cot_start():
        pltpu.make_async_copy(cot_hbm, ag_cot.slot(0), out_sem.at[17]).wait()
        ag_cot.start()

    def chips(ag):
        lax.fori_loop(0, 4, lambda b, carry: (ag.chip(2 * b), carry)[1], 0)

    def qk_step():
        chips(ag_normed)
        weights.finish(QK)
        over(rows_all, tile, make_qk)
        save(normed_all, normed_out, 0)
        save(w.at[QK], w_out.at[QK], 1)
        save(params_ref, params_out, 18)
        save(group_ref, group_out, 19)
        save(cum_row_ref, cumul_out, 20)

    def v_step():
        weights.finish(V)
        over(rows_all, tile, make_v)
        over(rows_all, tile, retention)
        save(w.at[V], w_out.at[V], 2)
        save(qkv, qkv_out, 3)
        save(mixed, mixed_out, 4)

    def g_step():
        weights.finish(G)
        over(rows_all, tile, gating)
        save(w.at[G], w_out.at[G], 5)
        save(gate_in, gate_out, 6)

    def o_step():
        weights.finish(O)
        lax.fori_loop(0, 4, branch_part, 0)
        save(w.at[O], w_out.at[O], 7)

    def second_step():
        branch.wait_own()
        over(tokens, 16, second_norm)
        save(middle, middle_out, 9)

    def feed_step(b):
        if b == 0:
            weights.finish(FG)
            weights.finish(FU)
            save(w.at[FG], w_out.at[FG], 10)
            save(w.at[FU], w_out.at[FU], 11)

        def one(i, carry):
            ag_two.chip(2 * i)
            feed(i)
            return carry

        lax.fori_loop(b, b + 1, one, 0)

    def last_step():
        save(ffn_in, ffn_in_out, 12)
        save(hidden, hidden_out, 13)
        chips(ag_cot)
        save(cot_all, cot_out, 8)
        weights.finish(FD)
        save(w.at[FD], w_out.at[FD], 14)
        over(rows_all, tile, feed_back)
        save(grads, grads_out, 15)

    steps = {
        "small": small_step,
        "ln": norm_step,
        "ns": ag_normed.start,
        "nfz": ag_normed.from_z,
        "nfy": ag_normed.from_y,
        "nfzy": ag_normed.from_zy,
        "ks": cot_start,
        "kfz": ag_cot.from_z,
        "kfy": ag_cot.from_y,
        "kfzy": ag_cot.from_zy,
        "ts": ag_two.start,
        "tfz": ag_two.from_z,
        "tfy": ag_two.from_y,
        "tfzy": ag_two.from_zy,
        "qk": qk_step,
        "v": v_step,
        "g": g_step,
        "o": o_step,
        "p3": lambda: branch.pass_on(3),
        "p1": lambda: branch.pass_on(1),
        "p2": lambda: branch.pass_on(2),
        "ln2": second_step,
        "feedA": lambda: feed_step(0),
        "feedB": lambda: feed_step(1),
        "feedC": lambda: feed_step(2),
        "feedD": lambda: feed_step(3),
        "back": last_step,
    }
    for name in FORWARD:
        if name[1:].isdigit():
            g = int(name[1])
            if name[0] == "x":
                weights.own(g)
            elif name[0] == "s":
                weights.start(g, int(name[2]) - 1)
            elif name[0] == "f":
                weights.forward(g, int(name[2]) - 1)
            else:
                steps[name]()
        else:
            steps[name]()
    for copy in outs:
        copy.wait()
    for g in range(GROUPS):
        weights.sent(g)
    ag_normed.sent()
    ag_cot.sent()
    ag_two.sent()
    branch.sent()


ROOT = math.sqrt(2.0 / math.pi)


def gelu(v):
    return 0.5 * v * (1.0 + jnp.tanh(ROOT * (v + 0.044715 * v * v * v)))


def gelu_and_slope(v):
    inside = jnp.tanh(ROOT * (v + 0.044715 * v * v * v))
    slope = 0.5 * (1.0 + inside) + 0.5 * v * (1.0 - inside * inside) * ROOT * (1.0 + 3 * 0.044715 * v * v)
    return 0.5 * v * (1.0 + inside), slope


def forward_call(n_dp, x, cot, smalls, sources):
    tokens, width = x.shape
    length = 4 * tokens
    block = width // n_dp
    rows_all = 8 * tokens
    cols = sources[2].shape[1] // 2
    small_rows = -(-(4 + 2 * (cols + length) // block) // 8) * 8
    masks = n_dp // 2 - 1
    vmem, hbm = pl.BlockSpec(memory_space=pltpu.VMEM), pl.BlockSpec(memory_space=pl.ANY)
    shape = jax.ShapeDtypeStruct
    outs = (
        shape((GROUPS, width, cols), BF),
        shape((rows_all, width), BF),
        shape((rows_all, 2 * cols), BF),
        shape((rows_all, cols), F32),
        shape((rows_all, cols), F32),
        shape((rows_all, width), BF),
        shape((rows_all, cols), BF),
        shape((rows_all, 2 * cols), BF),
        shape((rows_all, width), BF),
        shape((tokens, width), F32),
        shape((8, width), F32),
        shape((1, cols), F32),
        shape((2, length), F32),
    )
    dma = pltpu.SemaphoreType.DMA
    scratch = [
        pltpu.VMEM((small_rows, block), F32),
        pltpu.VMEM((n_dp - 1, small_rows, block), F32),
        pltpu.VMEM((2, block, 2 * cols), BF),
        pltpu.VMEM((2, 2 * cols, block), BF),
        pltpu.VMEM((8, width), F32),
        pltpu.VMEM((1, cols), F32),
        pltpu.VMEM((2, length), F32),
        pltpu.VMEM((tokens, width), BF),
        pltpu.VMEM((GROUPS, width, cols), BF),
        pltpu.VMEM((rows_all, width), BF),
        pltpu.VMEM((rows_all, width), BF),
        pltpu.VMEM((rows_all, width), BF),
        pltpu.VMEM((rows_all, 2 * cols), BF),
        pltpu.VMEM((rows_all, cols), F32),
        pltpu.VMEM((rows_all, cols), F32),
        pltpu.VMEM((rows_all, cols), BF),
        pltpu.VMEM((rows_all, cols), F32),
        pltpu.VMEM((rows_all, cols), F32),
        pltpu.VMEM((rows_all, cols), BF),
        pltpu.VMEM((rows_all, 2 * cols), BF),
        pltpu.VMEM((tokens, width), F32),
        pltpu.VMEM((4, tokens, width), F32),
        pltpu.VMEM((4, tokens, width), BF),
        pltpu.VMEM((4, tokens, width), BF),
        pltpu.VMEM((3, tokens, width), BF),
        pltpu.VMEM((3, tokens, width), BF),
        dma((GROUPS,)),
        dma((GROUPS, masks)),
        dma((GROUPS,)),
        dma((GROUPS,)),
        dma((GROUPS,)),
        dma((3, 7)),
        dma((3, 7)),
        dma((4,)),
        dma((4,)),
        dma((3,)),
        dma((3,)),
        dma((23,)),
        dma((n_dp - 1,)),
        dma((n_dp - 1,)),
    ]
    return pl.pallas_call(
        functools.partial(forward_kernel, n_dp),
        out_shape=outs,
        in_specs=[hbm, hbm] + [vmem] * 4 + [hbm] * len(sources),
        out_specs=(hbm,) * len(outs),
        scratch_shapes=scratch,
        compiler_params=pltpu.CompilerParams(
            collective_id=1, has_side_effects=True, vmem_limit_bytes=64_000_000
        ),
    )(x, cot, *smalls, *sources)


class Reduce:
    def __init__(self, place, keep, x_out, x_in, z_in, own_out, sems, own_sem):
        self.place = place
        self.keep, self.x_out, self.x_in, self.z_in, self.own_out = keep, x_out, x_in, z_in, own_out
        self.x_send, self.x_recv, self.z_send, self.z_recv = sems
        self.own_sem = own_sem
        self.block = z_in.shape[2]
        self.half = place.n_dp // 2
        z = place.z
        self.targets = [
            ((1 - z if flips else z) + above, i, place.peer(bits)) for i, (bits, above, flips) in enumerate(place.masks)
        ]
        self.targets.reverse()

    def rows(self, position):
        return pl.ds(pl.multiple_of(position * self.block, self.block), self.block)

    def x_copy(self, g, ring, position):
        return remote(
            self.x_out.at[ring, self.rows(position), :],
            self.x_in.at[g, self.rows(position), :],
            self.x_send.at[g],
            self.x_recv.at[g, position],
            self.place.x_peer(),
        )

    def z_copy(self, g, position, i, peer):
        return remote(
            self.keep.at[g, self.rows(position), :],
            self.z_in.at[g, i],
            self.z_send.at[g],
            self.z_recv.at[g, i],
            peer,
        )

    def upper(self, g, ring, left, right, col, step):
        width = left.shape[1] // 2
        cols = self.keep.shape[2]

        def body(i, carry):
            at = pl.multiple_of(i * step, step)
            value = dot_tn(left[:, pl.ds(pl.multiple_of(width + at, step), step)], right[:, col : col + cols])
            self.x_out[ring, pl.ds(at, step), :] = value.astype(BF)
            return carry

        lax.fori_loop(0, width // step, body, 0)
        for position, _, _ in self.targets:
            self.x_copy(g, ring, position).start()
        self.x_copy(g, ring, self.place.z).start()

    def lower(self, g, left, right, col, step):
        width = left.shape[1] // 2
        cols = self.keep.shape[2]

        def body(i, carry):
            at = pl.ds(pl.multiple_of(i * step, step), step)
            self.keep[g, at, :] = dot_tn(left[:, at], right[:, col : col + cols]).astype(BF)
            return carry

        lax.fori_loop(0, width // step, body, 0)

    def x_sent(self, g, ring):
        whole = self.x_out.at[ring]
        remote(whole, whole, self.x_send.at[g], self.x_recv.at[g, 0], self.place.x_peer()).wait_send()

    def add(self, g, ring, position):
        self.x_copy(g, ring, position).wait_recv()
        step = min(64, self.block)

        def body(i, carry):
            r = pl.ds(pl.multiple_of(position * self.block + i * step, step), step)
            self.keep[g, r, :] = (self.keep[g, r, :].astype(F32) + self.x_in[g, r, :].astype(F32)).astype(BF)
            return carry

        lax.fori_loop(0, self.block // step, body, 0)

    def own_copy(self, g):
        return pltpu.make_async_copy(
            self.keep.at[g, self.rows(self.place.z), :], self.own_out.at[g], self.own_sem.at[g]
        )

    def step(self, g, ring, third):
        if third == 0:
            self.add(g, ring, self.place.z)
            self.own_copy(g).start()
            return
        count = len(self.targets)
        for position, i, peer in self.targets[(3 - third) * count // 3 : (4 - third) * count // 3]:
            self.add(g, ring, position)
            self.z_copy(g, position, i, peer).start()

    def finish(self, g):
        self.own_copy(g).wait()
        for position, i, peer in self.targets:
            self.z_copy(g, position, i, peer).wait()


def norm_back(value, grad, gain):
    center = value - jnp.mean(value, axis=-1, keepdims=True)
    spread = jnp.mean(center * center, axis=-1, keepdims=True)
    r = lax.rsqrt(spread + EPSILON)
    hat = center * r
    scaled = grad * gain
    back = r * (
        scaled - jnp.mean(scaled, axis=-1, keepdims=True) - hat * jnp.mean(scaled * hat, axis=-1, keepdims=True)
    )
    return back, jnp.sum(grad * hat, axis=0, keepdims=True), jnp.sum(grad, axis=0, keepdims=True)


def backward_kernel(
    n_dp,
    x_hbm,
    params_ref,
    group_ref,
    cum_row_ref,
    w_ref,
    normed_ref,
    qkv_ref,
    gate_ref,
    mixed_ref,
    ffn_in_ref,
    hidden_ref,
    grads_ref,
    cot_ref,
    middle_ref,
    layer_out,
    input_grad_out,
    own_out,
    z_in,
    sums_out,
    w,
    tokens_a,
    ffn_in,
    branch_all,
    slim,
    qkv,
    gate_in,
    mixed,
    gated,
    x_ref,
    middle,
    grad_middle,
    sums,
    sums_in,
    group_sum,
    payload,
    payload_in,
    keep,
    c_out,
    c_in,
    far_in,
    c_in_two,
    far_in_two,
    dw_keep,
    x_out,
    x_in,
    ag_send,
    ag_recv,
    c_send,
    c_recv,
    far_send,
    far_recv,
    x_send,
    x_recv,
    z_send,
    z_recv,
    load_sem,
    own_sem,
    sum_send,
    sum_recv,
    pay_send,
    pay_recv,
):
    place = Place(n_dp)
    tokens, width = x_ref.shape
    rows_all = 8 * tokens
    length = rows_all // 2
    cols = gated.shape[1]
    head_k = cols // 2
    scale = 1.0 / math.sqrt(head_k)
    tile = 2 * tokens
    step = min(512, width // 2)
    block = z_in.shape[2]
    ag = Gather(place, branch_all, ag_send, ag_recv)

    def scatter(k, c, far):
        return Scatter(place, keep, c_out, c, None, far, (c_send.at[k], c_recv.at[k], far_send.at[k], far_recv.at[k]))

    rs_two = scatter(0, c_in, far_in)
    rs_out = scatter(1, c_in_two, far_in_two)
    rs_one = scatter(2, c_in, far_in)
    dw = Reduce(place, dw_keep, x_out, x_in, z_in, own_out, (x_send, x_recv, z_send, z_recv), own_sem)
    result = ffn_in.at[:tokens, :]
    weighted = ffn_in.at[tokens : tokens + length, :length]
    score_back = ffn_in.at[tokens : tokens + length, length : 2 * length]
    ring = {FD: 0, FG: 1, FU: 2, O: 3, G: 0, QK: 1, V: 2}

    def load(src, dst, index):
        copy = pltpu.make_async_copy(src, dst, load_sem.at[index])
        copy.start()
        return copy

    def over(count, size, body):
        def loop(i, carry):
            body(pl.ds(pl.multiple_of(i * size, size), size), i)
            return carry

        lax.fori_loop(0, count // size, loop, 0)

    in_cot = load(cot_ref, tokens_a, 3)
    in_hidden = load(hidden_ref, slim.at[:, 2 * cols :], 4)
    in_grads = load(grads_ref, slim.at[:, : 2 * cols], 0)
    in_fg = load(w_ref.at[FG], w.at[0], 1)
    in_fu = load(w_ref.at[FU], w.at[1], 2)
    in_ffn = load(ffn_in_ref, ffn_in, 5)
    in_middle = load(middle_ref, middle, 6)
    in_mixed = load(mixed_ref, mixed, 7)
    in_gate = load(gate_ref, gate_in, 8)
    in_o = load(w_ref.at[O], w.at[2], 9)
    in_qkv = load(qkv_ref, qkv, 10)
    for copy in column_copies(place, x_hbm, x_ref, load_sem.at[11], block):
        copy.start()
    sums[...] = jnp.zeros_like(sums)
    group_sum[...] = jnp.zeros_like(group_sum)
    entry_barrier(place, True)
    waited = []

    def ready(*copies):
        for copy in copies:
            if not any(copy is other for other in waited):
                waited.append(copy)
                copy.wait()

    def rows_of(i):
        return 3 - i, pl.ds(pl.multiple_of((3 - i) * tile, tile), tile)

    def two_part(i, carry):
        b, r = rows_of(i)
        rs_two.part(b, dot_nt(slim[r, :cols], w[0]) + dot_nt(slim[r, cols : 2 * cols], w[1]))
        return carry

    def gating(r, i):
        value = mixed[r, :]
        center = value - jnp.mean(value, axis=-1, keepdims=True)
        spread = jnp.mean(center * center, axis=-1, keepdims=True)
        gate = gate_in[r, :]
        flat = center * lax.rsqrt(jnp.maximum(spread, GROUP_FLOOR)) * group_ref[...]
        gated[r, :] = (flat * (gate * lax.logistic(gate))).astype(BF)

    def second_back(r, i):
        back, gain_sum, bias_sum = norm_back(middle[r, :], rs_two.own(r), params_ref[1:2, :])
        total = tokens_a[r, :].astype(F32) + back
        grad_middle[r, :] = total
        branch_all[r, :] = total.astype(BF)
        sums[1:2, :] += gain_sum
        sums[3:4, :] += bias_sum

    def out_part(i, carry):
        b, r = rows_of(i)
        rs_out.part(b, dot_nt(slim[r, 2 * cols :], w[0]))
        return carry

    def gating_back(b):
        r = pl.ds(pl.multiple_of(b * tile, tile), tile)
        back = dot_nn(branch_all[r, :], w[2])
        value = mixed[r, :]
        center = value - jnp.mean(value, axis=-1, keepdims=True)
        spread = jnp.mean(center * center, axis=-1, keepdims=True)
        inverse = lax.rsqrt(jnp.maximum(spread, GROUP_FLOOR))
        hat = center * inverse
        gate = gate_in[r, :]
        sigmoid = lax.logistic(gate)
        flat = hat * group_ref[...]
        slope = sigmoid * (1.0 + gate * (1.0 - sigmoid))
        slim[r, 2 * cols :] = (back * flat * slope).astype(BF)
        grad = back * (gate * sigmoid)
        group_sum[...] += jnp.sum(grad * hat, axis=0, keepdims=True)
        scaled = grad * group_ref[...]
        live = jnp.where(spread > GROUP_FLOOR, 1.0, jnp.where(spread == GROUP_FLOOR, 0.5, 0.0))
        moment = jnp.mean(scaled * hat, axis=-1, keepdims=True) * live
        mixed_back = inverse * (scaled - jnp.mean(scaled, axis=-1, keepdims=True) - hat * moment)
        slim[r, cols : 2 * cols] = mixed_back.astype(BF)

    def sequence_back(s):
        seq = pl.ds(pl.multiple_of(s * length, length), length)

        def body(i, carry):
            r = pl.ds(pl.multiple_of(s * length + i * tile, tile), tile)
            at = pl.ds(pl.multiple_of(i * tile, tile), tile)
            scores = dot_nt(qkv[r, :head_k], qkv[seq, head_k : 2 * head_k])
            here = cum_row_ref[pl.ds(s, 1), at]
            decays = decay_tile(
                place.t, cum_row_ref[pl.ds(s, 1), :], here, i * tile, tile, length, tokens
            )
            weighted[at, :] = (scores * decays * scale).astype(BF)
            back = dot_nt(slim[r, cols : 2 * cols], qkv[seq, 2 * head_k :])
            grad = (back * decays * scale).astype(BF)
            score_back[at, :] = grad
            slim[r, :head_k] = dot_nn(grad, qkv[seq, head_k : 2 * head_k]).astype(BF)
            return carry

        lax.fori_loop(0, length // tile, body, 0)
        slim[seq, head_k : 2 * head_k] = dot_tn(score_back[...], qkv[seq, :head_k]).astype(BF)
        slim[seq, cols : 2 * cols] = dot_tn(weighted[...], slim[seq, cols : 2 * cols]).astype(BF)


    def finish_out(r, i):
        result[r, :] = (middle[r, :] + rs_out.own(r)).astype(BF)

    def one_part(i, carry):
        b, r = rows_of(i)
        total = dot_nt(slim[r, :cols], w[1]) + dot_nt(slim[r, cols : 2 * cols], w[0])
        rs_one.part(b, total + dot_nt(slim[r, 2 * cols :], w[2]))
        return carry

    def first_back(r, i):
        back, gain_sum, bias_sum = norm_back(x_ref[r, :].astype(F32), rs_one.own(r), params_ref[0:1, :])
        result[r, :] = (grad_middle[r, :] + back).astype(BF)
        sums[0:1, :] += gain_sum
        sums[2:3, :] += bias_sum

    def sum_copy(k):
        peer = (place.c_peer(), place.y_peer())[k]
        return remote(sums, sums_in.at[k], sum_send.at[k], sum_recv.at[k], peer)

    pay = []
    for j, (bits, above, flips) in enumerate(place.pairs):
        position = (1 - place.z if flips else place.z) + above
        pay.append(remote(payload.at[position], payload_in.at[j], pay_send.at[j], pay_recv.at[j], place.peer(bits)))

    later = {}
    operands = {
        FD: (tokens_a, 2 * cols),
        FG: (ffn_in, 0),
        FU: (ffn_in, cols),
        O: (branch_all, None),
        QK: (tokens_a, 0),
        V: (tokens_a, cols),
        G: (tokens_a, 2 * cols),
    }

    def operands_of(g):
        ready(*{FD: (in_cot, in_hidden), FG: (in_ffn, in_grads), FU: (in_ffn, in_grads), O: ()}.get(g, (later.get(3),)))
        left, col = operands[g]
        return (left, gated, 0, step) if col is None else (left, slim, col, step)

    def two_step():
        ready(in_grads, in_fg, in_fu)
        lax.fori_loop(0, 4, two_part, 0)
        later[FD] = load(w_ref.at[FD], w.at[0], 1)
        later[QK] = load(w_ref.at[QK], w.at[1], 2)

    def gating_step():
        ready(in_mixed, in_gate)
        over(rows_all, tokens, gating)

    def second_step():
        ready(in_middle)
        rs_two.wait_own()
        over(tokens, 16, second_back)
        later[3] = load(normed_ref, tokens_a, 3)

    def out_step():
        rs_two.sent()
        ready(later[FD])
        lax.fori_loop(0, 4, out_part, 0)
        later[V] = load(w_ref.at[V], w.at[0], 1)

    def chip_step(first):
        ready(in_o, in_qkv)

        def chip(b, carry):
            ag.chip(2 * b)
            gating_back(b)
            return carry

        lax.fori_loop(first, first + 2, chip, 0)
        if first:
            later[G] = load(w_ref.at[G], w.at[2], 9)

    def sequence_step(s):
        lax.fori_loop(s, s + 1, lambda i, carry: (sequence_back(i), carry)[1], 0)

    def out_finish():
        rs_out.wait_own()
        over(tokens, 16, finish_out)
        later["layer"] = load(result, layer_out, 4)

    def one_step():
        rs_out.sent()
        ready(later[QK], later[V], later[G])
        lax.fori_loop(0, 4, one_part, 0)

    def first_step():
        pltpu.make_async_copy(x_hbm, x_ref, load_sem.at[11]).wait()
        ready(later["layer"])
        rs_one.wait_own()
        over(tokens, 16, first_back)
        later["grad"] = load(result, input_grad_out, 4)

    def sum_cores():
        sum_copy(0).start()

    def sum_chips():
        sum_copy(0).wait()
        sums[...] += sums_in[0]
        sum_copy(1).start()

    def pay_start():
        sum_copy(1).wait()
        sums[...] += sums_in[1]
        for p in range(n_dp):
            payload[p, 0:4, :] = sums[0:4, p * block : (p + 1) * block]
            for k in range(cols // block):
                payload[p, 4 + k : 5 + k, :] = group_sum[0:1, k * block : (k + 1) * block]
        for copy in pay:
            copy.start()

    def pay_finish():
        for copy in pay:
            copy.wait()
        mine = payload[place.z]
        other = jnp.zeros_like(mine)
        for j, (bits, above, flips) in enumerate(place.pairs):
            if flips:
                other = other + payload_in[j]
            else:
                mine = mine + payload_in[j]
        sums_out[0] = mine
        sums_out[1] = other

    before = {G: FD, QK: FG, V: FU}

    def upper(g):
        if g in before:
            dw.x_sent(before[g], ring[before[g]])
        dw.upper(g, ring[g], *operands_of(g))

    steps = {
        "two": two_step,
        "a3": lambda: rs_two.pass_on(3),
        "a1": lambda: rs_two.pass_on(1),
        "a2": lambda: rs_two.pass_on(2),
        "gat": gating_step,
        "lnb": second_step,
        "bs": ag.start,
        "bfz": ag.from_z,
        "bfy": ag.from_y,
        "bfzy": ag.from_zy,
        "out": out_step,
        "o3": lambda: rs_out.pass_on(3),
        "o1": lambda: rs_out.pass_on(1),
        "o2": lambda: rs_out.pass_on(2),
        "gbA": lambda: chip_step(0),
        "gbB": lambda: chip_step(2),
        "seq0": lambda: sequence_step(0),
        "seq1": lambda: sequence_step(1),
        "outf": out_finish,
        "one": one_step,
        "b3": lambda: rs_one.pass_on(3),
        "b1": lambda: rs_one.pass_on(1),
        "b2": lambda: rs_one.pass_on(2),
        "lna": first_step,
        "sc": sum_cores,
        "sy": sum_chips,
        "pay": pay_start,
        "payw": pay_finish,
    }
    for name in BACKWARD:
        if name in steps:
            steps[name]()
        elif name[0] == "u":
            upper(int(name[1]))
        elif name[0] == "l":
            dw.lower(int(name[1]), *operands_of(int(name[1])))
        else:
            dw.step(int(name[1]), ring[int(name[1])], int(name[2]))
    ready(later["grad"])
    for g in (O, G, QK, V):
        dw.x_sent(g, ring[g])
    ag.sent()
    rs_one.sent()
    for g in (FD, FG, FU, O, G, QK, V):
        dw.finish(g)


def backward_call(n_dp, x, params, group, cum_row, saved):
    tokens, width = x.shape
    rows_all = 8 * tokens
    w = saved[0]
    cols = w.shape[2]
    block = width // n_dp
    masks = n_dp // 2 - 1
    vmem, hbm = pl.BlockSpec(memory_space=pltpu.VMEM), pl.BlockSpec(memory_space=pl.ANY)
    shape = jax.ShapeDtypeStruct
    pay_rows = -(-(4 + cols // block) // 8) * 8
    outs = (
        shape((tokens, width), BF),
        shape((tokens, width), BF),
        shape((GROUPS, block, cols), BF),
        shape((GROUPS, masks, block, cols), BF),
        shape((2, pay_rows, block), F32),
    )
    dma = pltpu.SemaphoreType.DMA
    scratch = [
        pltpu.VMEM((3, width, cols), BF),
        pltpu.VMEM((rows_all, width), BF),
        pltpu.VMEM((rows_all, width), BF),
        pltpu.VMEM((rows_all, width), BF),
        pltpu.VMEM((rows_all, 3 * cols), BF),
        pltpu.VMEM((rows_all, 2 * cols), BF),
        pltpu.VMEM((rows_all, cols), F32),
        pltpu.VMEM((rows_all, cols), F32),
        pltpu.VMEM((rows_all, cols), BF),
        pltpu.VMEM((tokens, width), BF),
        pltpu.VMEM((tokens, width), F32),
        pltpu.VMEM((tokens, width), F32),
        pltpu.VMEM((8, width), F32),
        pltpu.VMEM((2, 8, width), F32),
        pltpu.VMEM((1, cols), F32),
        pltpu.VMEM((n_dp, pay_rows, block), F32),
        pltpu.VMEM((n_dp - 1, pay_rows, block), F32),
        pltpu.VMEM((4, tokens, width), BF),
        pltpu.VMEM((4, tokens, width), BF),
        pltpu.VMEM((4, tokens, width), BF),
        pltpu.VMEM((3, tokens, width), BF),
        pltpu.VMEM((4, tokens, width), BF),
        pltpu.VMEM((3, tokens, width), BF),
        pltpu.VMEM((GROUPS, width // 2, cols), BF),
        pltpu.VMEM((4, width // 2, cols), BF),
        pltpu.VMEM((GROUPS, width // 2, cols), BF),
        dma((7,)),
        dma((7,)),
        dma((3, 4)),
        dma((3, 4)),
        dma((3, 3)),
        dma((3, 3)),
        dma((GROUPS,)),
        dma((GROUPS, n_dp // 2)),
        dma((GROUPS,)),
        dma((GROUPS, masks)),
        dma((12,)),
        dma((GROUPS,)),
        dma((2,)),
        dma((2,)),
        dma((n_dp - 1,)),
        dma((n_dp - 1,)),
    ]
    return pl.pallas_call(
        functools.partial(backward_kernel, n_dp),
        out_shape=outs,
        in_specs=[hbm, vmem, vmem, vmem] + [hbm] * len(saved),
        out_specs=(hbm,) * 4 + (vmem,),
        scratch_shapes=scratch,
        compiler_params=pltpu.CompilerParams(
            collective_id=2, has_side_effects=True, vmem_limit_bytes=67_000_000
        ),
    )(x, params, group, cum_row, *saved)


def finish_kernel(
    n_dp,
    own_ref,
    others_ref,
    layer_ref,
    grad_ref,
    sums_ref,
    layer_out,
    input_grad,
    query_grad,
    key_grad,
    value_grad,
    gate_grad,
    out_grad,
    group_grad,
    gain_grad,
    bias_grad,
    ffn_gate_grad,
    ffn_up_grad,
    ffn_down_grad,
    own,
    others,
    rows,
    wide,
    tall,
    in_sem,
    out_sem,
    row_sem,
):
    place = Place(n_dp)
    z = place.z
    block, cols = own.shape[1:]
    loads = []
    for g in (FD, FG, FU, O, QK, V, G):
        pair = (
            pltpu.make_async_copy(own_ref.at[g], own.at[g], in_sem.at[0, g]),
            pltpu.make_async_copy(others_ref.at[g], others.at[g], in_sem.at[1, g]),
        )
        for copy in pair:
            copy.start()
        loads.append((g, pair))
    row_loads = [
        pltpu.make_async_copy(layer_ref, rows.at[0], row_sem.at[0]),
        pltpu.make_async_copy(grad_ref, rows.at[1], row_sem.at[1]),
    ]
    for copy in row_loads:
        copy.start()
    outs = []

    def save(src, dst, index):
        copy = pltpu.make_async_copy(src, dst, out_sem.at[index])
        copy.start()
        outs.append(copy)

    wide_at = {FG: 0, FU: 1, V: 2, G: 3, QK: 4}
    tall_at = {FD: 0, O: 1}
    targets = {FG: ffn_gate_grad, FU: ffn_up_grad, V: value_grad, G: gate_grad, FD: ffn_down_grad, O: out_grad}
    for g, pair in loads:
        for copy in pair:
            copy.wait()
        mine = own[g].astype(F32)
        theirs = None
        for i, (bits, above, flips) in enumerate(place.masks):
            value = others[g, i].astype(F32)
            if not flips:
                mine = mine + value
            else:
                theirs = value if theirs is None else theirs + value
        if g in tall_at:
            k = tall_at[g]
            tall[k, pl.ds(pl.multiple_of(z * cols, cols), cols), :] = mine.T
            tall[k, pl.ds(pl.multiple_of((1 - z) * cols, cols), cols), :] = theirs.T
            save(tall.at[k], targets[g], k)
            continue
        k = wide_at[g]
        if g == QK:
            half = cols // 2
            for which, dst in ((0, query_grad), (1, key_grad)):
                part = slice(which * half, (which + 1) * half)
                at = which * cols
                wide[k, :, pl.ds(pl.multiple_of(at + z * half, half), half)] = mine[:, part]
                wide[k, :, pl.ds(pl.multiple_of(at + (1 - z) * half, half), half)] = theirs[:, part]
                save(wide.at[k, :, pl.ds(at, cols)], dst, 2 + which)
            continue
        wide[k, :, pl.ds(pl.multiple_of(z * cols, cols), cols)] = mine
        wide[k, :, pl.ds(pl.multiple_of((1 - z) * cols, cols), cols)] = theirs
        save(wide.at[k], targets[g], 4 + k)
    for k, dst in ((0, layer_out), (1, input_grad)):
        row_loads[k].wait()
        for copy in column_copies(place, rows.at[k], dst, row_sem.at[k], block, True):
            copy.start()
    norm = sums_ref[0, 0:4, :] + sums_ref[1, 0:4, :]
    piece = gain_grad.shape[1]
    mine = norm[:, :piece]
    for k in range(1, block // piece):
        mine = jnp.where(place.t == k, norm[:, k * piece : (k + 1) * piece], mine)
    gain_grad[...] = mine[0:2, :]
    bias_grad[...] = mine[2:4, :]
    piece = group_grad.shape[1]
    here = place.d % (block // piece)
    row = place.d // (block // piece)

    def group_of(which):
        value = sums_ref[which, 4:5, :]
        for k in range(1, cols // block):
            value = jnp.where(row == k, sums_ref[which, 4 + k : 5 + k, :], value)
        out = value[:, :piece]
        for k in range(1, block // piece):
            out = jnp.where(here == k, value[:, k * piece : (k + 1) * piece], out)
        return out

    same, other = group_of(0), group_of(1)
    group_grad[0:1, :] = jnp.where(z == 0, same, other)
    group_grad[1:2, :] = jnp.where(z == 0, other, same)
    for copy in outs:
        copy.wait()
    for k, dst in ((0, layer_out), (1, input_grad)):
        pltpu.make_async_copy(rows.at[k], dst, row_sem.at[k]).wait()


def finish_call(n_dp, n_tensor, own, others, layer, grad, sums):
    tokens, width = layer.shape
    block, cols = own.shape[1:]
    masks = others.shape[1]
    vmem, hbm = pl.BlockSpec(memory_space=pltpu.VMEM), pl.BlockSpec(memory_space=pl.ANY)
    shape = jax.ShapeDtypeStruct
    rows, wide, tall = shape((tokens, width), BF), shape((block, 2 * cols), F32), shape((2 * cols, block), F32)
    thin, norm = shape((block, cols), F32), shape((2, width // (n_dp * n_tensor)), F32)
    outs = (rows, rows, thin, thin, wide, wide, tall, shape((2, cols // n_dp), F32), norm, norm, wide, wide, tall)
    specs = [vmem if o.shape[0] == 2 else hbm for o in outs]
    dma = pltpu.SemaphoreType.DMA
    return pl.pallas_call(
        functools.partial(finish_kernel, n_dp),
        out_shape=outs,
        in_specs=[hbm, hbm, hbm, hbm, vmem],
        out_specs=tuple(specs),
        scratch_shapes=[
            pltpu.VMEM((GROUPS, block, cols), BF),
            pltpu.VMEM((GROUPS, masks, block, cols), BF),
            pltpu.VMEM((2, tokens, width), BF),
            pltpu.VMEM((5, block, 2 * cols), F32),
            pltpu.VMEM((2, 2 * cols, block), F32),
            dma((2, GROUPS)),
            dma((8,)),
            dma((2,)),
        ],
        compiler_params=pltpu.CompilerParams(vmem_limit_bytes=67_000_000),
    )(own, others, layer, grad, sums)


def per_device(
    n_dp,
    n_tensor,
    inputs,
    cotangent,
    log_decay,
    query_weight,
    key_weight,
    value_weight,
    gate_weight,
    out_weight,
    group_gain,
    norm_gains,
    norm_biases,
    ffn_gate_weight,
    ffn_up_weight,
    ffn_down_weight,
):
    place = Place(n_dp)
    d, t = place.d, place.t
    tokens, width = inputs.shape
    block = width // n_dp

    def position_of(q):
        out = (q // PAIR) & 1
        for k, bit in enumerate(place.rest):
            out = out + ((d // bit) % 2 ^ ((q // bit) & 1)) * (2 << k)
        return out

    def moved(value, index):
        if block % 128 == 0:
            return value
        return jnp.concatenate(
            [lax.dynamic_slice_in_dim(value, index(p) * block, block, 1) for p in range(n_dp)], axis=1
        )

    smalls = (norm_gains, norm_biases, group_gain, log_decay)
    sources = (
        query_weight,
        key_weight,
        value_weight,
        gate_weight,
        out_weight,
        ffn_gate_weight,
        ffn_up_weight,
        ffn_down_weight,
    )
    x, cot = moved(inputs, place.dp_of), moved(cotangent, place.dp_of)
    *saved, params, group, cumul = forward_call(n_dp, x, cot, smalls, sources)
    layer, grad, own, others, sums = backward_call(n_dp, x, params, group, cumul, saved)
    outs = finish_call(n_dp, n_tensor, own, others, layer, grad, sums)
    return (moved(outs[0], position_of), moved(outs[1], position_of), *outs[2:])


def solution(mesh):
    tokens = P(("dp", "tensor"), None)
    rows, cols, norms = P("dp", "tensor"), P("tensor", "dp"), P(None, "dp")
    sums = P(None, ("dp", "tensor"))
    in_specs = (tokens, tokens, cols, rows, rows, rows, rows, cols, cols, norms, norms, rows, rows, cols)
    out_specs = (tokens, tokens, rows, rows, rows, rows, cols, cols, sums, sums, rows, rows, cols)
    body = functools.partial(per_device, mesh.shape["dp"], mesh.shape["tensor"])
    return jax.shard_map(body, mesh=mesh, in_specs=in_specs, out_specs=out_specs, check_vma=False)
```

```python
import functools
import math

import jax
import jax.numpy as jnp
from jax import lax
from jax.experimental import pallas as pl
from jax.experimental.pallas import tpu as pltpu
from jax.sharding import PartitionSpec as P

EPSILON = 1e-05
GROUP_FLOOR = 1.0
BF = jnp.bfloat16
F32 = jnp.float32
PAIR = 2
MESH = pl.DeviceIdType.MESH
QK, V, G, O, FG, FU, FD = range(7)
GROUPS = 7


FORWARD = (
    "s22", "s11", "x1", "small", "s32", "ks", "x4", "x3", "x2", "kfy", "ln", "s02", "ns", "s03", "s01", "s31",
    "f22", "nfy", "f11", "s13", "f32", "f02", "s33", "s23", "x0", "x6", "f01", "f31", "nfz", "nfzy", "s12", "f03",
    "s21", "f13", "f23", "kfz", "qk", "s51", "s42", "f12", "s52", "f21", "s41", "f33", "s61", "s63", "v", "g", "o",
    "p3", "f42", "f41", "f61", "p2", "x5", "kfzy", "f63", "s53", "p1", "p2B", "f51", "s43", "ln2", "f52", "ts",
    "tfy", "f53", "s62", "f43", "tfz", "tfzB", "f62", "feedA", "feedB", "feedC", "tfzy", "feedD", "back",
)
BACKWARD = (
    "u6", "two", "a3", "a1", "l6", "s63", "l4", "a2", "s62", "u4", "u5", "s43", "lnb", "bs", "bfz", "s42", "s41",
    "l5", "out", "o3", "s52", "bfy", "s51", "gat", "s40", "gbA", "bfzy", "gbB", "u3", "l2", "u2", "seq0", "s53",
    "o2", "seq1", "u0", "u1", "l0", "l3", "o1", "s33", "outf", "s32", "s31", "one", "s61", "s23", "s30", "b3",
    "l1", "b2", "s22", "s02", "b1", "s01", "s21", "s03", "s13", "lna", "s10", "s00", "s20", "sc", "sy", "pay",
    "s50", "s12", "s60", "s11", "payw",
)


def dot_nn(a, b):
    return lax.dot_general(a, b, (((1,), (0,)), ((), ())), preferred_element_type=F32)


def dot_nt(a, b):
    return lax.dot_general(a, b, (((1,), (1,)), ((), ())), preferred_element_type=F32)


def dot_tn(a, b):
    return lax.dot_general(a, b, (((0,), (0,)), ((), ())), preferred_element_type=F32)


def flip(index, bit):
    return index + bit - 2 * bit * ((index // bit) % 2)


class Place:
    def __init__(self, n_dp):
        self.n_dp = n_dp
        self.d = lax.axis_index("dp")
        self.t = lax.axis_index("tensor")
        self.z = (self.d // PAIR) % 2
        self.rest = [1 << i for i in range(2, n_dp.bit_length() - 1)] + [1]
        self.inner = self.rest[:-1]
        self.masks = []
        for pick in range(1, 1 << (1 + len(self.inner))):
            bits = [PAIR] * (pick & 1) + [b for k, b in enumerate(self.inner) if (pick >> (k + 1)) & 1]
            self.masks.append((bits, pick & ~1, pick & 1))
        half = n_dp // 2
        self.pairs = self.masks + [([1], half, 0)] + [(bits + [1], above + half, flips) for bits, above, flips in self.masks]

    def slot(self, above, flips):
        return next((j for j, pair in enumerate(self.pairs) if pair[1:] == (above, flips)), None)

    def dp_of(self, p):
        out = (p & 1) * PAIR
        for k, bit in enumerate(self.rest):
            here = (self.d // bit) % 2
            out = out + (1 - here if (p >> (k + 1)) & 1 else here) * bit
        return out

    def peer(self, bits):
        out = self.d
        for bit in bits:
            out = flip(out, bit)
        return {"dp": out}

    def x_peer(self):
        return {"dp": flip(self.d, 1)}

    def z_peer(self):
        return {"dp": flip(self.d, PAIR)}

    def y_peer(self):
        return {"tensor": flip(self.t, 2)}

    def c_peer(self):
        return {"tensor": flip(self.t, 1)}

    def everyone(self, far):
        near = [self.x_peer(), self.y_peer(), self.c_peer()]
        if far:
            return near[1:] + [self.peer(bits) for bits, _, _ in self.pairs]
        return near + [self.peer(bits) for bits, _, _ in self.masks]


def greet(place, far):
    barrier = pltpu.get_barrier_semaphore()
    for peer in place.everyone(far):
        pl.semaphore_signal(barrier, inc=1, device_id=peer, device_id_type=MESH)


def met(place, far):
    pl.semaphore_wait(pltpu.get_barrier_semaphore(), len(place.everyone(far)))


def entry_barrier(place, far=False):
    greet(place, far)
    met(place, far)


def column_copies(place, src, dst, sem, block, back=False):
    if block % 128:
        return [pltpu.make_async_copy(src, dst, sem)]
    out = []
    for p in range(place.n_dp):
        natural = pl.ds(pl.multiple_of(place.dp_of(p) * block, block), block)
        here = pl.ds(p * block, block)
        a, b = (here, natural) if back else (natural, here)
        out.append(pltpu.make_async_copy(src.at[:, a], dst.at[:, b], sem))
    return out


def remote(src, dst, send, recv, peer):
    return pltpu.make_async_remote_copy(
        src_ref=src, dst_ref=dst, send_sem=send, recv_sem=recv, device_id=peer, device_id_type=MESH
    )


class Weights:
    def __init__(self, place, sources, full, sems):
        self.place, self.sources, self.full = place, sources, full
        self.z_send, self.z_recv, self.x_send, self.x_recv, self.local = sems
        self.block = sources[-1].shape[0]
        self.cols = sources[-1].shape[1] // 2
        self.half = place.n_dp // 2

    def rows(self, position, count=1):
        return pl.ds(pl.multiple_of(position * self.block, self.block), count * self.block)

    def pairs(self, g, half, position):
        parts = self.sources[g] if isinstance(self.sources[g], tuple) else (self.sources[g],)
        count = self.cols // len(parts)
        for k, part in enumerate(parts):
            columns = pl.ds(pl.multiple_of(half * count, count), count)
            yield part.at[:, columns], self.full.at[g, self.rows(position), k * count : (k + 1) * count]

    def own(self, g):
        z = self.place.z
        for src, dst in self.pairs(g, z, z):
            pltpu.make_async_copy(src, dst, self.local.at[g]).start()
        for src, dst in self.pairs(g, z, z + self.half):
            remote(src, dst, self.x_send.at[g], self.x_recv.at[g], self.place.x_peer()).start()

    def some(self, third):
        count = len(self.place.masks)
        return reversed(range(third * count // 3, (third + 1) * count // 3))

    def start(self, g, third):
        z = self.place.z
        for i in self.some(third):
            bits, above, flips = self.place.masks[i]
            for src, dst in self.pairs(g, 1 - z if flips else z, z + above):
                remote(src, dst, self.z_send.at[g], self.z_recv.at[g, i], self.place.peer(bits)).start()

    def forward(self, g, third):
        for i in self.some(third):
            bits, above, flips = self.place.masks[i]
            position = (1 - self.place.z if flips else self.place.z) + above
            here = self.full.at[g, self.rows(position), :]
            remote(here, here, self.z_send.at[g], self.z_recv.at[g, i], self.place.peer(bits)).wait_recv()
            remote(
                here,
                self.full.at[g, self.rows(position + self.half), :],
                self.x_send.at[g],
                self.x_recv.at[g],
                self.place.x_peer(),
            ).start()

    def finish(self, g):
        z = self.place.z
        here = self.full.at[g, self.rows(z), :]
        pltpu.make_async_copy(here, here, self.local.at[g]).wait()
        there = self.full.at[g, self.rows(self.half, self.half), :]
        remote(there, there, self.x_send.at[g], self.x_recv.at[g], self.place.x_peer()).wait_recv()

    def sent(self, g):
        there = self.full.at[g, self.rows(self.half, self.half), :]
        remote(there, there, self.x_send.at[g], self.x_recv.at[g], self.place.x_peer()).wait_send()
        count = self.half - 1
        those = self.full.at[g, self.rows(0, count), :]
        remote(those, those, self.z_send.at[g], self.z_recv.at[g, 0], self.place.x_peer()).wait_send()


class Gather:
    def __init__(self, place, buffer, send, recv):
        self.place, self.buffer = place, buffer
        self.send, self.recv = send, recv
        self.tokens = buffer.shape[0] // 8
        self.peers = {1: place.c_peer(), 2: place.y_peer(), 4: place.z_peer()}

    def slot(self, s):
        return self.buffer.at[pl.ds(pl.multiple_of(s * self.tokens, self.tokens), self.tokens), :]

    def copy(self, source, bit, src=None):
        s = source + bit
        return remote(self.slot(source) if src is None else src, self.slot(s), self.send.at[s - 1], self.recv.at[s - 1], self.peers[bit])

    def start(self, src=None):
        for bit in (4, 2, 1):
            self.copy(0, bit, src).start()

    def from_z(self):
        self.copy(0, 4).wait_recv()
        self.copy(4, 2).start()
        self.copy(4, 1).start()

    def from_y(self):
        self.copy(0, 2).wait_recv()
        self.copy(2, 1).start()

    def from_zy(self):
        self.copy(4, 2).wait_recv()
        self.copy(6, 1).start()

    def chip(self, source):
        self.copy(source, 1).wait_recv()

    def sent(self, src=None):
        self.copy(0, 4, src).wait_send()
        self.copy(0, 2, src).wait_send()
        self.copy(0, 1, src).wait_send()
        self.copy(4, 2).wait_send()
        self.copy(4, 1).wait_send()
        self.copy(2, 1).wait_send()
        self.copy(6, 1).wait_send()


class HalfGather(Gather):
    def part(self, source, bit, h):
        count = self.tokens // 2
        s = source + bit
        index = s - 1 if h == 0 else 5 + s // 2
        src = self.buffer.at[pl.ds(source * self.tokens + h * count, count), :]
        dst = self.buffer.at[pl.ds(s * self.tokens + h * count, count), :]
        return remote(src, dst, self.send.at[index], self.recv.at[index], self.peers[bit])

    def start(self):
        for h in range(2):
            self.part(0, 4, h).start()
        self.copy(0, 2).start()
        self.copy(0, 1).start()

    def from_z(self):
        self.part(0, 4, 0).wait_recv()
        self.part(4, 2, 0).start()

    def from_z_rest(self):
        self.part(0, 4, 1).wait_recv()
        self.part(4, 2, 1).start()
        self.copy(4, 1).start()

    def from_zy(self):
        for h in range(2):
            self.part(4, 2, h).wait_recv()
        self.copy(6, 1).start()

    def sent(self):
        for h in range(2):
            self.part(0, 4, h).wait_send()
            self.part(4, 2, h).wait_send()
        for source, bit in ((0, 2), (0, 1), (4, 1), (2, 1), (6, 1)):
            self.copy(source, bit).wait_send()


class Scatter:
    def __init__(self, place, keep, c_out, c_in, far_out, far_in, sems):
        self.place = place
        self.keep, self.c_out, self.c_in, self.far_out, self.far_in = keep, c_out, c_in, far_out, far_in
        self.c_send, self.c_recv, self.far_send, self.far_recv = sems
        self.tokens = c_out.shape[1]

    def part(self, b, value):
        self.keep[b] = value[: self.tokens].astype(self.keep.dtype)
        self.c_out[b] = value[self.tokens :].astype(BF)
        self.c_copy(b).start()

    def c_copy(self, b):
        return remote(self.c_out.at[b], self.c_in.at[b], self.c_send.at[b], self.c_recv.at[b], self.place.c_peer())

    def far_copy(self, b):
        peer = self.place.z_peer() if b == 2 else self.place.y_peer()
        return remote(
            self.far_source(b), self.far_in.at[b - 1], self.far_send.at[b - 1], self.far_recv.at[b - 1], peer
        )

    def far_source(self, b):
        return self.keep.at[b] if self.far_out is None else self.far_out.at[b - 1]

    def rows(self, body, step=16):
        def loop(i, carry):
            body(pl.ds(pl.multiple_of(i * step, step), step))
            return carry

        lax.fori_loop(0, self.tokens // step, loop, 0)

    def pass_on(self, b):
        self.c_copy(b).wait_recv()
        if b == 2:
            self.far_copy(3).wait_recv()

        def body(r):
            total = self.keep[b, r, :].astype(F32) + self.c_in[b, r, :].astype(F32)
            if b == 2:
                total = total + self.far_in[2, r, :].astype(F32)
            self.far_source(b)[r, :] = total.astype(BF)

        self.rows(body)
        self.far_copy(b).start()

    def wait_own(self):
        self.c_copy(0).wait_recv()
        self.far_copy(1).wait_recv()
        self.far_copy(2).wait_recv()

    def own(self, r):
        return (
            self.keep[0, r, :].astype(F32)
            + self.c_in[0, r, :].astype(F32)
            + self.far_in[0, r, :].astype(F32)
            + self.far_in[1, r, :].astype(F32)
        )

    def sent(self):
        for b in range(4):
            self.c_copy(b).wait_send()
        for b in (3, 2, 1):
            self.far_copy(b).wait_send()


class HalfScatter(Scatter):
    def half_copy(self, b, h):
        peer = self.place.z_peer() if b == 2 else self.place.y_peer()
        count = self.tokens // 2
        rows = pl.ds(h * count, count)
        index = b - 1 if h == 0 else b + 1
        return remote(
            self.far_source(b).at[rows, :],
            self.far_in.at[b - 1, rows, :],
            self.far_send.at[index],
            self.far_recv.at[index],
            peer,
        )

    def pass_on(self, b, h=0):
        if b == 1:
            super().pass_on(1)
            return
        if h == 0:
            self.c_copy(b).wait_recv()
        if b == 2:
            self.half_copy(3, h).wait_recv()
        step = 16
        count = self.tokens // 2

        def body(i, carry):
            r = pl.ds(pl.multiple_of(h * count + i * step, step), step)
            total = self.keep[b, r, :].astype(F32) + self.c_in[b, r, :].astype(F32)
            if b == 2:
                total = total + self.far_in[2, r, :].astype(F32)
            self.far_source(b)[r, :] = total.astype(BF)
            return carry

        lax.fori_loop(0, count // step, body, 0)
        self.half_copy(b, h).start()
        if b == 3 and h == 0:
            self.pass_on(3, 1)

    def wait_own(self):
        self.c_copy(0).wait_recv()
        self.far_copy(1).wait_recv()
        for h in range(2):
            self.half_copy(2, h).wait_recv()

    def sent(self):
        for b in range(4):
            self.c_copy(b).wait_send()
        self.far_copy(1).wait_send()
        for h in range(2):
            self.half_copy(3, h).wait_send()
            self.half_copy(2, h).wait_send()


def normalized(value):
    center = value - jnp.mean(value, axis=-1, keepdims=True)
    spread = jnp.mean(center * center, axis=-1, keepdims=True)
    return center * lax.rsqrt(spread + EPSILON)


def decay_tile(t, cumul_rows, cumul_here, first, rows, length, tokens):
    square = (rows, rows)
    same = lax.broadcasted_iota(jnp.int32, square, 0) == lax.broadcasted_iota(jnp.int32, square, 1)
    cumul_cols = jnp.sum(jnp.where(same, cumul_here, 0.0), axis=1, keepdims=True)
    index = lax.broadcasted_iota(jnp.int32, (rows, length), 0) + first
    other = lax.broadcasted_iota(jnp.int32, (rows, length), 1)
    at = ((index // tokens) ^ t) * tokens + index % tokens
    to = ((other // tokens) ^ t) * tokens + other % tokens
    causal = at >= to
    return jnp.where(causal, jnp.exp(jnp.where(causal, cumul_cols - cumul_rows, 0.0)), 0.0)


def pack_small(place, small, gains, biases, group, decay, tokens):
    block = small.shape[1]
    wide = place.n_dp * group.shape[1]
    length = decay.shape[1]
    small[...] = jnp.zeros_like(small)
    small[0:2, :] = gains[...].astype(F32)
    small[2:4, :] = biases[...].astype(F32)
    lane = lax.broadcasted_iota(jnp.int32, (2, wide), 1)
    tiled = jnp.concatenate([group[...].astype(F32)] * place.n_dp, axis=1)
    spread = jnp.where(lane // group.shape[1] == place.d, tiled, 0.0)
    at = 4
    for h in range(2):
        for k in range(wide // block):
            small[at : at + 1, :] = spread[h : h + 1, k * block : (k + 1) * block]
            at += 1
    total = decay[...]
    lane = lax.broadcasted_iota(jnp.int32, total.shape, 1)
    shift = 1
    while shift < length:
        total = total + jnp.where(lane >= shift, pltpu.roll(total, shift, 1), 0.0)
        shift *= 2
    for bit in (1, 2):
        pieces = [total[:, (j ^ bit) * tokens : ((j ^ bit) + 1) * tokens] for j in range(length // tokens)]
        total = jnp.where((place.t // bit) % 2 == 1, jnp.concatenate(pieces, axis=1), total)
    for h in range(2):
        for k in range(length // block):
            small[at : at + 1, :] = total[h : h + 1, k * block : (k + 1) * block]
            at += 1


def spread_small(place, own, others, params, group, cumul, block):
    pieces = group.shape[1] // block
    steps = cumul.shape[1] // block
    first = place.z == 0

    def of(above, flips, rows):
        j = place.slot(above, flips)
        return own[rows, :] if j is None else others[j, rows, :]

    head = slice(0, 4)
    for p in range(place.n_dp):
        same, flipped = of(p & ~1, 0, head), of(p & ~1, 1, head)
        params[head, p * block : (p + 1) * block] = jnp.where(place.z == p % 2, same, flipped)

    def head_rows(above, flips, at, count):
        one = of(above, flips, slice(at, at + count))
        two = of(above, flips, slice(at + count, at + 2 * count))
        return jnp.where(first, one, two)

    total = head_rows(0, 0, 4, pieces)
    for bits, above, flips in place.pairs:
        total = total + head_rows(above, flips, 4, pieces)
    for k in range(pieces):
        group[0:1, k * block : (k + 1) * block] = total[k : k + 1, :]
    at = 4 + 2 * pieces
    for row, flips in ((0, 0), (1, 1)):
        value = head_rows(0, flips, at, steps)
        for k in range(steps):
            cumul[row : row + 1, k * block : (k + 1) * block] = value[k : k + 1, :]


def forward_kernel(
    n_dp,
    x_hbm,
    cot_hbm,
    gains_ref,
    biases_ref,
    group_gain_ref,
    decay_ref,
    s_q,
    s_k,
    s_v,
    s_g,
    s_o,
    s_fg,
    s_fu,
    s_fd,
    w_out,
    normed_out,
    qkv_out,
    gate_out,
    mixed_out,
    ffn_in_out,
    hidden_out,
    grads_out,
    cot_out,
    middle_out,
    params_out,
    group_out,
    cumul_out,
    small_ref,
    small_in,
    turned,
    natural,
    params_ref,
    group_ref,
    cum_row_ref,
    x_ref,
    w,
    normed_all,
    cot_all,
    ffn_in,
    qkv,
    gate_in,
    mixed,
    gated,
    gate_hidden,
    up_hidden,
    hidden,
    grads,
    middle,
    keep,
    c_out,
    c_in,
    far_out,
    far_in,
    z_send,
    z_recv,
    x_send,
    x_recv,
    w_local,
    ag_send,
    ag_recv,
    c_send,
    c_recv,
    far_send,
    far_recv,
    out_sem,
    small_send,
    small_recv,
):
    place = Place(n_dp)
    tokens, width = x_ref.shape
    block = width // n_dp
    rows_all = 8 * tokens
    length = rows_all // 2
    head_k = qkv.shape[1] // 4
    scale = 1.0 / math.sqrt(head_k)
    tile = 2 * tokens
    weights = Weights(place, [(s_q, s_k), s_v, s_g, turned.at[0], s_fg, s_fu, turned.at[1]], w, (z_send, z_recv, x_send, x_recv, w_local))
    ag_normed = Gather(place, normed_all, ag_send.at[0], ag_recv.at[0])
    ag_cot = Gather(place, cot_all, ag_send.at[1], ag_recv.at[1])
    ag_two = HalfGather(place, ffn_in, ag_send.at[2], ag_recv.at[2])
    branch = HalfScatter(place, keep, c_out, c_in, far_out, far_in, (c_send, c_recv, far_send, far_recv))
    outs = []

    def save(src, dst, index):
        copy = pltpu.make_async_copy(src, dst, out_sem.at[index])
        copy.start()
        outs.append(copy)

    def over(count, step, body):
        def loop(i, carry):
            body(pl.ds(pl.multiple_of(i * step, step), step), i)
            return carry

        lax.fori_loop(0, count // step, loop, 0)

    for copy in column_copies(place, x_hbm, x_ref, out_sem.at[16], block):
        copy.start()
    for copy in column_copies(place, cot_hbm, ag_cot.slot(0), out_sem.at[17], block):
        copy.start()
    flat = [
        pltpu.make_async_copy(s_o, natural.at[0], out_sem.at[21]),
        pltpu.make_async_copy(s_fd, natural.at[1], out_sem.at[22]),
    ]
    for copy in flat:
        copy.start()
    greet(place, True)
    pack_small(place, small_ref, gains_ref, biases_ref, group_gain_ref, decay_ref, tokens)
    for k, copy in enumerate(flat):
        copy.wait()
        cols = w.shape[2]
        for j in range(2):
            turned[k, :, j * cols : (j + 1) * cols] = natural[k, j * cols : (j + 1) * cols, :].T
    met(place, True)
    small = []
    for j, (bits, above, flips) in enumerate(place.pairs):
        copy = remote(small_ref, small_in.at[j], small_send.at[j], small_recv.at[j], place.peer(bits))
        copy.start()
        small.append(copy)
    size = gate_hidden.shape[1]

    def first_norm(r, i):
        value = normalized(x_ref[r, :].astype(F32))
        normed_all[r, :] = (value * params_ref[0:1, :] + params_ref[2:3, :]).astype(BF)

    def make_qk(r, i):
        qkv[r, : 2 * head_k] = dot_nn(normed_all[r, :], w[QK]).astype(BF)

    def make_v(r, i):
        qkv[r, 2 * head_k :] = dot_nn(normed_all[r, :], w[V]).astype(BF)

    def retention(r, i):
        start = pl.multiple_of((i // 2) * length, length)
        seq = pl.ds(start, length)
        scores = dot_nt(qkv[r, :head_k], qkv[seq, head_k : 2 * head_k])
        here = cum_row_ref[pl.ds(i // 2, 1), pl.ds(pl.multiple_of((i % 2) * tile, tile), tile)]
        decays = decay_tile(
            place.t, cum_row_ref[pl.ds(i // 2, 1), :], here, (i % 2) * tile, tile, length, tokens
        )
        weighted = (scores * decays * scale).astype(BF)
        mixed[r, :] = dot_nn(weighted, qkv[seq, 2 * head_k :])

    def gating(r, i):
        gate = dot_nn(normed_all[r, :], w[G])
        gate_in[r, :] = gate
        value = mixed[r, :]
        center = value - jnp.mean(value, axis=-1, keepdims=True)
        spread = jnp.mean(center * center, axis=-1, keepdims=True)
        flat = center * lax.rsqrt(jnp.maximum(spread, GROUP_FLOOR)) * group_ref[...]
        gated[r, :] = (flat * (gate * lax.logistic(gate))).astype(BF)

    def branch_part(i, carry):
        r = pl.ds(pl.multiple_of((3 - i) * tile, tile), tile)
        branch.part(3 - i, dot_nt(gated[r, :], w[O]))
        return carry

    def second_norm(r, i):
        value = x_ref[r, :].astype(F32) + branch.own(r)
        middle[r, :] = value
        ffn_in[r, :] = (normalized(value) * params_ref[1:2, :] + params_ref[3:4, :]).astype(BF)

    def feed(b):
        r = pl.ds(pl.multiple_of(b * tile, tile), tile)
        gate = dot_nn(ffn_in[r, :], w[FG])
        up = dot_nn(ffn_in[r, :], w[FU])
        gate_hidden[r, :] = gate
        up_hidden[r, :] = up
        hidden[r, :] = (gelu(gate) * up).astype(BF)

    def feed_back(r, i):
        back = dot_nn(cot_all[r, :], w[FD])
        gate = gate_hidden[r, :]
        value, slope = gelu_and_slope(gate)
        grads[r, :size] = (back * up_hidden[r, :] * slope).astype(BF)
        grads[r, size:] = (back * value).astype(BF)

    def small_step():
        pltpu.make_async_copy(x_hbm, x_ref, out_sem.at[16]).wait()
        for copy in small:
            copy.wait()
        spread_small(place, small_ref, small_in, params_ref, group_ref, cum_row_ref, block)

    def norm_step():
        over(tokens, 16, first_norm)

    def cot_start():
        pltpu.make_async_copy(cot_hbm, ag_cot.slot(0), out_sem.at[17]).wait()
        ag_cot.start()

    def chips(ag):
        lax.fori_loop(0, 4, lambda b, carry: (ag.chip(2 * b), carry)[1], 0)

    def qk_step():
        chips(ag_normed)
        weights.finish(QK)
        over(rows_all, tile, make_qk)
        save(normed_all, normed_out, 0)
        save(w.at[QK], w_out.at[QK], 1)
        save(params_ref, params_out, 18)
        save(group_ref, group_out, 19)
        save(cum_row_ref, cumul_out, 20)

    def v_step():
        weights.finish(V)
        over(rows_all, tile, make_v)
        over(rows_all, tile, retention)
        save(w.at[V], w_out.at[V], 2)
        save(qkv, qkv_out, 3)
        save(mixed, mixed_out, 4)

    def g_step():
        weights.finish(G)
        over(rows_all, tile, gating)
        save(w.at[G], w_out.at[G], 5)
        save(gate_in, gate_out, 6)

    def o_step():
        weights.finish(O)
        lax.fori_loop(0, 4, branch_part, 0)
        save(w.at[O], w_out.at[O], 7)

    def second_step():
        branch.wait_own()
        over(tokens, 16, second_norm)
        save(middle, middle_out, 9)

    def feed_step(b):
        if b == 0:
            weights.finish(FG)
            weights.finish(FU)
            save(w.at[FG], w_out.at[FG], 10)
            save(w.at[FU], w_out.at[FU], 11)

        def one(i, carry):
            ag_two.chip(2 * i)
            feed(i)
            return carry

        lax.fori_loop(b, b + 1, one, 0)

    def last_step():
        save(ffn_in, ffn_in_out, 12)
        save(hidden, hidden_out, 13)
        chips(ag_cot)
        save(cot_all, cot_out, 8)
        weights.finish(FD)
        save(w.at[FD], w_out.at[FD], 14)
        over(rows_all, tile, feed_back)
        save(grads, grads_out, 15)

    steps = {
        "small": small_step,
        "ln": norm_step,
        "ns": ag_normed.start,
        "nfz": ag_normed.from_z,
        "nfy": ag_normed.from_y,
        "nfzy": ag_normed.from_zy,
        "ks": cot_start,
        "kfz": ag_cot.from_z,
        "kfy": ag_cot.from_y,
        "kfzy": ag_cot.from_zy,
        "ts": ag_two.start,
        "tfz": ag_two.from_z,
        "tfzB": ag_two.from_z_rest,
        "tfy": ag_two.from_y,
        "tfzy": ag_two.from_zy,
        "qk": qk_step,
        "v": v_step,
        "g": g_step,
        "o": o_step,
        "p3": lambda: branch.pass_on(3),
        "p1": lambda: branch.pass_on(1),
        "p2": lambda: branch.pass_on(2),
        "p2B": lambda: branch.pass_on(2, 1),
        "ln2": second_step,
        "feedA": lambda: feed_step(0),
        "feedB": lambda: feed_step(1),
        "feedC": lambda: feed_step(2),
        "feedD": lambda: feed_step(3),
        "back": last_step,
    }
    for name in FORWARD:
        if name[1:].isdigit():
            g = int(name[1])
            if name[0] == "x":
                weights.own(g)
            elif name[0] == "s":
                weights.start(g, int(name[2]) - 1)
            elif name[0] == "f":
                weights.forward(g, int(name[2]) - 1)
            else:
                steps[name]()
        else:
            steps[name]()
    for copy in outs:
        copy.wait()
    for g in range(GROUPS):
        weights.sent(g)
    ag_normed.sent()
    ag_cot.sent()
    ag_two.sent()
    branch.sent()


ROOT = math.sqrt(2.0 / math.pi)


def gelu(v):
    return 0.5 * v * (1.0 + jnp.tanh(ROOT * (v + 0.044715 * v * v * v)))


def gelu_and_slope(v):
    inside = jnp.tanh(ROOT * (v + 0.044715 * v * v * v))
    slope = 0.5 * (1.0 + inside) + 0.5 * v * (1.0 - inside * inside) * ROOT * (1.0 + 3 * 0.044715 * v * v)
    return 0.5 * v * (1.0 + inside), slope


def forward_call(n_dp, x, cot, smalls, sources):
    tokens, width = x.shape
    length = 4 * tokens
    block = width // n_dp
    rows_all = 8 * tokens
    cols = sources[2].shape[1] // 2
    small_rows = -(-(4 + 2 * (cols + length) // block) // 8) * 8
    masks = n_dp // 2 - 1
    vmem, hbm = pl.BlockSpec(memory_space=pltpu.VMEM), pl.BlockSpec(memory_space=pl.ANY)
    shape = jax.ShapeDtypeStruct
    outs = (
        shape((GROUPS, width, cols), BF),
        shape((rows_all, width), BF),
        shape((rows_all, 2 * cols), BF),
        shape((rows_all, cols), F32),
        shape((rows_all, cols), F32),
        shape((rows_all, width), BF),
        shape((rows_all, cols), BF),
        shape((rows_all, 2 * cols), BF),
        shape((rows_all, width), BF),
        shape((tokens, width), F32),
        shape((8, width), F32),
        shape((1, cols), F32),
        shape((2, length), F32),
    )
    dma = pltpu.SemaphoreType.DMA
    scratch = [
        pltpu.VMEM((small_rows, block), F32),
        pltpu.VMEM((n_dp - 1, small_rows, block), F32),
        pltpu.VMEM((2, block, 2 * cols), BF),
        pltpu.VMEM((2, 2 * cols, block), BF),
        pltpu.VMEM((8, width), F32),
        pltpu.VMEM((1, cols), F32),
        pltpu.VMEM((2, length), F32),
        pltpu.VMEM((tokens, width), BF),
        pltpu.VMEM((GROUPS, width, cols), BF),
        pltpu.VMEM((rows_all, width), BF),
        pltpu.VMEM((rows_all, width), BF),
        pltpu.VMEM((rows_all, width), BF),
        pltpu.VMEM((rows_all, 2 * cols), BF),
        pltpu.VMEM((rows_all, cols), F32),
        pltpu.VMEM((rows_all, cols), F32),
        pltpu.VMEM((rows_all, cols), BF),
        pltpu.VMEM((rows_all, cols), F32),
        pltpu.VMEM((rows_all, cols), F32),
        pltpu.VMEM((rows_all, cols), BF),
        pltpu.VMEM((rows_all, 2 * cols), BF),
        pltpu.VMEM((tokens, width), F32),
        pltpu.VMEM((4, tokens, width), F32),
        pltpu.VMEM((4, tokens, width), BF),
        pltpu.VMEM((4, tokens, width), BF),
        pltpu.VMEM((3, tokens, width), BF),
        pltpu.VMEM((3, tokens, width), BF),
        dma((GROUPS,)),
        dma((GROUPS, masks)),
        dma((GROUPS,)),
        dma((GROUPS,)),
        dma((GROUPS,)),
        dma((3, 9)),
        dma((3, 9)),
        dma((4,)),
        dma((4,)),
        dma((5,)),
        dma((5,)),
        dma((23,)),
        dma((n_dp - 1,)),
        dma((n_dp - 1,)),
    ]
    return pl.pallas_call(
        functools.partial(forward_kernel, n_dp),
        out_shape=outs,
        in_specs=[hbm, hbm] + [vmem] * 4 + [hbm] * len(sources),
        out_specs=(hbm,) * len(outs),
        scratch_shapes=scratch,
        compiler_params=pltpu.CompilerParams(
            collective_id=1, has_side_effects=True, vmem_limit_bytes=64_000_000
        ),
    )(x, cot, *smalls, *sources)


class Reduce:
    def __init__(self, place, keep, x_out, x_in, z_in, own_out, sems, own_sem):
        self.place = place
        self.keep, self.x_out, self.x_in, self.z_in, self.own_out = keep, x_out, x_in, z_in, own_out
        self.x_send, self.x_recv, self.z_send, self.z_recv = sems
        self.own_sem = own_sem
        self.block = z_in.shape[2]
        self.half = place.n_dp // 2
        z = place.z
        self.targets = [
            ((1 - z if flips else z) + above, i, place.peer(bits)) for i, (bits, above, flips) in enumerate(place.masks)
        ]
        self.targets.reverse()

    def rows(self, position):
        return pl.ds(pl.multiple_of(position * self.block, self.block), self.block)

    def x_copy(self, g, ring, position):
        return remote(
            self.x_out.at[ring, self.rows(position), :],
            self.x_in.at[g, self.rows(position), :],
            self.x_send.at[g],
            self.x_recv.at[g, position],
            self.place.x_peer(),
        )

    def z_copy(self, g, position, i, peer):
        return remote(
            self.keep.at[g, self.rows(position), :],
            self.z_in.at[g, i],
            self.z_send.at[g],
            self.z_recv.at[g, i],
            peer,
        )

    def upper(self, g, ring, left, right, col, step):
        width = left.shape[1] // 2
        cols = self.keep.shape[2]

        def body(i, carry):
            at = pl.multiple_of(i * step, step)
            value = dot_tn(left[:, pl.ds(pl.multiple_of(width + at, step), step)], right[:, col : col + cols])
            self.x_out[ring, pl.ds(at, step), :] = value.astype(BF)
            return carry

        lax.fori_loop(0, width // step, body, 0)
        for position, _, _ in self.targets:
            self.x_copy(g, ring, position).start()
        self.x_copy(g, ring, self.place.z).start()

    def lower(self, g, left, right, col, step):
        width = left.shape[1] // 2
        cols = self.keep.shape[2]

        def body(i, carry):
            at = pl.ds(pl.multiple_of(i * step, step), step)
            self.keep[g, at, :] = dot_tn(left[:, at], right[:, col : col + cols]).astype(BF)
            return carry

        lax.fori_loop(0, width // step, body, 0)

    def x_sent(self, g, ring):
        whole = self.x_out.at[ring]
        remote(whole, whole, self.x_send.at[g], self.x_recv.at[g, 0], self.place.x_peer()).wait_send()

    def add(self, g, ring, position):
        self.x_copy(g, ring, position).wait_recv()
        step = min(64, self.block)

        def body(i, carry):
            r = pl.ds(pl.multiple_of(position * self.block + i * step, step), step)
            self.keep[g, r, :] = (self.keep[g, r, :].astype(F32) + self.x_in[g, r, :].astype(F32)).astype(BF)
            return carry

        lax.fori_loop(0, self.block // step, body, 0)

    def own_copy(self, g):
        return pltpu.make_async_copy(
            self.keep.at[g, self.rows(self.place.z), :], self.own_out.at[g], self.own_sem.at[g]
        )

    def step(self, g, ring, third):
        if third == 0:
            self.add(g, ring, self.place.z)
            self.own_copy(g).start()
            return
        count = len(self.targets)
        for position, i, peer in self.targets[(3 - third) * count // 3 : (4 - third) * count // 3]:
            self.add(g, ring, position)
            self.z_copy(g, position, i, peer).start()

    def finish(self, g):
        self.own_copy(g).wait()
        for position, i, peer in self.targets:
            self.z_copy(g, position, i, peer).wait()


def norm_back(value, grad, gain):
    center = value - jnp.mean(value, axis=-1, keepdims=True)
    spread = jnp.mean(center * center, axis=-1, keepdims=True)
    r = lax.rsqrt(spread + EPSILON)
    hat = center * r
    scaled = grad * gain
    back = r * (
        scaled - jnp.mean(scaled, axis=-1, keepdims=True) - hat * jnp.mean(scaled * hat, axis=-1, keepdims=True)
    )
    return back, jnp.sum(grad * hat, axis=0, keepdims=True), jnp.sum(grad, axis=0, keepdims=True)


def backward_kernel(
    n_dp,
    x_hbm,
    params_ref,
    group_ref,
    cum_row_ref,
    w_ref,
    normed_ref,
    qkv_ref,
    gate_ref,
    mixed_ref,
    ffn_in_ref,
    hidden_ref,
    grads_ref,
    cot_ref,
    middle_ref,
    layer_out,
    input_grad_out,
    own_out,
    z_in,
    sums_out,
    w,
    tokens_a,
    ffn_in,
    branch_all,
    slim,
    qkv,
    gate_in,
    mixed,
    gated,
    x_ref,
    middle,
    grad_middle,
    sums,
    sums_in,
    group_sum,
    payload,
    payload_in,
    keep,
    c_out,
    c_in,
    far_in,
    c_in_two,
    far_in_two,
    dw_keep,
    x_out,
    x_in,
    ag_send,
    ag_recv,
    c_send,
    c_recv,
    far_send,
    far_recv,
    x_send,
    x_recv,
    z_send,
    z_recv,
    load_sem,
    own_sem,
    sum_send,
    sum_recv,
    pay_send,
    pay_recv,
):
    place = Place(n_dp)
    tokens, width = x_ref.shape
    rows_all = 8 * tokens
    length = rows_all // 2
    cols = gated.shape[1]
    head_k = cols // 2
    scale = 1.0 / math.sqrt(head_k)
    tile = 2 * tokens
    step = min(512, width // 2)
    block = z_in.shape[2]
    ag = Gather(place, branch_all, ag_send, ag_recv)

    def scatter(k, c, far):
        return Scatter(place, keep, c_out, c, None, far, (c_send.at[k], c_recv.at[k], far_send.at[k], far_recv.at[k]))

    rs_two = scatter(0, c_in, far_in)
    rs_out = scatter(1, c_in_two, far_in_two)
    rs_one = scatter(2, c_in, far_in)
    dw = Reduce(place, dw_keep, x_out, x_in, z_in, own_out, (x_send, x_recv, z_send, z_recv), own_sem)
    result = ffn_in.at[:tokens, :]
    weighted = ffn_in.at[tokens : tokens + length, :length]
    score_back = ffn_in.at[tokens : tokens + length, length : 2 * length]
    ring = {FD: 0, FG: 1, FU: 2, O: 3, G: 0, QK: 1, V: 2}

    def load(src, dst, index):
        copy = pltpu.make_async_copy(src, dst, load_sem.at[index])
        copy.start()
        return copy

    def over(count, size, body):
        def loop(i, carry):
            body(pl.ds(pl.multiple_of(i * size, size), size), i)
            return carry

        lax.fori_loop(0, count // size, loop, 0)

    in_cot = load(cot_ref, tokens_a, 3)
    in_hidden = load(hidden_ref, slim.at[:, 2 * cols :], 4)
    in_grads = load(grads_ref, slim.at[:, : 2 * cols], 0)
    in_fg = load(w_ref.at[FG], w.at[0], 1)
    in_fu = load(w_ref.at[FU], w.at[1], 2)
    in_ffn = load(ffn_in_ref, ffn_in, 5)
    in_middle = load(middle_ref, middle, 6)
    in_mixed = load(mixed_ref, mixed, 7)
    in_gate = load(gate_ref, gate_in, 8)
    in_o = load(w_ref.at[O], w.at[2], 9)
    in_qkv = load(qkv_ref, qkv, 10)
    for copy in column_copies(place, x_hbm, x_ref, load_sem.at[11], block):
        copy.start()
    sums[...] = jnp.zeros_like(sums)
    group_sum[...] = jnp.zeros_like(group_sum)
    entry_barrier(place, True)
    waited = []

    def ready(*copies):
        for copy in copies:
            if not any(copy is other for other in waited):
                waited.append(copy)
                copy.wait()

    def rows_of(i):
        return 3 - i, pl.ds(pl.multiple_of((3 - i) * tile, tile), tile)

    def two_part(i, carry):
        b, r = rows_of(i)
        rs_two.part(b, dot_nt(slim[r, :cols], w[0]) + dot_nt(slim[r, cols : 2 * cols], w[1]))
        return carry

    def gating(r, i):
        value = mixed[r, :]
        center = value - jnp.mean(value, axis=-1, keepdims=True)
        spread = jnp.mean(center * center, axis=-1, keepdims=True)
        gate = gate_in[r, :]
        flat = center * lax.rsqrt(jnp.maximum(spread, GROUP_FLOOR)) * group_ref[...]
        gated[r, :] = (flat * (gate * lax.logistic(gate))).astype(BF)

    def second_back(r, i):
        back, gain_sum, bias_sum = norm_back(middle[r, :], rs_two.own(r), params_ref[1:2, :])
        total = tokens_a[r, :].astype(F32) + back
        grad_middle[r, :] = total
        branch_all[r, :] = total.astype(BF)
        sums[1:2, :] += gain_sum
        sums[3:4, :] += bias_sum

    def out_part(i, carry):
        b, r = rows_of(i)
        rs_out.part(b, dot_nt(slim[r, 2 * cols :], w[0]))
        return carry

    def gating_back(b):
        r = pl.ds(pl.multiple_of(b * tile, tile), tile)
        back = dot_nn(branch_all[r, :], w[2])
        value = mixed[r, :]
        center = value - jnp.mean(value, axis=-1, keepdims=True)
        spread = jnp.mean(center * center, axis=-1, keepdims=True)
        inverse = lax.rsqrt(jnp.maximum(spread, GROUP_FLOOR))
        hat = center * inverse
        gate = gate_in[r, :]
        sigmoid = lax.logistic(gate)
        flat = hat * group_ref[...]
        slope = sigmoid * (1.0 + gate * (1.0 - sigmoid))
        slim[r, 2 * cols :] = (back * flat * slope).astype(BF)
        grad = back * (gate * sigmoid)
        group_sum[...] += jnp.sum(grad * hat, axis=0, keepdims=True)
        scaled = grad * group_ref[...]
        live = jnp.where(spread > GROUP_FLOOR, 1.0, jnp.where(spread == GROUP_FLOOR, 0.5, 0.0))
        moment = jnp.mean(scaled * hat, axis=-1, keepdims=True) * live
        mixed_back = inverse * (scaled - jnp.mean(scaled, axis=-1, keepdims=True) - hat * moment)
        slim[r, cols : 2 * cols] = mixed_back.astype(BF)

    def sequence_back(s):
        seq = pl.ds(pl.multiple_of(s * length, length), length)

        def body(i, carry):
            r = pl.ds(pl.multiple_of(s * length + i * tile, tile), tile)
            at = pl.ds(pl.multiple_of(i * tile, tile), tile)
            scores = dot_nt(qkv[r, :head_k], qkv[seq, head_k : 2 * head_k])
            here = cum_row_ref[pl.ds(s, 1), at]
            decays = decay_tile(
                place.t, cum_row_ref[pl.ds(s, 1), :], here, i * tile, tile, length, tokens
            )
            weighted[at, :] = (scores * decays * scale).astype(BF)
            back = dot_nt(slim[r, cols : 2 * cols], qkv[seq, 2 * head_k :])
            grad = (back * decays * scale).astype(BF)
            score_back[at, :] = grad
            slim[r, :head_k] = dot_nn(grad, qkv[seq, head_k : 2 * head_k]).astype(BF)
            return carry

        lax.fori_loop(0, length // tile, body, 0)
        slim[seq, head_k : 2 * head_k] = dot_tn(score_back[...], qkv[seq, :head_k]).astype(BF)
        slim[seq, cols : 2 * cols] = dot_tn(weighted[...], slim[seq, cols : 2 * cols]).astype(BF)


    def finish_out(r, i):
        result[r, :] = (middle[r, :] + rs_out.own(r)).astype(BF)

    def one_part(i, carry):
        b, r = rows_of(i)
        total = dot_nt(slim[r, :cols], w[1]) + dot_nt(slim[r, cols : 2 * cols], w[0])
        rs_one.part(b, total + dot_nt(slim[r, 2 * cols :], w[2]))
        return carry

    def first_back(r, i):
        back, gain_sum, bias_sum = norm_back(x_ref[r, :].astype(F32), rs_one.own(r), params_ref[0:1, :])
        result[r, :] = (grad_middle[r, :] + back).astype(BF)
        sums[0:1, :] += gain_sum
        sums[2:3, :] += bias_sum

    def sum_copy(k):
        peer = (place.c_peer(), place.y_peer())[k]
        return remote(sums, sums_in.at[k], sum_send.at[k], sum_recv.at[k], peer)

    pay = []
    for j, (bits, above, flips) in enumerate(place.pairs):
        position = (1 - place.z if flips else place.z) + above
        pay.append(remote(payload.at[position], payload_in.at[j], pay_send.at[j], pay_recv.at[j], place.peer(bits)))

    later = {}
    operands = {
        FD: (tokens_a, 2 * cols),
        FG: (ffn_in, 0),
        FU: (ffn_in, cols),
        O: (branch_all, None),
        QK: (tokens_a, 0),
        V: (tokens_a, cols),
        G: (tokens_a, 2 * cols),
    }

    def operands_of(g):
        ready(*{FD: (in_cot, in_hidden), FG: (in_ffn, in_grads), FU: (in_ffn, in_grads), O: ()}.get(g, (later.get(3),)))
        left, col = operands[g]
        return (left, gated, 0, step) if col is None else (left, slim, col, step)

    def two_step():
        ready(in_grads, in_fg, in_fu)
        lax.fori_loop(0, 4, two_part, 0)
        later[FD] = load(w_ref.at[FD], w.at[0], 1)
        later[QK] = load(w_ref.at[QK], w.at[1], 2)

    def gating_step():
        ready(in_mixed, in_gate)
        over(rows_all, tokens, gating)

    def second_step():
        ready(in_middle)
        rs_two.wait_own()
        over(tokens, 16, second_back)
        later[3] = load(normed_ref, tokens_a, 3)

    def out_step():
        rs_two.sent()
        ready(later[FD])
        lax.fori_loop(0, 4, out_part, 0)
        later[V] = load(w_ref.at[V], w.at[0], 1)

    def chip_step(first):
        ready(in_o, in_qkv)

        def chip(b, carry):
            ag.chip(2 * b)
            gating_back(b)
            return carry

        lax.fori_loop(first, first + 2, chip, 0)
        if first:
            later[G] = load(w_ref.at[G], w.at[2], 9)

    def sequence_step(s):
        lax.fori_loop(s, s + 1, lambda i, carry: (sequence_back(i), carry)[1], 0)

    def out_finish():
        rs_out.wait_own()
        over(tokens, 16, finish_out)
        later["layer"] = load(result, layer_out, 4)

    def one_step():
        rs_out.sent()
        ready(later[QK], later[V], later[G])
        lax.fori_loop(0, 4, one_part, 0)

    def first_step():
        pltpu.make_async_copy(x_hbm, x_ref, load_sem.at[11]).wait()
        ready(later["layer"])
        rs_one.wait_own()
        over(tokens, 16, first_back)
        later["grad"] = load(result, input_grad_out, 4)

    def sum_cores():
        sum_copy(0).start()

    def sum_chips():
        sum_copy(0).wait()
        sums[...] += sums_in[0]
        sum_copy(1).start()

    def pay_start():
        sum_copy(1).wait()
        sums[...] += sums_in[1]
        for p in range(n_dp):
            payload[p, 0:4, :] = sums[0:4, p * block : (p + 1) * block]
            for k in range(cols // block):
                payload[p, 4 + k : 5 + k, :] = group_sum[0:1, k * block : (k + 1) * block]
        for copy in pay:
            copy.start()

    def pay_finish():
        for copy in pay:
            copy.wait()
        mine = payload[place.z]
        other = jnp.zeros_like(mine)
        for j, (bits, above, flips) in enumerate(place.pairs):
            if flips:
                other = other + payload_in[j]
            else:
                mine = mine + payload_in[j]
        sums_out[0] = mine
        sums_out[1] = other

    before = {G: FD, QK: FG, V: FU}

    def upper(g):
        if g in before:
            dw.x_sent(before[g], ring[before[g]])
        dw.upper(g, ring[g], *operands_of(g))

    steps = {
        "two": two_step,
        "a3": lambda: rs_two.pass_on(3),
        "a1": lambda: rs_two.pass_on(1),
        "a2": lambda: rs_two.pass_on(2),
        "gat": gating_step,
        "lnb": second_step,
        "bs": ag.start,
        "bfz": ag.from_z,
        "bfy": ag.from_y,
        "bfzy": ag.from_zy,
        "out": out_step,
        "o3": lambda: rs_out.pass_on(3),
        "o1": lambda: rs_out.pass_on(1),
        "o2": lambda: rs_out.pass_on(2),
        "gbA": lambda: chip_step(0),
        "gbB": lambda: chip_step(2),
        "seq0": lambda: sequence_step(0),
        "seq1": lambda: sequence_step(1),
        "outf": out_finish,
        "one": one_step,
        "b3": lambda: rs_one.pass_on(3),
        "b1": lambda: rs_one.pass_on(1),
        "b2": lambda: rs_one.pass_on(2),
        "lna": first_step,
        "sc": sum_cores,
        "sy": sum_chips,
        "pay": pay_start,
        "payw": pay_finish,
    }
    for name in BACKWARD:
        if name in steps:
            steps[name]()
        elif name[0] == "u":
            upper(int(name[1]))
        elif name[0] == "l":
            dw.lower(int(name[1]), *operands_of(int(name[1])))
        else:
            dw.step(int(name[1]), ring[int(name[1])], int(name[2]))
    ready(later["grad"])
    for g in (O, G, QK, V):
        dw.x_sent(g, ring[g])
    ag.sent()
    rs_one.sent()
    for g in (FD, FG, FU, O, G, QK, V):
        dw.finish(g)


def backward_call(n_dp, x, params, group, cum_row, saved):
    tokens, width = x.shape
    rows_all = 8 * tokens
    w = saved[0]
    cols = w.shape[2]
    block = width // n_dp
    masks = n_dp // 2 - 1
    vmem, hbm = pl.BlockSpec(memory_space=pltpu.VMEM), pl.BlockSpec(memory_space=pl.ANY)
    shape = jax.ShapeDtypeStruct
    pay_rows = -(-(4 + cols // block) // 8) * 8
    outs = (
        shape((tokens, width), BF),
        shape((tokens, width), BF),
        shape((GROUPS, block, cols), BF),
        shape((GROUPS, masks, block, cols), BF),
        shape((2, pay_rows, block), F32),
    )
    dma = pltpu.SemaphoreType.DMA
    scratch = [
        pltpu.VMEM((3, width, cols), BF),
        pltpu.VMEM((rows_all, width), BF),
        pltpu.VMEM((rows_all, width), BF),
        pltpu.VMEM((rows_all, width), BF),
        pltpu.VMEM((rows_all, 3 * cols), BF),
        pltpu.VMEM((rows_all, 2 * cols), BF),
        pltpu.VMEM((rows_all, cols), F32),
        pltpu.VMEM((rows_all, cols), F32),
        pltpu.VMEM((rows_all, cols), BF),
        pltpu.VMEM((tokens, width), BF),
        pltpu.VMEM((tokens, width), F32),
        pltpu.VMEM((tokens, width), F32),
        pltpu.VMEM((8, width), F32),
        pltpu.VMEM((2, 8, width), F32),
        pltpu.VMEM((1, cols), F32),
        pltpu.VMEM((n_dp, pay_rows, block), F32),
        pltpu.VMEM((n_dp - 1, pay_rows, block), F32),
        pltpu.VMEM((4, tokens, width), BF),
        pltpu.VMEM((4, tokens, width), BF),
        pltpu.VMEM((4, tokens, width), BF),
        pltpu.VMEM((3, tokens, width), BF),
        pltpu.VMEM((4, tokens, width), BF),
        pltpu.VMEM((3, tokens, width), BF),
        pltpu.VMEM((GROUPS, width // 2, cols), BF),
        pltpu.VMEM((4, width // 2, cols), BF),
        pltpu.VMEM((GROUPS, width // 2, cols), BF),
        dma((7,)),
        dma((7,)),
        dma((3, 4)),
        dma((3, 4)),
        dma((3, 3)),
        dma((3, 3)),
        dma((GROUPS,)),
        dma((GROUPS, n_dp // 2)),
        dma((GROUPS,)),
        dma((GROUPS, masks)),
        dma((12,)),
        dma((GROUPS,)),
        dma((2,)),
        dma((2,)),
        dma((n_dp - 1,)),
        dma((n_dp - 1,)),
    ]
    return pl.pallas_call(
        functools.partial(backward_kernel, n_dp),
        out_shape=outs,
        in_specs=[hbm, vmem, vmem, vmem] + [hbm] * len(saved),
        out_specs=(hbm,) * 4 + (vmem,),
        scratch_shapes=scratch,
        compiler_params=pltpu.CompilerParams(
            collective_id=2, has_side_effects=True, vmem_limit_bytes=67_000_000
        ),
    )(x, params, group, cum_row, *saved)


def finish_kernel(
    n_dp,
    own_ref,
    others_ref,
    layer_ref,
    grad_ref,
    sums_ref,
    layer_out,
    input_grad,
    query_grad,
    key_grad,
    value_grad,
    gate_grad,
    out_grad,
    group_grad,
    gain_grad,
    bias_grad,
    ffn_gate_grad,
    ffn_up_grad,
    ffn_down_grad,
    own,
    others,
    rows,
    wide,
    tall,
    in_sem,
    out_sem,
    row_sem,
):
    place = Place(n_dp)
    z = place.z
    block, cols = own.shape[1:]
    loads = []
    for g in (FD, FG, FU, O, QK, V, G):
        pair = (
            pltpu.make_async_copy(own_ref.at[g], own.at[g], in_sem.at[0, g]),
            pltpu.make_async_copy(others_ref.at[g], others.at[g], in_sem.at[1, g]),
        )
        for copy in pair:
            copy.start()
        loads.append((g, pair))
    row_loads = [
        pltpu.make_async_copy(layer_ref, rows.at[0], row_sem.at[0]),
        pltpu.make_async_copy(grad_ref, rows.at[1], row_sem.at[1]),
    ]
    for copy in row_loads:
        copy.start()
    outs = []

    def save(src, dst, index):
        copy = pltpu.make_async_copy(src, dst, out_sem.at[index])
        copy.start()
        outs.append(copy)

    wide_at = {FG: 0, FU: 1, V: 2, G: 3, QK: 4}
    tall_at = {FD: 0, O: 1}
    targets = {FG: ffn_gate_grad, FU: ffn_up_grad, V: value_grad, G: gate_grad, FD: ffn_down_grad, O: out_grad}
    for g, pair in loads:
        for copy in pair:
            copy.wait()
        mine = own[g].astype(F32)
        theirs = None
        for i, (bits, above, flips) in enumerate(place.masks):
            value = others[g, i].astype(F32)
            if not flips:
                mine = mine + value
            else:
                theirs = value if theirs is None else theirs + value
        if g in tall_at:
            k = tall_at[g]
            tall[k, pl.ds(pl.multiple_of(z * cols, cols), cols), :] = mine.T
            tall[k, pl.ds(pl.multiple_of((1 - z) * cols, cols), cols), :] = theirs.T
            save(tall.at[k], targets[g], k)
            continue
        k = wide_at[g]
        if g == QK:
            half = cols // 2
            for which, dst in ((0, query_grad), (1, key_grad)):
                part = slice(which * half, (which + 1) * half)
                at = which * cols
                wide[k, :, pl.ds(pl.multiple_of(at + z * half, half), half)] = mine[:, part]
                wide[k, :, pl.ds(pl.multiple_of(at + (1 - z) * half, half), half)] = theirs[:, part]
                save(wide.at[k, :, pl.ds(at, cols)], dst, 2 + which)
            continue
        wide[k, :, pl.ds(pl.multiple_of(z * cols, cols), cols)] = mine
        wide[k, :, pl.ds(pl.multiple_of((1 - z) * cols, cols), cols)] = theirs
        save(wide.at[k], targets[g], 4 + k)
    for k, dst in ((0, layer_out), (1, input_grad)):
        row_loads[k].wait()
        for copy in column_copies(place, rows.at[k], dst, row_sem.at[k], block, True):
            copy.start()
    norm = sums_ref[0, 0:4, :] + sums_ref[1, 0:4, :]
    piece = gain_grad.shape[1]
    mine = norm[:, :piece]
    for k in range(1, block // piece):
        mine = jnp.where(place.t == k, norm[:, k * piece : (k + 1) * piece], mine)
    gain_grad[...] = mine[0:2, :]
    bias_grad[...] = mine[2:4, :]
    piece = group_grad.shape[1]
    here = place.d % (block // piece)
    row = place.d // (block // piece)

    def group_of(which):
        value = sums_ref[which, 4:5, :]
        for k in range(1, cols // block):
            value = jnp.where(row == k, sums_ref[which, 4 + k : 5 + k, :], value)
        out = value[:, :piece]
        for k in range(1, block // piece):
            out = jnp.where(here == k, value[:, k * piece : (k + 1) * piece], out)
        return out

    same, other = group_of(0), group_of(1)
    group_grad[0:1, :] = jnp.where(z == 0, same, other)
    group_grad[1:2, :] = jnp.where(z == 0, other, same)
    for copy in outs:
        copy.wait()
    for k, dst in ((0, layer_out), (1, input_grad)):
        pltpu.make_async_copy(rows.at[k], dst, row_sem.at[k]).wait()


def finish_call(n_dp, n_tensor, own, others, layer, grad, sums):
    tokens, width = layer.shape
    block, cols = own.shape[1:]
    masks = others.shape[1]
    vmem, hbm = pl.BlockSpec(memory_space=pltpu.VMEM), pl.BlockSpec(memory_space=pl.ANY)
    shape = jax.ShapeDtypeStruct
    rows, wide, tall = shape((tokens, width), BF), shape((block, 2 * cols), F32), shape((2 * cols, block), F32)
    thin, norm = shape((block, cols), F32), shape((2, width // (n_dp * n_tensor)), F32)
    outs = (rows, rows, thin, thin, wide, wide, tall, shape((2, cols // n_dp), F32), norm, norm, wide, wide, tall)
    specs = [vmem if o.shape[0] == 2 else hbm for o in outs]
    dma = pltpu.SemaphoreType.DMA
    return pl.pallas_call(
        functools.partial(finish_kernel, n_dp),
        out_shape=outs,
        in_specs=[hbm, hbm, hbm, hbm, vmem],
        out_specs=tuple(specs),
        scratch_shapes=[
            pltpu.VMEM((GROUPS, block, cols), BF),
            pltpu.VMEM((GROUPS, masks, block, cols), BF),
            pltpu.VMEM((2, tokens, width), BF),
            pltpu.VMEM((5, block, 2 * cols), F32),
            pltpu.VMEM((2, 2 * cols, block), F32),
            dma((2, GROUPS)),
            dma((8,)),
            dma((2,)),
        ],
        compiler_params=pltpu.CompilerParams(vmem_limit_bytes=67_000_000),
    )(own, others, layer, grad, sums)


def per_device(
    n_dp,
    n_tensor,
    inputs,
    cotangent,
    log_decay,
    query_weight,
    key_weight,
    value_weight,
    gate_weight,
    out_weight,
    group_gain,
    norm_gains,
    norm_biases,
    ffn_gate_weight,
    ffn_up_weight,
    ffn_down_weight,
):
    place = Place(n_dp)
    d, t = place.d, place.t
    tokens, width = inputs.shape
    block = width // n_dp

    def position_of(q):
        out = (q // PAIR) & 1
        for k, bit in enumerate(place.rest):
            out = out + ((d // bit) % 2 ^ ((q // bit) & 1)) * (2 << k)
        return out

    def moved(value, index):
        if block % 128 == 0:
            return value
        return jnp.concatenate(
            [lax.dynamic_slice_in_dim(value, index(p) * block, block, 1) for p in range(n_dp)], axis=1
        )

    smalls = (norm_gains, norm_biases, group_gain, log_decay)
    sources = (
        query_weight,
        key_weight,
        value_weight,
        gate_weight,
        out_weight,
        ffn_gate_weight,
        ffn_up_weight,
        ffn_down_weight,
    )
    x, cot = moved(inputs, place.dp_of), moved(cotangent, place.dp_of)
    *saved, params, group, cumul = forward_call(n_dp, x, cot, smalls, sources)
    layer, grad, own, others, sums = backward_call(n_dp, x, params, group, cumul, saved)
    outs = finish_call(n_dp, n_tensor, own, others, layer, grad, sums)
    return (moved(outs[0], position_of), moved(outs[1], position_of), *outs[2:])


def solution(mesh):
    tokens = P(("dp", "tensor"), None)
    rows, cols, norms = P("dp", "tensor"), P("tensor", "dp"), P(None, "dp")
    sums = P(None, ("dp", "tensor"))
    in_specs = (tokens, tokens, cols, rows, rows, rows, rows, cols, cols, norms, norms, rows, rows, cols)
    out_specs = (tokens, tokens, rows, rows, rows, rows, cols, cols, sums, sums, rows, rows, cols)
    body = functools.partial(per_device, mesh.shape["dp"], mesh.shape["tensor"])
    return jax.shard_map(body, mesh=mesh, in_specs=in_specs, out_specs=out_specs, check_vma=False)
```

```python
import functools
import math

import jax
import jax.numpy as jnp
from jax import lax
from jax.experimental import pallas as pl
from jax.experimental.pallas import tpu as pltpu
from jax.sharding import PartitionSpec as P

EPSILON = 1e-05
GROUP_FLOOR = 1.0
BF = jnp.bfloat16
F32 = jnp.float32
PAIR = 2
MESH = pl.DeviceIdType.MESH
QK, V, G, O, FG, FU, FD = range(7)
GROUPS = 7


FORWARD = (
    "s22", "s11", "x1", "small", "s32", "ks", "x4", "x3", "x2", "kfy", "ln", "s02", "ns", "s03", "s01", "s31",
    "f22", "nfy", "f11", "s13", "f32", "f02", "s33", "s23", "x0", "x6", "f01", "f31", "nfz", "nfzy", "s12", "f03",
    "s21", "f13", "f23", "kfz", "qk", "s51", "s42", "f12", "s52", "f21", "s41", "f33", "s61", "s63", "v", "g", "o",
    "p3", "f42", "f41", "f61", "p2", "x5", "kfzy", "f63", "s53", "p1", "p2B", "f51", "s43", "ln2", "f52", "ts",
    "tfy", "f53", "s62", "f43", "tfz", "tfzB", "f62", "feedA", "feedB", "feedC", "tfzy", "feedD", "back",
)
BACKWARD = (
    "u6", "two", "a3", "a1", "l6", "s63", "l4", "a2", "s62", "u4", "u5", "s43", "lnb", "bs", "bfz", "s42", "s41",
    "l5", "out", "o3", "s52", "bfy", "s51", "gat", "s40", "gbA", "bfzy", "gbB", "u3", "l2", "u2", "seq0", "s53",
    "o2", "seq1", "u0", "u1", "l0", "l3", "o1", "s33", "outf", "s32", "s31", "one", "s61", "s23", "s30", "b3",
    "l1", "b2", "s22", "s02", "b1", "s01", "s21", "s03", "s13", "lna", "s10", "s00", "s20", "sc", "sy", "pay",
    "s50", "s12", "s60", "s11", "payw",
)


def dot_nn(a, b):
    return lax.dot_general(a, b, (((1,), (0,)), ((), ())), preferred_element_type=F32)


def dot_nt(a, b):
    return lax.dot_general(a, b, (((1,), (1,)), ((), ())), preferred_element_type=F32)


def dot_tn(a, b):
    return lax.dot_general(a, b, (((0,), (0,)), ((), ())), preferred_element_type=F32)


def flip(index, bit):
    return index + bit - 2 * bit * ((index // bit) % 2)


class Place:
    def __init__(self, n_dp):
        self.n_dp = n_dp
        self.d = lax.axis_index("dp")
        self.t = lax.axis_index("tensor")
        self.z = (self.d // PAIR) % 2
        self.rest = [1 << i for i in range(2, n_dp.bit_length() - 1)] + [1]
        self.inner = self.rest[:-1]
        self.masks = []
        for pick in range(1, 1 << (1 + len(self.inner))):
            bits = [PAIR] * (pick & 1) + [b for k, b in enumerate(self.inner) if (pick >> (k + 1)) & 1]
            self.masks.append((bits, pick & ~1, pick & 1))
        half = n_dp // 2
        self.pairs = self.masks + [([1], half, 0)] + [(bits + [1], above + half, flips) for bits, above, flips in self.masks]

    def slot(self, above, flips):
        return next((j for j, pair in enumerate(self.pairs) if pair[1:] == (above, flips)), None)

    def dp_of(self, p):
        out = (p & 1) * PAIR
        for k, bit in enumerate(self.rest):
            here = (self.d // bit) % 2
            out = out + (1 - here if (p >> (k + 1)) & 1 else here) * bit
        return out

    def peer(self, bits):
        out = self.d
        for bit in bits:
            out = flip(out, bit)
        return {"dp": out}

    def x_peer(self):
        return {"dp": flip(self.d, 1)}

    def z_peer(self):
        return {"dp": flip(self.d, PAIR)}

    def y_peer(self):
        return {"tensor": flip(self.t, 2)}

    def c_peer(self):
        return {"tensor": flip(self.t, 1)}

    def everyone(self, far):
        near = [self.x_peer(), self.y_peer(), self.c_peer()]
        if far:
            return near[1:] + [self.peer(bits) for bits, _, _ in self.pairs]
        return near + [self.peer(bits) for bits, _, _ in self.masks]


def greet(place, far):
    barrier = pltpu.get_barrier_semaphore()
    for peer in place.everyone(far):
        pl.semaphore_signal(barrier, inc=1, device_id=peer, device_id_type=MESH)


def met(place, far):
    pl.semaphore_wait(pltpu.get_barrier_semaphore(), len(place.everyone(far)))


def entry_barrier(place, far=False):
    greet(place, far)
    met(place, far)


def column_copies(place, src, dst, sem, block, back=False):
    if block % 128:
        return [pltpu.make_async_copy(src, dst, sem)]
    out = []
    for p in range(place.n_dp):
        natural = pl.ds(pl.multiple_of(place.dp_of(p) * block, block), block)
        here = pl.ds(p * block, block)
        a, b = (here, natural) if back else (natural, here)
        out.append(pltpu.make_async_copy(src.at[:, a], dst.at[:, b], sem))
    return out


def remote(src, dst, send, recv, peer):
    return pltpu.make_async_remote_copy(
        src_ref=src, dst_ref=dst, send_sem=send, recv_sem=recv, device_id=peer, device_id_type=MESH
    )


class Weights:
    def __init__(self, place, sources, full, sems):
        self.place, self.sources, self.full = place, sources, full
        self.z_send, self.z_recv, self.x_send, self.x_recv, self.local = sems
        self.block = sources[-1].shape[0]
        self.cols = sources[-1].shape[1] // 2
        self.half = place.n_dp // 2

    def rows(self, position, count=1):
        return pl.ds(pl.multiple_of(position * self.block, self.block), count * self.block)

    def pairs(self, g, half, position):
        parts = self.sources[g] if isinstance(self.sources[g], tuple) else (self.sources[g],)
        count = self.cols // len(parts)
        for k, part in enumerate(parts):
            columns = pl.ds(pl.multiple_of(half * count, count), count)
            yield part.at[:, columns], self.full.at[g, self.rows(position), k * count : (k + 1) * count]

    def own(self, g):
        z = self.place.z
        for src, dst in self.pairs(g, z, z):
            pltpu.make_async_copy(src, dst, self.local.at[g]).start()
        for src, dst in self.pairs(g, z, z + self.half):
            remote(src, dst, self.x_send.at[g], self.x_recv.at[g], self.place.x_peer()).start()

    def some(self, third):
        count = len(self.place.masks)
        return reversed(range(third * count // 3, (third + 1) * count // 3))

    def start(self, g, third):
        z = self.place.z
        for i in self.some(third):
            bits, above, flips = self.place.masks[i]
            for src, dst in self.pairs(g, 1 - z if flips else z, z + above):
                remote(src, dst, self.z_send.at[g], self.z_recv.at[g, i], self.place.peer(bits)).start()

    def forward(self, g, third):
        for i in self.some(third):
            bits, above, flips = self.place.masks[i]
            position = (1 - self.place.z if flips else self.place.z) + above
            here = self.full.at[g, self.rows(position), :]
            remote(here, here, self.z_send.at[g], self.z_recv.at[g, i], self.place.peer(bits)).wait_recv()
            remote(
                here,
                self.full.at[g, self.rows(position + self.half), :],
                self.x_send.at[g],
                self.x_recv.at[g],
                self.place.x_peer(),
            ).start()

    def finish(self, g):
        z = self.place.z
        here = self.full.at[g, self.rows(z), :]
        pltpu.make_async_copy(here, here, self.local.at[g]).wait()
        there = self.full.at[g, self.rows(self.half, self.half), :]
        remote(there, there, self.x_send.at[g], self.x_recv.at[g], self.place.x_peer()).wait_recv()

    def sent(self, g):
        there = self.full.at[g, self.rows(self.half, self.half), :]
        remote(there, there, self.x_send.at[g], self.x_recv.at[g], self.place.x_peer()).wait_send()
        count = self.half - 1
        those = self.full.at[g, self.rows(0, count), :]
        remote(those, those, self.z_send.at[g], self.z_recv.at[g, 0], self.place.x_peer()).wait_send()


class Gather:
    def __init__(self, place, buffer, send, recv):
        self.place, self.buffer = place, buffer
        self.send, self.recv = send, recv
        self.tokens = buffer.shape[0] // 8
        self.peers = {1: place.c_peer(), 2: place.y_peer(), 4: place.z_peer()}

    def slot(self, s):
        return self.buffer.at[pl.ds(pl.multiple_of(s * self.tokens, self.tokens), self.tokens), :]

    def copy(self, source, bit, src=None):
        s = source + bit
        return remote(self.slot(source) if src is None else src, self.slot(s), self.send.at[s - 1], self.recv.at[s - 1], self.peers[bit])

    def start(self, src=None):
        for bit in (4, 2, 1):
            self.copy(0, bit, src).start()

    def from_z(self):
        self.copy(0, 4).wait_recv()
        self.copy(4, 2).start()
        self.copy(4, 1).start()

    def from_y(self):
        self.copy(0, 2).wait_recv()
        self.copy(2, 1).start()

    def from_zy(self):
        self.copy(4, 2).wait_recv()
        self.copy(6, 1).start()

    def chip(self, source):
        self.copy(source, 1).wait_recv()

    def sent(self, src=None):
        self.copy(0, 4, src).wait_send()
        self.copy(0, 2, src).wait_send()
        self.copy(0, 1, src).wait_send()
        self.copy(4, 2).wait_send()
        self.copy(4, 1).wait_send()
        self.copy(2, 1).wait_send()
        self.copy(6, 1).wait_send()


class HalfGather(Gather):
    def part(self, source, bit, h):
        count = self.tokens // 2
        s = source + bit
        index = s - 1 if h == 0 else 5 + s // 2
        src = self.buffer.at[pl.ds(source * self.tokens + h * count, count), :]
        dst = self.buffer.at[pl.ds(s * self.tokens + h * count, count), :]
        return remote(src, dst, self.send.at[index], self.recv.at[index], self.peers[bit])

    def start(self):
        for h in range(2):
            self.part(0, 4, h).start()
        self.copy(0, 2).start()
        self.copy(0, 1).start()

    def from_z(self):
        self.part(0, 4, 0).wait_recv()
        self.part(4, 2, 0).start()

    def from_z_rest(self):
        self.part(0, 4, 1).wait_recv()
        self.part(4, 2, 1).start()
        self.copy(4, 1).start()

    def from_zy(self):
        for h in range(2):
            self.part(4, 2, h).wait_recv()
        self.copy(6, 1).start()

    def sent(self):
        for h in range(2):
            self.part(0, 4, h).wait_send()
            self.part(4, 2, h).wait_send()
        for source, bit in ((0, 2), (0, 1), (4, 1), (2, 1), (6, 1)):
            self.copy(source, bit).wait_send()


class Scatter:
    def __init__(self, place, keep, c_out, c_in, far_out, far_in, sems):
        self.place = place
        self.keep, self.c_out, self.c_in, self.far_out, self.far_in = keep, c_out, c_in, far_out, far_in
        self.c_send, self.c_recv, self.far_send, self.far_recv = sems
        self.tokens = c_out.shape[1]

    def part(self, b, value):
        self.keep[b] = value[: self.tokens].astype(self.keep.dtype)
        self.c_out[b] = value[self.tokens :].astype(BF)
        self.c_copy(b).start()

    def c_copy(self, b):
        return remote(self.c_out.at[b], self.c_in.at[b], self.c_send.at[b], self.c_recv.at[b], self.place.c_peer())

    def far_copy(self, b):
        peer = self.place.z_peer() if b == 2 else self.place.y_peer()
        return remote(
            self.far_source(b), self.far_in.at[b - 1], self.far_send.at[b - 1], self.far_recv.at[b - 1], peer
        )

    def far_source(self, b):
        return self.keep.at[b] if self.far_out is None else self.far_out.at[b - 1]

    def rows(self, body, step=64):
        def loop(i, carry):
            body(pl.ds(pl.multiple_of(i * step, step), step))
            return carry

        lax.fori_loop(0, self.tokens // step, loop, 0)

    def pass_on(self, b):
        self.c_copy(b).wait_recv()
        if b == 2:
            self.far_copy(3).wait_recv()

        def body(r):
            total = self.keep[b, r, :].astype(F32) + self.c_in[b, r, :].astype(F32)
            if b == 2:
                total = total + self.far_in[2, r, :].astype(F32)
            self.far_source(b)[r, :] = total.astype(BF)

        self.rows(body)
        self.far_copy(b).start()

    def wait_own(self):
        self.c_copy(0).wait_recv()
        self.far_copy(1).wait_recv()
        self.far_copy(2).wait_recv()

    def own(self, r):
        return (
            self.keep[0, r, :].astype(F32)
            + self.c_in[0, r, :].astype(F32)
            + self.far_in[0, r, :].astype(F32)
            + self.far_in[1, r, :].astype(F32)
        )

    def sent(self):
        for b in range(4):
            self.c_copy(b).wait_send()
        for b in (3, 2, 1):
            self.far_copy(b).wait_send()


class HalfScatter(Scatter):
    def half_copy(self, b, h):
        peer = self.place.z_peer() if b == 2 else self.place.y_peer()
        count = self.tokens // 2
        rows = pl.ds(h * count, count)
        index = b - 1 if h == 0 else b + 1
        return remote(
            self.far_source(b).at[rows, :],
            self.far_in.at[b - 1, rows, :],
            self.far_send.at[index],
            self.far_recv.at[index],
            peer,
        )

    def pass_on(self, b, h=0):
        if b == 1:
            super().pass_on(1)
            return
        if h == 0:
            self.c_copy(b).wait_recv()
        if b == 2:
            self.half_copy(3, h).wait_recv()
        step = 64
        count = self.tokens // 2

        def body(i, carry):
            r = pl.ds(pl.multiple_of(h * count + i * step, step), step)
            total = self.keep[b, r, :].astype(F32) + self.c_in[b, r, :].astype(F32)
            if b == 2:
                total = total + self.far_in[2, r, :].astype(F32)
            self.far_source(b)[r, :] = total.astype(BF)
            return carry

        lax.fori_loop(0, count // step, body, 0)
        self.half_copy(b, h).start()
        if b == 3 and h == 0:
            self.pass_on(3, 1)

    def wait_own(self):
        self.c_copy(0).wait_recv()
        self.far_copy(1).wait_recv()
        for h in range(2):
            self.half_copy(2, h).wait_recv()

    def sent(self):
        for b in range(4):
            self.c_copy(b).wait_send()
        self.far_copy(1).wait_send()
        for h in range(2):
            self.half_copy(3, h).wait_send()
            self.half_copy(2, h).wait_send()


def normalized(value):
    center = value - jnp.mean(value, axis=-1, keepdims=True)
    spread = jnp.mean(center * center, axis=-1, keepdims=True)
    return center * lax.rsqrt(spread + EPSILON)


def decay_tile(t, cumul_rows, cumul_here, first, rows, length, tokens):
    square = (rows, rows)
    same = lax.broadcasted_iota(jnp.int32, square, 0) == lax.broadcasted_iota(jnp.int32, square, 1)
    cumul_cols = jnp.sum(jnp.where(same, cumul_here, 0.0), axis=1, keepdims=True)
    index = lax.broadcasted_iota(jnp.int32, (rows, length), 0) + first
    other = lax.broadcasted_iota(jnp.int32, (rows, length), 1)
    at = ((index // tokens) ^ t) * tokens + index % tokens
    to = ((other // tokens) ^ t) * tokens + other % tokens
    causal = at >= to
    return jnp.where(causal, jnp.exp(jnp.where(causal, cumul_cols - cumul_rows, 0.0)), 0.0)


def pack_small(place, small, gains, biases, group, decay, tokens):
    block = small.shape[1]
    wide = place.n_dp * group.shape[1]
    length = decay.shape[1]
    small[...] = jnp.zeros_like(small)
    small[0:2, :] = gains[...].astype(F32)
    small[2:4, :] = biases[...].astype(F32)
    lane = lax.broadcasted_iota(jnp.int32, (2, wide), 1)
    tiled = jnp.concatenate([group[...].astype(F32)] * place.n_dp, axis=1)
    spread = jnp.where(lane // group.shape[1] == place.d, tiled, 0.0)
    at = 4
    for h in range(2):
        for k in range(wide // block):
            small[at : at + 1, :] = spread[h : h + 1, k * block : (k + 1) * block]
            at += 1
    total = decay[...]
    lane = lax.broadcasted_iota(jnp.int32, total.shape, 1)
    shift = 1
    while shift < length:
        total = total + jnp.where(lane >= shift, pltpu.roll(total, shift, 1), 0.0)
        shift *= 2
    for bit in (1, 2):
        pieces = [total[:, (j ^ bit) * tokens : ((j ^ bit) + 1) * tokens] for j in range(length // tokens)]
        total = jnp.where((place.t // bit) % 2 == 1, jnp.concatenate(pieces, axis=1), total)
    for h in range(2):
        for k in range(length // block):
            small[at : at + 1, :] = total[h : h + 1, k * block : (k + 1) * block]
            at += 1


def spread_small(place, own, others, params, group, cumul, block):
    pieces = group.shape[1] // block
    steps = cumul.shape[1] // block
    first = place.z == 0

    def of(above, flips, rows):
        j = place.slot(above, flips)
        return own[rows, :] if j is None else others[j, rows, :]

    head = slice(0, 4)
    for p in range(place.n_dp):
        same, flipped = of(p & ~1, 0, head), of(p & ~1, 1, head)
        params[head, p * block : (p + 1) * block] = jnp.where(place.z == p % 2, same, flipped)

    def head_rows(above, flips, at, count):
        one = of(above, flips, slice(at, at + count))
        two = of(above, flips, slice(at + count, at + 2 * count))
        return jnp.where(first, one, two)

    total = head_rows(0, 0, 4, pieces)
    for bits, above, flips in place.pairs:
        total = total + head_rows(above, flips, 4, pieces)
    for k in range(pieces):
        group[0:1, k * block : (k + 1) * block] = total[k : k + 1, :]
    at = 4 + 2 * pieces
    for row, flips in ((0, 0), (1, 1)):
        value = head_rows(0, flips, at, steps)
        for k in range(steps):
            cumul[row : row + 1, k * block : (k + 1) * block] = value[k : k + 1, :]


def forward_kernel(
    n_dp,
    x_hbm,
    cot_hbm,
    gains_ref,
    biases_ref,
    group_gain_ref,
    decay_ref,
    s_q,
    s_k,
    s_v,
    s_g,
    s_o,
    s_fg,
    s_fu,
    s_fd,
    w_out,
    normed_out,
    qkv_out,
    gate_out,
    mixed_out,
    ffn_in_out,
    hidden_out,
    grads_out,
    cot_out,
    middle_out,
    params_out,
    group_out,
    cumul_out,
    small_ref,
    small_in,
    turned,
    natural,
    params_ref,
    group_ref,
    cum_row_ref,
    x_ref,
    w,
    normed_all,
    cot_all,
    ffn_in,
    qkv,
    gate_in,
    mixed,
    gated,
    gate_hidden,
    up_hidden,
    hidden,
    grads,
    middle,
    keep,
    c_out,
    c_in,
    far_out,
    far_in,
    z_send,
    z_recv,
    x_send,
    x_recv,
    w_local,
    ag_send,
    ag_recv,
    c_send,
    c_recv,
    far_send,
    far_recv,
    out_sem,
    small_send,
    small_recv,
):
    place = Place(n_dp)
    tokens, width = x_ref.shape
    block = width // n_dp
    rows_all = 8 * tokens
    length = rows_all // 2
    head_k = qkv.shape[1] // 4
    scale = 1.0 / math.sqrt(head_k)
    tile = 2 * tokens
    weights = Weights(place, [(s_q, s_k), s_v, s_g, turned.at[0], s_fg, s_fu, turned.at[1]], w, (z_send, z_recv, x_send, x_recv, w_local))
    ag_normed = Gather(place, normed_all, ag_send.at[0], ag_recv.at[0])
    ag_cot = Gather(place, cot_all, ag_send.at[1], ag_recv.at[1])
    ag_two = HalfGather(place, ffn_in, ag_send.at[2], ag_recv.at[2])
    branch = HalfScatter(place, keep, c_out, c_in, far_out, far_in, (c_send, c_recv, far_send, far_recv))
    outs = []

    def save(src, dst, index):
        copy = pltpu.make_async_copy(src, dst, out_sem.at[index])
        copy.start()
        outs.append(copy)

    def over(count, step, body):
        def loop(i, carry):
            body(pl.ds(pl.multiple_of(i * step, step), step), i)
            return carry

        lax.fori_loop(0, count // step, loop, 0)

    for copy in column_copies(place, x_hbm, x_ref, out_sem.at[16], block):
        copy.start()
    for copy in column_copies(place, cot_hbm, ag_cot.slot(0), out_sem.at[17], block):
        copy.start()
    flat = [
        pltpu.make_async_copy(s_o, natural.at[0], out_sem.at[21]),
        pltpu.make_async_copy(s_fd, natural.at[1], out_sem.at[22]),
    ]
    for copy in flat:
        copy.start()
    greet(place, True)
    pack_small(place, small_ref, gains_ref, biases_ref, group_gain_ref, decay_ref, tokens)
    for k, copy in enumerate(flat):
        copy.wait()
        cols = w.shape[2]
        for j in range(2):
            turned[k, :, j * cols : (j + 1) * cols] = natural[k, j * cols : (j + 1) * cols, :].T
    met(place, True)
    small = []
    for j, (bits, above, flips) in enumerate(place.pairs):
        copy = remote(small_ref, small_in.at[j], small_send.at[j], small_recv.at[j], place.peer(bits))
        copy.start()
        small.append(copy)
    size = gate_hidden.shape[1]

    def first_norm(r, i):
        value = normalized(x_ref[r, :].astype(F32))
        normed_all[r, :] = (value * params_ref[0:1, :] + params_ref[2:3, :]).astype(BF)

    def make_qk(r, i):
        qkv[r, : 2 * head_k] = dot_nn(normed_all[r, :], w[QK]).astype(BF)

    def make_v(r, i):
        qkv[r, 2 * head_k :] = dot_nn(normed_all[r, :], w[V]).astype(BF)

    def retention(r, i):
        start = pl.multiple_of((i // 2) * length, length)
        seq = pl.ds(start, length)
        scores = dot_nt(qkv[r, :head_k], qkv[seq, head_k : 2 * head_k])
        here = cum_row_ref[pl.ds(i // 2, 1), pl.ds(pl.multiple_of((i % 2) * tile, tile), tile)]
        decays = decay_tile(
            place.t, cum_row_ref[pl.ds(i // 2, 1), :], here, (i % 2) * tile, tile, length, tokens
        )
        weighted = (scores * decays * scale).astype(BF)
        mixed[r, :] = dot_nn(weighted, qkv[seq, 2 * head_k :])

    def gating(r, i):
        gate = dot_nn(normed_all[r, :], w[G])
        gate_in[r, :] = gate
        value = mixed[r, :]
        center = value - jnp.mean(value, axis=-1, keepdims=True)
        spread = jnp.mean(center * center, axis=-1, keepdims=True)
        flat = center * lax.rsqrt(jnp.maximum(spread, GROUP_FLOOR)) * group_ref[...]
        gated[r, :] = (flat * (gate * lax.logistic(gate))).astype(BF)

    def branch_part(i, carry):
        r = pl.ds(pl.multiple_of((3 - i) * tile, tile), tile)
        branch.part(3 - i, dot_nt(gated[r, :], w[O]))
        return carry

    def second_norm(r, i):
        value = x_ref[r, :].astype(F32) + branch.own(r)
        middle[r, :] = value
        ffn_in[r, :] = (normalized(value) * params_ref[1:2, :] + params_ref[3:4, :]).astype(BF)

    def feed(b):
        r = pl.ds(pl.multiple_of(b * tile, tile), tile)
        gate = dot_nn(ffn_in[r, :], w[FG])
        up = dot_nn(ffn_in[r, :], w[FU])
        gate_hidden[r, :] = gate
        up_hidden[r, :] = up
        hidden[r, :] = (gelu(gate) * up).astype(BF)

    def feed_back(r, i):
        back = dot_nn(cot_all[r, :], w[FD])
        gate = gate_hidden[r, :]
        value, slope = gelu_and_slope(gate)
        grads[r, :size] = (back * up_hidden[r, :] * slope).astype(BF)
        grads[r, size:] = (back * value).astype(BF)

    def small_step():
        pltpu.make_async_copy(x_hbm, x_ref, out_sem.at[16]).wait()
        for copy in small:
            copy.wait()
        spread_small(place, small_ref, small_in, params_ref, group_ref, cum_row_ref, block)

    def norm_step():
        over(tokens, 32, first_norm)

    def cot_start():
        pltpu.make_async_copy(cot_hbm, ag_cot.slot(0), out_sem.at[17]).wait()
        ag_cot.start()

    def chips(ag):
        lax.fori_loop(0, 4, lambda b, carry: (ag.chip(2 * b), carry)[1], 0)

    def qk_step():
        chips(ag_normed)
        weights.finish(QK)
        over(rows_all, tile, make_qk)
        save(normed_all, normed_out, 0)
        save(w.at[QK], w_out.at[QK], 1)
        save(params_ref, params_out, 18)
        save(group_ref, group_out, 19)
        save(cum_row_ref, cumul_out, 20)

    def v_step():
        weights.finish(V)
        over(rows_all, tile, make_v)
        over(rows_all, tile, retention)
        save(w.at[V], w_out.at[V], 2)
        save(qkv, qkv_out, 3)
        save(mixed, mixed_out, 4)

    def g_step():
        weights.finish(G)
        over(rows_all, tile, gating)
        save(w.at[G], w_out.at[G], 5)
        save(gate_in, gate_out, 6)

    def o_step():
        weights.finish(O)
        lax.fori_loop(0, 4, branch_part, 0)
        save(w.at[O], w_out.at[O], 7)

    def second_step():
        branch.wait_own()
        over(tokens, 32, second_norm)
        save(middle, middle_out, 9)

    def feed_step(b):
        if b == 0:
            weights.finish(FG)
            weights.finish(FU)
            save(w.at[FG], w_out.at[FG], 10)
            save(w.at[FU], w_out.at[FU], 11)

        def one(i, carry):
            ag_two.chip(2 * i)
            feed(i)
            return carry

        lax.fori_loop(b, b + 1, one, 0)

    def last_step():
        save(ffn_in, ffn_in_out, 12)
        save(hidden, hidden_out, 13)
        chips(ag_cot)
        save(cot_all, cot_out, 8)
        weights.finish(FD)
        save(w.at[FD], w_out.at[FD], 14)
        over(rows_all, tile, feed_back)
        save(grads, grads_out, 15)

    steps = {
        "small": small_step,
        "ln": norm_step,
        "ns": ag_normed.start,
        "nfz": ag_normed.from_z,
        "nfy": ag_normed.from_y,
        "nfzy": ag_normed.from_zy,
        "ks": cot_start,
        "kfz": ag_cot.from_z,
        "kfy": ag_cot.from_y,
        "kfzy": ag_cot.from_zy,
        "ts": ag_two.start,
        "tfz": ag_two.from_z,
        "tfzB": ag_two.from_z_rest,
        "tfy": ag_two.from_y,
        "tfzy": ag_two.from_zy,
        "qk": qk_step,
        "v": v_step,
        "g": g_step,
        "o": o_step,
        "p3": lambda: branch.pass_on(3),
        "p1": lambda: branch.pass_on(1),
        "p2": lambda: branch.pass_on(2),
        "p2B": lambda: branch.pass_on(2, 1),
        "ln2": second_step,
        "feedA": lambda: feed_step(0),
        "feedB": lambda: feed_step(1),
        "feedC": lambda: feed_step(2),
        "feedD": lambda: feed_step(3),
        "back": last_step,
    }
    for name in FORWARD:
        if name[1:].isdigit():
            g = int(name[1])
            if name[0] == "x":
                weights.own(g)
            elif name[0] == "s":
                weights.start(g, int(name[2]) - 1)
            elif name[0] == "f":
                weights.forward(g, int(name[2]) - 1)
            else:
                steps[name]()
        else:
            steps[name]()
    for copy in outs:
        copy.wait()
    for g in range(GROUPS):
        weights.sent(g)
    ag_normed.sent()
    ag_cot.sent()
    ag_two.sent()
    branch.sent()


ROOT = math.sqrt(2.0 / math.pi)


def gelu(v):
    return 0.5 * v * (1.0 + jnp.tanh(ROOT * (v + 0.044715 * v * v * v)))


def gelu_and_slope(v):
    inside = jnp.tanh(ROOT * (v + 0.044715 * v * v * v))
    slope = 0.5 * (1.0 + inside) + 0.5 * v * (1.0 - inside * inside) * ROOT * (1.0 + 3 * 0.044715 * v * v)
    return 0.5 * v * (1.0 + inside), slope


def forward_call(n_dp, x, cot, smalls, sources):
    tokens, width = x.shape
    length = 4 * tokens
    block = width // n_dp
    rows_all = 8 * tokens
    cols = sources[2].shape[1] // 2
    small_rows = -(-(4 + 2 * (cols + length) // block) // 8) * 8
    masks = n_dp // 2 - 1
    vmem, hbm = pl.BlockSpec(memory_space=pltpu.VMEM), pl.BlockSpec(memory_space=pl.ANY)
    shape = jax.ShapeDtypeStruct
    outs = (
        shape((GROUPS, width, cols), BF),
        shape((rows_all, width), BF),
        shape((rows_all, 2 * cols), BF),
        shape((rows_all, cols), F32),
        shape((rows_all, cols), F32),
        shape((rows_all, width), BF),
        shape((rows_all, cols), BF),
        shape((rows_all, 2 * cols), BF),
        shape((rows_all, width), BF),
        shape((tokens, width), F32),
        shape((8, width), F32),
        shape((1, cols), F32),
        shape((2, length), F32),
    )
    dma = pltpu.SemaphoreType.DMA
    scratch = [
        pltpu.VMEM((small_rows, block), F32),
        pltpu.VMEM((n_dp - 1, small_rows, block), F32),
        pltpu.VMEM((2, block, 2 * cols), BF),
        pltpu.VMEM((2, 2 * cols, block), BF),
        pltpu.VMEM((8, width), F32),
        pltpu.VMEM((1, cols), F32),
        pltpu.VMEM((2, length), F32),
        pltpu.VMEM((tokens, width), BF),
        pltpu.VMEM((GROUPS, width, cols), BF),
        pltpu.VMEM((rows_all, width), BF),
        pltpu.VMEM((rows_all, width), BF),
        pltpu.VMEM((rows_all, width), BF),
        pltpu.VMEM((rows_all, 2 * cols), BF),
        pltpu.VMEM((rows_all, cols), F32),
        pltpu.VMEM((rows_all, cols), F32),
        pltpu.VMEM((rows_all, cols), BF),
        pltpu.VMEM((rows_all, cols), F32),
        pltpu.VMEM((rows_all, cols), F32),
        pltpu.VMEM((rows_all, cols), BF),
        pltpu.VMEM((rows_all, 2 * cols), BF),
        pltpu.VMEM((tokens, width), F32),
        pltpu.VMEM((4, tokens, width), F32),
        pltpu.VMEM((4, tokens, width), BF),
        pltpu.VMEM((4, tokens, width), BF),
        pltpu.VMEM((3, tokens, width), BF),
        pltpu.VMEM((3, tokens, width), BF),
        dma((GROUPS,)),
        dma((GROUPS, masks)),
        dma((GROUPS,)),
        dma((GROUPS,)),
        dma((GROUPS,)),
        dma((3, 9)),
        dma((3, 9)),
        dma((4,)),
        dma((4,)),
        dma((5,)),
        dma((5,)),
        dma((23,)),
        dma((n_dp - 1,)),
        dma((n_dp - 1,)),
    ]
    return pl.pallas_call(
        functools.partial(forward_kernel, n_dp),
        out_shape=outs,
        in_specs=[hbm, hbm] + [vmem] * 4 + [hbm] * len(sources),
        out_specs=(hbm,) * len(outs),
        scratch_shapes=scratch,
        compiler_params=pltpu.CompilerParams(
            collective_id=1, has_side_effects=True, vmem_limit_bytes=64_000_000
        ),
    )(x, cot, *smalls, *sources)


class Reduce:
    def __init__(self, place, keep, x_out, x_in, z_in, own_out, sems, own_sem):
        self.place = place
        self.keep, self.x_out, self.x_in, self.z_in, self.own_out = keep, x_out, x_in, z_in, own_out
        self.x_send, self.x_recv, self.z_send, self.z_recv = sems
        self.own_sem = own_sem
        self.block = z_in.shape[2]
        self.half = place.n_dp // 2
        z = place.z
        self.targets = [
            ((1 - z if flips else z) + above, i, place.peer(bits)) for i, (bits, above, flips) in enumerate(place.masks)
        ]
        self.targets.reverse()

    def rows(self, position):
        return pl.ds(pl.multiple_of(position * self.block, self.block), self.block)

    def x_copy(self, g, ring, position):
        return remote(
            self.x_out.at[ring, self.rows(position), :],
            self.x_in.at[g, self.rows(position), :],
            self.x_send.at[g],
            self.x_recv.at[g, position],
            self.place.x_peer(),
        )

    def z_copy(self, g, position, i, peer):
        return remote(
            self.keep.at[g, self.rows(position), :],
            self.z_in.at[g, i],
            self.z_send.at[g],
            self.z_recv.at[g, i],
            peer,
        )

    def upper(self, g, ring, left, right, col, step):
        width = left.shape[1] // 2
        cols = self.keep.shape[2]

        def body(i, carry):
            at = pl.multiple_of(i * step, step)
            value = dot_tn(left[:, pl.ds(pl.multiple_of(width + at, step), step)], right[:, col : col + cols])
            self.x_out[ring, pl.ds(at, step), :] = value.astype(BF)
            return carry

        lax.fori_loop(0, width // step, body, 0)
        for position, _, _ in self.targets:
            self.x_copy(g, ring, position).start()
        self.x_copy(g, ring, self.place.z).start()

    def lower(self, g, left, right, col, step):
        width = left.shape[1] // 2
        cols = self.keep.shape[2]

        def body(i, carry):
            at = pl.ds(pl.multiple_of(i * step, step), step)
            self.keep[g, at, :] = dot_tn(left[:, at], right[:, col : col + cols]).astype(BF)
            return carry

        lax.fori_loop(0, width // step, body, 0)

    def x_sent(self, g, ring):
        whole = self.x_out.at[ring]
        remote(whole, whole, self.x_send.at[g], self.x_recv.at[g, 0], self.place.x_peer()).wait_send()

    def add(self, g, ring, position):
        self.x_copy(g, ring, position).wait_recv()
        step = min(64, self.block)

        def body(i, carry):
            r = pl.ds(pl.multiple_of(position * self.block + i * step, step), step)
            self.keep[g, r, :] = (self.keep[g, r, :].astype(F32) + self.x_in[g, r, :].astype(F32)).astype(BF)
            return carry

        lax.fori_loop(0, self.block // step, body, 0)

    def own_copy(self, g):
        return pltpu.make_async_copy(
            self.keep.at[g, self.rows(self.place.z), :], self.own_out.at[g], self.own_sem.at[g]
        )

    def step(self, g, ring, third):
        if third == 0:
            self.add(g, ring, self.place.z)
            self.own_copy(g).start()
            return
        count = len(self.targets)
        for position, i, peer in self.targets[(3 - third) * count // 3 : (4 - third) * count // 3]:
            self.add(g, ring, position)
            self.z_copy(g, position, i, peer).start()

    def finish(self, g):
        self.own_copy(g).wait()
        for position, i, peer in self.targets:
            self.z_copy(g, position, i, peer).wait()


def norm_back(value, grad, gain):
    center = value - jnp.mean(value, axis=-1, keepdims=True)
    spread = jnp.mean(center * center, axis=-1, keepdims=True)
    r = lax.rsqrt(spread + EPSILON)
    hat = center * r
    scaled = grad * gain
    back = r * (
        scaled - jnp.mean(scaled, axis=-1, keepdims=True) - hat * jnp.mean(scaled * hat, axis=-1, keepdims=True)
    )
    return back, jnp.sum(grad * hat, axis=0, keepdims=True), jnp.sum(grad, axis=0, keepdims=True)


def backward_kernel(
    n_dp,
    x_hbm,
    params_ref,
    group_ref,
    cum_row_ref,
    w_ref,
    normed_ref,
    qkv_ref,
    gate_ref,
    mixed_ref,
    ffn_in_ref,
    hidden_ref,
    grads_ref,
    cot_ref,
    middle_ref,
    layer_out,
    input_grad_out,
    own_out,
    z_in,
    sums_out,
    w,
    tokens_a,
    ffn_in,
    branch_all,
    slim,
    qkv,
    gate_in,
    mixed,
    gated,
    x_ref,
    middle,
    grad_middle,
    sums,
    sums_in,
    group_sum,
    payload,
    payload_in,
    keep,
    c_out,
    c_in,
    far_in,
    c_in_two,
    far_in_two,
    dw_keep,
    x_out,
    x_in,
    ag_send,
    ag_recv,
    c_send,
    c_recv,
    far_send,
    far_recv,
    x_send,
    x_recv,
    z_send,
    z_recv,
    load_sem,
    own_sem,
    sum_send,
    sum_recv,
    pay_send,
    pay_recv,
):
    place = Place(n_dp)
    tokens, width = x_ref.shape
    rows_all = 8 * tokens
    length = rows_all // 2
    cols = gated.shape[1]
    head_k = cols // 2
    scale = 1.0 / math.sqrt(head_k)
    tile = 2 * tokens
    step = min(512, width // 2)
    block = z_in.shape[2]
    ag = Gather(place, branch_all, ag_send, ag_recv)

    def scatter(k, c, far):
        return Scatter(place, keep, c_out, c, None, far, (c_send.at[k], c_recv.at[k], far_send.at[k], far_recv.at[k]))

    rs_two = scatter(0, c_in, far_in)
    rs_out = scatter(1, c_in_two, far_in_two)
    rs_one = scatter(2, c_in, far_in)
    dw = Reduce(place, dw_keep, x_out, x_in, z_in, own_out, (x_send, x_recv, z_send, z_recv), own_sem)
    result = ffn_in.at[:tokens, :]
    weighted = ffn_in.at[tokens : tokens + length, :length]
    score_back = ffn_in.at[tokens : tokens + length, length : 2 * length]
    ring = {FD: 0, FG: 1, FU: 2, O: 3, G: 0, QK: 1, V: 2}

    def load(src, dst, index):
        copy = pltpu.make_async_copy(src, dst, load_sem.at[index])
        copy.start()
        return copy

    def over(count, size, body):
        def loop(i, carry):
            body(pl.ds(pl.multiple_of(i * size, size), size), i)
            return carry

        lax.fori_loop(0, count // size, loop, 0)

    in_cot = load(cot_ref, tokens_a, 3)
    in_hidden = load(hidden_ref, slim.at[:, 2 * cols :], 4)
    in_grads = load(grads_ref, slim.at[:, : 2 * cols], 0)
    in_fg = load(w_ref.at[FG], w.at[0], 1)
    in_fu = load(w_ref.at[FU], w.at[1], 2)
    in_ffn = load(ffn_in_ref, ffn_in, 5)
    in_middle = load(middle_ref, middle, 6)
    in_mixed = load(mixed_ref, mixed, 7)
    in_gate = load(gate_ref, gate_in, 8)
    in_o = load(w_ref.at[O], w.at[2], 9)
    in_qkv = load(qkv_ref, qkv, 10)
    for copy in column_copies(place, x_hbm, x_ref, load_sem.at[11], block):
        copy.start()
    sums[...] = jnp.zeros_like(sums)
    group_sum[...] = jnp.zeros_like(group_sum)
    entry_barrier(place, True)
    waited = []

    def ready(*copies):
        for copy in copies:
            if not any(copy is other for other in waited):
                waited.append(copy)
                copy.wait()

    def rows_of(i):
        return 3 - i, pl.ds(pl.multiple_of((3 - i) * tile, tile), tile)

    def two_part(i, carry):
        b, r = rows_of(i)
        rs_two.part(b, dot_nt(slim[r, :cols], w[0]) + dot_nt(slim[r, cols : 2 * cols], w[1]))
        return carry

    def gating(r, i):
        value = mixed[r, :]
        center = value - jnp.mean(value, axis=-1, keepdims=True)
        spread = jnp.mean(center * center, axis=-1, keepdims=True)
        gate = gate_in[r, :]
        flat = center * lax.rsqrt(jnp.maximum(spread, GROUP_FLOOR)) * group_ref[...]
        gated[r, :] = (flat * (gate * lax.logistic(gate))).astype(BF)

    def second_back(r, i):
        back, gain_sum, bias_sum = norm_back(middle[r, :], rs_two.own(r), params_ref[1:2, :])
        total = tokens_a[r, :].astype(F32) + back
        grad_middle[r, :] = total
        branch_all[r, :] = total.astype(BF)
        sums[1:2, :] += gain_sum
        sums[3:4, :] += bias_sum

    def out_part(i, carry):
        b, r = rows_of(i)
        rs_out.part(b, dot_nt(slim[r, 2 * cols :], w[0]))
        return carry

    def gating_back(b):
        r = pl.ds(pl.multiple_of(b * tile, tile), tile)
        back = dot_nn(branch_all[r, :], w[2])
        value = mixed[r, :]
        center = value - jnp.mean(value, axis=-1, keepdims=True)
        spread = jnp.mean(center * center, axis=-1, keepdims=True)
        inverse = lax.rsqrt(jnp.maximum(spread, GROUP_FLOOR))
        hat = center * inverse
        gate = gate_in[r, :]
        sigmoid = lax.logistic(gate)
        flat = hat * group_ref[...]
        slope = sigmoid * (1.0 + gate * (1.0 - sigmoid))
        slim[r, 2 * cols :] = (back * flat * slope).astype(BF)
        grad = back * (gate * sigmoid)
        group_sum[...] += jnp.sum(grad * hat, axis=0, keepdims=True)
        scaled = grad * group_ref[...]
        live = jnp.where(spread > GROUP_FLOOR, 1.0, jnp.where(spread == GROUP_FLOOR, 0.5, 0.0))
        moment = jnp.mean(scaled * hat, axis=-1, keepdims=True) * live
        mixed_back = inverse * (scaled - jnp.mean(scaled, axis=-1, keepdims=True) - hat * moment)
        slim[r, cols : 2 * cols] = mixed_back.astype(BF)

    def sequence_back(s):
        seq = pl.ds(pl.multiple_of(s * length, length), length)

        def body(i, carry):
            r = pl.ds(pl.multiple_of(s * length + i * tile, tile), tile)
            at = pl.ds(pl.multiple_of(i * tile, tile), tile)
            scores = dot_nt(qkv[r, :head_k], qkv[seq, head_k : 2 * head_k])
            here = cum_row_ref[pl.ds(s, 1), at]
            decays = decay_tile(
                place.t, cum_row_ref[pl.ds(s, 1), :], here, i * tile, tile, length, tokens
            )
            weighted[at, :] = (scores * decays * scale).astype(BF)
            back = dot_nt(slim[r, cols : 2 * cols], qkv[seq, 2 * head_k :])
            grad = (back * decays * scale).astype(BF)
            score_back[at, :] = grad
            slim[r, :head_k] = dot_nn(grad, qkv[seq, head_k : 2 * head_k]).astype(BF)
            return carry

        lax.fori_loop(0, length // tile, body, 0)
        slim[seq, head_k : 2 * head_k] = dot_tn(score_back[...], qkv[seq, :head_k]).astype(BF)
        slim[seq, cols : 2 * cols] = dot_tn(weighted[...], slim[seq, cols : 2 * cols]).astype(BF)


    def finish_out(r, i):
        result[r, :] = (middle[r, :] + rs_out.own(r)).astype(BF)

    def one_part(i, carry):
        b, r = rows_of(i)
        total = dot_nt(slim[r, :cols], w[1]) + dot_nt(slim[r, cols : 2 * cols], w[0])
        rs_one.part(b, total + dot_nt(slim[r, 2 * cols :], w[2]))
        return carry

    def first_back(r, i):
        back, gain_sum, bias_sum = norm_back(x_ref[r, :].astype(F32), rs_one.own(r), params_ref[0:1, :])
        result[r, :] = (grad_middle[r, :] + back).astype(BF)
        sums[0:1, :] += gain_sum
        sums[2:3, :] += bias_sum

    def sum_copy(k):
        peer = (place.c_peer(), place.y_peer())[k]
        return remote(sums, sums_in.at[k], sum_send.at[k], sum_recv.at[k], peer)

    pay = []
    for j, (bits, above, flips) in enumerate(place.pairs):
        position = (1 - place.z if flips else place.z) + above
        pay.append(remote(payload.at[position], payload_in.at[j], pay_send.at[j], pay_recv.at[j], place.peer(bits)))

    later = {}
    operands = {
        FD: (tokens_a, 2 * cols),
        FG: (ffn_in, 0),
        FU: (ffn_in, cols),
        O: (branch_all, None),
        QK: (tokens_a, 0),
        V: (tokens_a, cols),
        G: (tokens_a, 2 * cols),
    }

    def operands_of(g):
        ready(*{FD: (in_cot, in_hidden), FG: (in_ffn, in_grads), FU: (in_ffn, in_grads), O: ()}.get(g, (later.get(3),)))
        left, col = operands[g]
        return (left, gated, 0, step) if col is None else (left, slim, col, step)

    def two_step():
        ready(in_grads, in_fg, in_fu)
        lax.fori_loop(0, 4, two_part, 0)
        later[FD] = load(w_ref.at[FD], w.at[0], 1)
        later[QK] = load(w_ref.at[QK], w.at[1], 2)

    def gating_step():
        ready(in_mixed, in_gate)
        over(rows_all, tokens, gating)

    def second_step():
        ready(in_middle)
        rs_two.wait_own()
        over(tokens, 32, second_back)
        later[3] = load(normed_ref, tokens_a, 3)

    def out_step():
        rs_two.sent()
        ready(later[FD])
        lax.fori_loop(0, 4, out_part, 0)
        later[V] = load(w_ref.at[V], w.at[0], 1)

    def chip_step(first):
        ready(in_o, in_qkv)

        def chip(b, carry):
            ag.chip(2 * b)
            gating_back(b)
            return carry

        lax.fori_loop(first, first + 2, chip, 0)
        if first:
            later[G] = load(w_ref.at[G], w.at[2], 9)

    def sequence_step(s):
        lax.fori_loop(s, s + 1, lambda i, carry: (sequence_back(i), carry)[1], 0)

    def out_finish():
        rs_out.wait_own()
        over(tokens, 16, finish_out)
        later["layer"] = load(result, layer_out, 4)

    def one_step():
        rs_out.sent()
        ready(later[QK], later[V], later[G])
        lax.fori_loop(0, 4, one_part, 0)

    def first_step():
        pltpu.make_async_copy(x_hbm, x_ref, load_sem.at[11]).wait()
        ready(later["layer"])
        rs_one.wait_own()
        over(tokens, 32, first_back)
        later["grad"] = load(result, input_grad_out, 4)

    def sum_cores():
        sum_copy(0).start()

    def sum_chips():
        sum_copy(0).wait()
        sums[...] += sums_in[0]
        sum_copy(1).start()

    def pay_start():
        sum_copy(1).wait()
        sums[...] += sums_in[1]
        for p in range(n_dp):
            payload[p, 0:4, :] = sums[0:4, p * block : (p + 1) * block]
            for k in range(cols // block):
                payload[p, 4 + k : 5 + k, :] = group_sum[0:1, k * block : (k + 1) * block]
        for copy in pay:
            copy.start()

    def pay_finish():
        for copy in pay:
            copy.wait()
        mine = payload[place.z]
        other = jnp.zeros_like(mine)
        for j, (bits, above, flips) in enumerate(place.pairs):
            if flips:
                other = other + payload_in[j]
            else:
                mine = mine + payload_in[j]
        sums_out[0] = mine
        sums_out[1] = other

    before = {G: FD, QK: FG, V: FU}

    def upper(g):
        if g in before:
            dw.x_sent(before[g], ring[before[g]])
        dw.upper(g, ring[g], *operands_of(g))

    steps = {
        "two": two_step,
        "a3": lambda: rs_two.pass_on(3),
        "a1": lambda: rs_two.pass_on(1),
        "a2": lambda: rs_two.pass_on(2),
        "gat": gating_step,
        "lnb": second_step,
        "bs": ag.start,
        "bfz": ag.from_z,
        "bfy": ag.from_y,
        "bfzy": ag.from_zy,
        "out": out_step,
        "o3": lambda: rs_out.pass_on(3),
        "o1": lambda: rs_out.pass_on(1),
        "o2": lambda: rs_out.pass_on(2),
        "gbA": lambda: chip_step(0),
        "gbB": lambda: chip_step(2),
        "seq0": lambda: sequence_step(0),
        "seq1": lambda: sequence_step(1),
        "outf": out_finish,
        "one": one_step,
        "b3": lambda: rs_one.pass_on(3),
        "b1": lambda: rs_one.pass_on(1),
        "b2": lambda: rs_one.pass_on(2),
        "lna": first_step,
        "sc": sum_cores,
        "sy": sum_chips,
        "pay": pay_start,
        "payw": pay_finish,
    }
    for name in BACKWARD:
        if name in steps:
            steps[name]()
        elif name[0] == "u":
            upper(int(name[1]))
        elif name[0] == "l":
            dw.lower(int(name[1]), *operands_of(int(name[1])))
        else:
            dw.step(int(name[1]), ring[int(name[1])], int(name[2]))
    ready(later["grad"])
    for g in (O, G, QK, V):
        dw.x_sent(g, ring[g])
    ag.sent()
    rs_one.sent()
    for g in (FD, FG, FU, O, G, QK, V):
        dw.finish(g)


def backward_call(n_dp, x, params, group, cum_row, saved):
    tokens, width = x.shape
    rows_all = 8 * tokens
    w = saved[0]
    cols = w.shape[2]
    block = width // n_dp
    masks = n_dp // 2 - 1
    vmem, hbm = pl.BlockSpec(memory_space=pltpu.VMEM), pl.BlockSpec(memory_space=pl.ANY)
    shape = jax.ShapeDtypeStruct
    pay_rows = -(-(4 + cols // block) // 8) * 8
    outs = (
        shape((tokens, width), BF),
        shape((tokens, width), BF),
        shape((GROUPS, block, cols), BF),
        shape((GROUPS, masks, block, cols), BF),
        shape((2, pay_rows, block), F32),
    )
    dma = pltpu.SemaphoreType.DMA
    scratch = [
        pltpu.VMEM((3, width, cols), BF),
        pltpu.VMEM((rows_all, width), BF),
        pltpu.VMEM((rows_all, width), BF),
        pltpu.VMEM((rows_all, width), BF),
        pltpu.VMEM((rows_all, 3 * cols), BF),
        pltpu.VMEM((rows_all, 2 * cols), BF),
        pltpu.VMEM((rows_all, cols), F32),
        pltpu.VMEM((rows_all, cols), F32),
        pltpu.VMEM((rows_all, cols), BF),
        pltpu.VMEM((tokens, width), BF),
        pltpu.VMEM((tokens, width), F32),
        pltpu.VMEM((tokens, width), F32),
        pltpu.VMEM((8, width), F32),
        pltpu.VMEM((2, 8, width), F32),
        pltpu.VMEM((1, cols), F32),
        pltpu.VMEM((n_dp, pay_rows, block), F32),
        pltpu.VMEM((n_dp - 1, pay_rows, block), F32),
        pltpu.VMEM((4, tokens, width), BF),
        pltpu.VMEM((4, tokens, width), BF),
        pltpu.VMEM((4, tokens, width), BF),
        pltpu.VMEM((3, tokens, width), BF),
        pltpu.VMEM((4, tokens, width), BF),
        pltpu.VMEM((3, tokens, width), BF),
        pltpu.VMEM((GROUPS, width // 2, cols), BF),
        pltpu.VMEM((4, width // 2, cols), BF),
        pltpu.VMEM((GROUPS, width // 2, cols), BF),
        dma((7,)),
        dma((7,)),
        dma((3, 4)),
        dma((3, 4)),
        dma((3, 3)),
        dma((3, 3)),
        dma((GROUPS,)),
        dma((GROUPS, n_dp // 2)),
        dma((GROUPS,)),
        dma((GROUPS, masks)),
        dma((12,)),
        dma((GROUPS,)),
        dma((2,)),
        dma((2,)),
        dma((n_dp - 1,)),
        dma((n_dp - 1,)),
    ]
    return pl.pallas_call(
        functools.partial(backward_kernel, n_dp),
        out_shape=outs,
        in_specs=[hbm, vmem, vmem, vmem] + [hbm] * len(saved),
        out_specs=(hbm,) * 4 + (vmem,),
        scratch_shapes=scratch,
        compiler_params=pltpu.CompilerParams(
            collective_id=2, has_side_effects=True, vmem_limit_bytes=67_000_000
        ),
    )(x, params, group, cum_row, *saved)


def finish_kernel(
    n_dp,
    own_ref,
    others_ref,
    layer_ref,
    grad_ref,
    sums_ref,
    layer_out,
    input_grad,
    query_grad,
    key_grad,
    value_grad,
    gate_grad,
    out_grad,
    group_grad,
    gain_grad,
    bias_grad,
    ffn_gate_grad,
    ffn_up_grad,
    ffn_down_grad,
    own,
    others,
    rows,
    wide,
    tall,
    in_sem,
    out_sem,
    row_sem,
):
    place = Place(n_dp)
    z = place.z
    block, cols = own.shape[1:]
    loads = []
    for g in (FD, FG, FU, O, QK, V, G):
        pair = (
            pltpu.make_async_copy(own_ref.at[g], own.at[g], in_sem.at[0, g]),
            pltpu.make_async_copy(others_ref.at[g], others.at[g], in_sem.at[1, g]),
        )
        for copy in pair:
            copy.start()
        loads.append((g, pair))
    row_loads = [
        pltpu.make_async_copy(layer_ref, rows.at[0], row_sem.at[0]),
        pltpu.make_async_copy(grad_ref, rows.at[1], row_sem.at[1]),
    ]
    for copy in row_loads:
        copy.start()
    outs = []

    def save(src, dst, index):
        copy = pltpu.make_async_copy(src, dst, out_sem.at[index])
        copy.start()
        outs.append(copy)

    wide_at = {FG: 0, FU: 1, V: 2, G: 3, QK: 4}
    tall_at = {FD: 0, O: 1}
    targets = {FG: ffn_gate_grad, FU: ffn_up_grad, V: value_grad, G: gate_grad, FD: ffn_down_grad, O: out_grad}
    for g, pair in loads:
        for copy in pair:
            copy.wait()
        mine = own[g].astype(F32)
        theirs = None
        for i, (bits, above, flips) in enumerate(place.masks):
            value = others[g, i].astype(F32)
            if not flips:
                mine = mine + value
            else:
                theirs = value if theirs is None else theirs + value
        if g in tall_at:
            k = tall_at[g]
            tall[k, pl.ds(pl.multiple_of(z * cols, cols), cols), :] = mine.T
            tall[k, pl.ds(pl.multiple_of((1 - z) * cols, cols), cols), :] = theirs.T
            save(tall.at[k], targets[g], k)
            continue
        k = wide_at[g]
        if g == QK:
            half = cols // 2
            for which, dst in ((0, query_grad), (1, key_grad)):
                part = slice(which * half, (which + 1) * half)
                at = which * cols
                wide[k, :, pl.ds(pl.multiple_of(at + z * half, half), half)] = mine[:, part]
                wide[k, :, pl.ds(pl.multiple_of(at + (1 - z) * half, half), half)] = theirs[:, part]
                save(wide.at[k, :, pl.ds(at, cols)], dst, 2 + which)
            continue
        wide[k, :, pl.ds(pl.multiple_of(z * cols, cols), cols)] = mine
        wide[k, :, pl.ds(pl.multiple_of((1 - z) * cols, cols), cols)] = theirs
        save(wide.at[k], targets[g], 4 + k)
    for k, dst in ((0, layer_out), (1, input_grad)):
        row_loads[k].wait()
        for copy in column_copies(place, rows.at[k], dst, row_sem.at[k], block, True):
            copy.start()
    norm = sums_ref[0, 0:4, :] + sums_ref[1, 0:4, :]
    piece = gain_grad.shape[1]
    mine = norm[:, :piece]
    for k in range(1, block // piece):
        mine = jnp.where(place.t == k, norm[:, k * piece : (k + 1) * piece], mine)
    gain_grad[...] = mine[0:2, :]
    bias_grad[...] = mine[2:4, :]
    piece = group_grad.shape[1]
    here = place.d % (block // piece)
    row = place.d // (block // piece)

    def group_of(which):
        value = sums_ref[which, 4:5, :]
        for k in range(1, cols // block):
            value = jnp.where(row == k, sums_ref[which, 4 + k : 5 + k, :], value)
        out = value[:, :piece]
        for k in range(1, block // piece):
            out = jnp.where(here == k, value[:, k * piece : (k + 1) * piece], out)
        return out

    same, other = group_of(0), group_of(1)
    group_grad[0:1, :] = jnp.where(z == 0, same, other)
    group_grad[1:2, :] = jnp.where(z == 0, other, same)
    for copy in outs:
        copy.wait()
    for k, dst in ((0, layer_out), (1, input_grad)):
        pltpu.make_async_copy(rows.at[k], dst, row_sem.at[k]).wait()


def finish_call(n_dp, n_tensor, own, others, layer, grad, sums):
    tokens, width = layer.shape
    block, cols = own.shape[1:]
    masks = others.shape[1]
    vmem, hbm = pl.BlockSpec(memory_space=pltpu.VMEM), pl.BlockSpec(memory_space=pl.ANY)
    shape = jax.ShapeDtypeStruct
    rows, wide, tall = shape((tokens, width), BF), shape((block, 2 * cols), F32), shape((2 * cols, block), F32)
    thin, norm = shape((block, cols), F32), shape((2, width // (n_dp * n_tensor)), F32)
    outs = (rows, rows, thin, thin, wide, wide, tall, shape((2, cols // n_dp), F32), norm, norm, wide, wide, tall)
    specs = [vmem if o.shape[0] == 2 else hbm for o in outs]
    dma = pltpu.SemaphoreType.DMA
    return pl.pallas_call(
        functools.partial(finish_kernel, n_dp),
        out_shape=outs,
        in_specs=[hbm, hbm, hbm, hbm, vmem],
        out_specs=tuple(specs),
        scratch_shapes=[
            pltpu.VMEM((GROUPS, block, cols), BF),
            pltpu.VMEM((GROUPS, masks, block, cols), BF),
            pltpu.VMEM((2, tokens, width), BF),
            pltpu.VMEM((5, block, 2 * cols), F32),
            pltpu.VMEM((2, 2 * cols, block), F32),
            dma((2, GROUPS)),
            dma((8,)),
            dma((2,)),
        ],
        compiler_params=pltpu.CompilerParams(vmem_limit_bytes=67_000_000),
    )(own, others, layer, grad, sums)


def per_device(
    n_dp,
    n_tensor,
    inputs,
    cotangent,
    log_decay,
    query_weight,
    key_weight,
    value_weight,
    gate_weight,
    out_weight,
    group_gain,
    norm_gains,
    norm_biases,
    ffn_gate_weight,
    ffn_up_weight,
    ffn_down_weight,
):
    place = Place(n_dp)
    d, t = place.d, place.t
    tokens, width = inputs.shape
    block = width // n_dp

    def position_of(q):
        out = (q // PAIR) & 1
        for k, bit in enumerate(place.rest):
            out = out + ((d // bit) % 2 ^ ((q // bit) & 1)) * (2 << k)
        return out

    def moved(value, index):
        if block % 128 == 0:
            return value
        return jnp.concatenate(
            [lax.dynamic_slice_in_dim(value, index(p) * block, block, 1) for p in range(n_dp)], axis=1
        )

    smalls = (norm_gains, norm_biases, group_gain, log_decay)
    sources = (
        query_weight,
        key_weight,
        value_weight,
        gate_weight,
        out_weight,
        ffn_gate_weight,
        ffn_up_weight,
        ffn_down_weight,
    )
    x, cot = moved(inputs, place.dp_of), moved(cotangent, place.dp_of)
    *saved, params, group, cumul = forward_call(n_dp, x, cot, smalls, sources)
    layer, grad, own, others, sums = backward_call(n_dp, x, params, group, cumul, saved)
    outs = finish_call(n_dp, n_tensor, own, others, layer, grad, sums)
    return (moved(outs[0], position_of), moved(outs[1], position_of), *outs[2:])


def solution(mesh):
    tokens = P(("dp", "tensor"), None)
    rows, cols, norms = P("dp", "tensor"), P("tensor", "dp"), P(None, "dp")
    sums = P(None, ("dp", "tensor"))
    in_specs = (tokens, tokens, cols, rows, rows, rows, rows, cols, cols, norms, norms, rows, rows, cols)
    out_specs = (tokens, tokens, rows, rows, rows, rows, cols, cols, sums, sums, rows, rows, cols)
    body = functools.partial(per_device, mesh.shape["dp"], mesh.shape["tensor"])
    return jax.shard_map(body, mesh=mesh, in_specs=in_specs, out_specs=out_specs, check_vma=False)
```
